256 devices in a mesh: wide: 64 (over y, z, x_hi), narrow: 4 (over x_lo, core).
Axes of the slice: x: 4 (x_hi: 2, x_lo: 2; x = x_hi * 2 + x_lo), y: 4, z: 8, core: 2. Of those that a mesh axis runs over, the one named last changes fastest.
Arguments:
- rhs: float32 [3, 256, 32, 128], P(None, 'wide', 'narrow'), may hold values from -12 to 12
- start: float32 [3, 256, 32, 128], P(None, 'wide', 'narrow'), may hold values from -2 to 2
- trans: float32 [3, 256, 32, 128], P(None, 'wide', 'narrow'), may hold values from 0.2 to 2
- accum: float32 [256, 32, 128], P('wide', 'narrow'), may hold values from 2 to 8
- coupling: float32 [3, 3, 256, 32, 128], P(None, None, 'wide', 'narrow'), may hold values from -0.3 to 0.3
- well_cells: int32 [64, 4, 64], P('wide', 'narrow'), may hold values from 0 to 4095
- well_index: float32 [64, 4, 64], P('wide', 'narrow'), may hold values from 1 to 20
- agg_map: int32 [256, 32, 128], P('wide', 'narrow'), may hold values from 0 to 31
- tile_factors: bfloat16 [384, 48, 128, 128], P('wide', 'narrow')
- coarse_inverse: float32 [8192, 8192], P(('wide', 'narrow')), as said below
Outputs:
- iterate: float32 [3, 256, 32, 128], P(None, 'wide', 'narrow')
- residual: float32 [3, 256, 32, 128], P(None, 'wide', 'narrow')
The draws below stay inside these ranges and needn't reach their ends.
Inputs may be any that keep to these rules, and one draw needn't show every extreme that they name: well_cells names, for each device's 64 connections, one of that device's own 4 * 8 * 128 cells, counted by pair, then column, then position in the tile; connections may share a cell. agg_map names one of the 32 aggregates of the device that owns the cell. coarse_inverse is symmetric.
All inputs are finite; a program needn't handle non-finite values.
Results may differ from the reference program's by a relative error of at most 0.00095.
Values sent between devices are 32-bit elements; how exact they have to be, the bound alone decides.
No kernel may reach another device: no remote copies, remote signals or barrier semaphores. Data moves between devices by JAX's collectives and lax.ppermute only.
A program may use at most 64 MiB of HBM per device.

```python
import math
import jax
import jax.numpy as jnp
from jax import lax

PHASES = 3
PX = 4
CY = 8
AGG_LOC = 32
CONN = 64
SWEEPS = 3
INNER = 3
TILE = 128
NX2 = 256
NY = 32
TX_ALL = 384
TY_ALL = 48
NAGG = 8192
N_WIDE = 64
N_NARROW = 4


def draw_tile_factors(key, part):
    full_shape = (TX_ALL, TY_ALL, TILE, TILE)
    deviation = 0.02 * jax.random.normal(key, full_shape, jnp.float32)
    return (jnp.eye(TILE, dtype=jnp.float32) + deviation).astype(jnp.bfloat16)


def draw_coarse_inverse(key, part):
    subkeys = jax.random.split(jax.random.fold_in(key, 7), 4)
    owners = NAGG // AGG_LOC
    shuffle = jax.random.permutation(subkeys[0], owners)
    position = jnp.argsort(shuffle)
    partner = shuffle[position ^ 1]
    device_of = jnp.arange(NAGG) // AGG_LOC
    paired = partner[device_of][:, None] == device_of[None, :]
    background = jax.random.normal(subkeys[1], (NAGG, NAGG), jnp.float32)
    partner_part = jax.random.normal(subkeys[2], (NAGG, NAGG), jnp.float32)
    diag_scale = jax.random.uniform(subkeys[3], (NAGG,), jnp.float32, 0.0005, 0.0015)
    back_scale = 5e-06
    sym_back = (background + background.T) * (back_scale / math.sqrt(2.0))
    sym_partner = (partner_part + partner_part.T) * (0.0004 / math.sqrt(2.0))
    return jnp.diag(diag_scale) + sym_back + jnp.where(paired, sym_partner, 0.0)


def set_ends(values, rng, smallest, high):
    longest = values.shape.index(max(values.shape))
    spots = []
    for shift in (0, 1):
        where = [jax.random.randint(jax.random.fold_in(rng, axis), (), 0, length) for axis, length in enumerate(values.shape)]
        where[longest] = (where[longest] + shift) % values.shape[longest]
        spots.append(tuple(where))
    return values.at[spots[0]].set(smallest).at[spots[1]].set(high)


def level_of(rng, shape, shards, least, largest):
    factor_of, own = 1.0, jax.random.fold_in(rng, 6)
    for dim, parts in shards:
        draws = jnp.exp(jax.random.uniform(jax.random.fold_in(own, dim), (parts,), jnp.float32, least / len(shards), largest / len(shards)))
        factor_of = factor_of * jnp.repeat(draws, shape[dim] // parts).reshape([-1 if axis == dim else 1 for axis in range(len(shape))])
    return factor_of


def normal_values(own_key, extent, width, limit, pieces=(), kind=jnp.bfloat16):
    entries = width * jax.random.normal(own_key, extent, jnp.float32)
    if pieces:
        entries = entries * level_of(own_key, extent, pieces, -0.22, 0.18)
    return jnp.clip(entries, -limit, limit).astype(kind)


def setup_inputs(seed: int = 0) -> dict:
    key_of = jax.random.split(jax.random.key(seed), 11)
    rhs = normal_values(key_of[0], (PHASES, NX2, NY, TILE), 2.0, 12.0, ((1, 64), (2, 4)), jnp.float32)
    start = normal_values(key_of[1], (PHASES, NX2, NY, TILE), 0.3, 2.0, ((1, 64), (2, 4)), jnp.float32)
    trans = jnp.clip(jnp.exp(math.log(2.0) - 2.3025851 * jax.random.uniform(key_of[2], (3, NX2, NY, TILE), jnp.float32) ** level_of(key_of[2], (3, NX2, NY, TILE), ((1, 64), (2, 4)), -0.2, 0.2)), 0.2, 2.0)
    accum = jnp.clip(jnp.exp(math.log(8.0) - 1.3862944 * jax.random.uniform(key_of[3], (NX2, NY, TILE), jnp.float32) ** level_of(key_of[3], (NX2, NY, TILE), ((0, 64), (1, 4)), -0.2, 0.2)), 2.0, 8.0)
    coupling = jnp.clip(jax.random.uniform(key_of[4], (PHASES, PHASES, NX2, NY, TILE), jnp.float32, -0.3, 0.3) * level_of(key_of[4], (PHASES, PHASES, NX2, NY, TILE), ((2, 64), (3, 4)), -0.4, 0.0), -0.3, 0.3)
    well_cells = set_ends(jax.random.randint(key_of[5], (N_WIDE, N_NARROW, CONN), 0, PX * CY * TILE), jax.random.fold_in(key_of[5], 1), 0, (PX * CY * TILE) - 1).astype(jnp.int32)
    well_index = jnp.clip(jnp.exp(math.log(20.0) - 2.9957323 * jax.random.uniform(key_of[6], (N_WIDE, N_NARROW, CONN), jnp.float32) ** level_of(key_of[6], (N_WIDE, N_NARROW, CONN), ((0, 64), (1, 4)), -0.2, 0.2)), 1.0, 20.0)
    agg_map = set_ends(jax.random.randint(key_of[7], (NX2, NY, TILE), 0, AGG_LOC), jax.random.fold_in(key_of[7], 1), 0, AGG_LOC - 1).astype(jnp.int32)
    tile_factors = draw_tile_factors(jax.random.fold_in(key_of[10], 71), 0)
    coarse_inverse = draw_coarse_inverse(jax.random.fold_in(key_of[10], 71), 0)
    return {"rhs": rhs, "start": start, "trans": trans, "accum": accum, "coupling": coupling, "well_cells": well_cells, "well_index": well_index, "agg_map": agg_map, "tile_factors": tile_factors, "coarse_inverse": coarse_inverse}


best_precision = lax.Precision.HIGHEST


def neighbour(values, along, offset, periodic):
    along = along % values.ndim
    if periodic:
        return jnp.roll(values, -offset, axis=along)
    length = values.shape[along]
    padding = [(0, 0)] * values.ndim
    if offset > 0:
        padding[along] = (0, offset)
        return lax.slice_in_dim(jnp.pad(values, padding), offset, offset + length, axis=along)
    padding[along] = (-offset, 0)
    return lax.slice_in_dim(jnp.pad(values, padding), 0, length, axis=along)


def east_of(values, periodic):
    middle = values.shape[-1] // 2
    from_next = neighbour(values, -3, 1, periodic)[..., :middle]
    return jnp.concatenate([values[..., middle:], from_next], axis=-1)


def west_of(values, periodic):
    middle = values.shape[-1] // 2
    from_prev = neighbour(values, -3, -1, periodic)[..., middle:]
    return jnp.concatenate([from_prev, values[..., :middle]], axis=-1)


def prepare(trans, accum_w, periodic):
    middle = trans.shape[-1] // 2
    layer_no = lax.broadcasted_iota(jnp.int32, accum_w.shape, accum_w.ndim - 1) % middle
    trans_x = trans[0]
    trans_y = trans[1]
    trans_z = jnp.where(layer_no < middle - 1, trans[2], 0.0)
    face_sum = trans_x + west_of(trans_x, periodic) + trans_y + neighbour(trans_y, -2, -1, periodic)
    face_sum = face_sum + trans_z + neighbour(trans_z, -1, -1, False)
    return trans_x, trans_y, trans_z, accum_w + face_sum


def operate(values, trans_x, trans_y, trans_z, centre, coupling, periodic):
    mixing = jnp.sum(coupling * values[None], axis=1)
    inflow = trans_x * east_of(values, periodic) + west_of(trans_x, periodic) * west_of(values, periodic)
    inflow = inflow + trans_y * neighbour(values, -2, 1, periodic)
    inflow = inflow + neighbour(trans_y, -2, -1, periodic) * neighbour(values, -2, -1, periodic)
    inflow = inflow + trans_z * neighbour(values, -1, 1, False)
    inflow = inflow + neighbour(trans_z, -1, -1, False) * neighbour(values, -1, -1, False)
    return centre * values + mixing - inflow


def tile_apply(values, inverse_diag, factors):
    scaled = (inverse_diag * values).astype(jnp.bfloat16)
    return jnp.einsum("cpyj,pykj->cpyk", scaled.astype(jnp.float32), factors.astype(jnp.float32), precision=best_precision)


def local_solve(misfit, coeffs, inverse_diag, factors):
    trans_x, trans_y, trans_z, centre, coupling = coeffs
    update = tile_apply(misfit, inverse_diag, factors)
    for _ in range(INNER - 1):
        applied = operate(update, trans_x, trans_y, trans_z, centre, coupling, False)
        update = update + tile_apply(misfit - applied, inverse_diag, factors)
    return update


def wrap_pad(values):
    widths = ((1, 1), (2, 2), (0, 0))
    return jnp.pad(values, ((0, 0),) * (values.ndim - 3) + widths, mode="wrap")


def subdomains(misfit_pad, padded, tile_factors):
    def one_device(device_no):
        wide_pos = (device_no // N_NARROW).astype(jnp.int32)
        narrow_pos = (device_no % N_NARROW).astype(jnp.int32)
        zero = jnp.zeros((), jnp.int32)

        def window(values):
            cut_x = lax.dynamic_slice_in_dim(values, (wide_pos * PX).astype(jnp.int32), PX + 2, values.ndim - 3)
            return lax.dynamic_slice_in_dim(cut_x, (narrow_pos * CY).astype(jnp.int32), CY + 4, values.ndim - 2)

        coeffs = [window(member) for member in padded[:5]]
        starts = ((wide_pos * (PX + 2)).astype(jnp.int32), (narrow_pos * (CY + 4)).astype(jnp.int32), zero, zero)
        factors = lax.dynamic_slice(tile_factors, starts, (PX + 2, CY + 4, TILE, TILE))
        update = local_solve(window(misfit_pad), coeffs, window(padded[5]), factors)
        return update[:, 1:-1, 2:-2, :]

    blocks = lax.map(one_device, jnp.arange(N_WIDE * N_NARROW, dtype=jnp.int32))
    blocks = blocks.reshape(N_WIDE, N_NARROW, PHASES, PX, CY, TILE)
    return blocks.transpose(2, 0, 3, 1, 4, 5).reshape(PHASES, N_WIDE * PX, N_NARROW * CY, TILE)


def reference(rhs, start, trans, accum, coupling, well_cells, well_index, agg_map, tile_factors, coarse_inverse):
    flat_local = well_cells.astype(jnp.int32)
    pair_pos = jnp.arange(N_WIDE, dtype=jnp.int32)[:, None, None] * PX + flat_local // (CY * TILE)
    row_pos = jnp.arange(N_NARROW, dtype=jnp.int32)[None, :, None] * CY + (flat_local // TILE) % CY
    cell_pos = flat_local % TILE
    accum_w = accum.at[pair_pos, row_pos, cell_pos].add(well_index)
    trans_x, trans_y, trans_z, centre = prepare(trans, accum_w, True)
    coupling_diag = jnp.stack([coupling[member, member] for member in range(PHASES)])
    inverse_diag = 1.0 / (centre[None] + coupling_diag)
    padded = [wrap_pad(member) for member in (trans_x, trans_y, trans_z, centre, coupling, inverse_diag)]
    owner_no = (lax.broadcasted_iota(jnp.int32, accum.shape, 0) // PX) * N_NARROW
    owner_no = owner_no + lax.broadcasted_iota(jnp.int32, accum.shape, 1) // CY
    group_ids = (owner_no * AGG_LOC + agg_map.astype(jnp.int32)).reshape(-1)
    current = start
    for _ in range(SWEEPS):
        misfit = rhs - operate(current, trans_x, trans_y, trans_z, centre, coupling, True)
        correction = subdomains(wrap_pad(misfit), padded, tile_factors)
        coarse_rhs = jax.ops.segment_sum(misfit[0].reshape(-1), group_ids, num_segments=NAGG)
        coarse_sol = jnp.dot(coarse_inverse, coarse_rhs, precision=best_precision)
        correction = correction.at[0].add(coarse_sol[group_ids].reshape(accum.shape))
        current = current + correction
    final_misfit = rhs - operate(current, trans_x, trans_y, trans_z, centre, coupling, True)
    return current, final_misfit
```

```python
import jax
import jax.numpy as jnp
from jax import lax
from jax.sharding import PartitionSpec as P

AGG_LOC = 32
SWEEPS = 3
INNER = 3


best_precision = lax.Precision.HIGHEST


def padded(cells, sides, width):
    for axis, dim in sides:
        count = lax.axis_size(axis)
        head = lax.slice_in_dim(cells, 0, width, axis=dim)
        tail = lax.slice_in_dim(cells, cells.shape[dim] - width, cells.shape[dim], axis=dim)
        cells = jnp.concatenate(
            [
                lax.ppermute(tail, axis, [(i, (i + 1) % count) for i in range(count)]),
                cells,
                lax.ppermute(head, axis, [((i + 1) % count, i) for i in range(count)]),
            ],
            axis=dim,
        )
    return cells


def neighbour(values, along, offset):
    along = along % values.ndim
    length = values.shape[along]
    padding = [(0, 0)] * values.ndim
    if offset > 0:
        padding[along] = (0, offset)
        return lax.slice_in_dim(jnp.pad(values, padding), offset, offset + length, axis=along)
    padding[along] = (-offset, 0)
    return lax.slice_in_dim(jnp.pad(values, padding), 0, length, axis=along)


def east_of(values):
    middle = values.shape[-1] // 2
    from_next = neighbour(values, -3, 1)[..., :middle]
    return jnp.concatenate([values[..., middle:], from_next], axis=-1)


def west_of(values):
    middle = values.shape[-1] // 2
    from_prev = neighbour(values, -3, -1)[..., middle:]
    return jnp.concatenate([from_prev, values[..., :middle]], axis=-1)


def prepare(trans, accum_w):
    middle = trans.shape[-1] // 2
    layer_no = lax.broadcasted_iota(jnp.int32, accum_w.shape, accum_w.ndim - 1) % middle
    trans_x = trans[0]
    trans_y = trans[1]
    trans_z = jnp.where(layer_no < middle - 1, trans[2], 0.0)
    face_sum = trans_x + west_of(trans_x) + trans_y + neighbour(trans_y, -2, -1)
    face_sum = face_sum + trans_z + neighbour(trans_z, -1, -1)
    return (trans_x, trans_y, trans_z, accum_w + face_sum)


def operate(values, trans_x, trans_y, trans_z, centre, coupling):
    mixing = jnp.sum(coupling * values[None], axis=1)
    inflow = trans_x * east_of(values) + west_of(trans_x) * west_of(values)
    inflow = inflow + trans_y * neighbour(values, -2, 1)
    inflow = inflow + neighbour(trans_y, -2, -1) * neighbour(values, -2, -1)
    inflow = inflow + trans_z * neighbour(values, -1, 1)
    inflow = inflow + neighbour(trans_z, -1, -1) * neighbour(values, -1, -1)
    return centre * values + mixing - inflow


def tile_apply(values, inverse_diag, factors):
    scaled = (inverse_diag * values).astype(jnp.bfloat16)
    return jnp.einsum("cpyj,pykj->cpyk", scaled, factors, preferred_element_type=jnp.float32)


def local_solve(misfit, coeffs, inverse_diag, factors):
    trans_x, trans_y, trans_z, centre, coupling = coeffs
    update = tile_apply(misfit, inverse_diag, factors)
    for _ in range(INNER - 1):
        applied = operate(update, trans_x, trans_y, trans_z, centre, coupling)
        update = update + tile_apply(misfit - applied, inverse_diag, factors)
    return update


def per_device(
    rhs,
    start,
    trans,
    accum,
    coupling,
    well_cells,
    well_index,
    agg_map,
    tile_factors,
    coarse_inverse,
):
    phases = rhs.shape[0]
    devices = lax.axis_size("wide") * lax.axis_size("narrow")
    accum_flat = accum.reshape(-1).at[well_cells.reshape(-1)].add(well_index.reshape(-1))
    accum_w = accum_flat.reshape(accum.shape)
    stacked = jnp.concatenate(
        [trans, accum_w[None], coupling.reshape((phases * phases,) + accum.shape)], axis=0
    )
    stacked = jnp.concatenate([stacked, rhs], axis=0)
    rim_wide = padded(stacked, (("wide", 1),), 2)
    rim_full = padded(rim_wide, (("narrow", 2),), 3)
    trans_x, trans_y, trans_z, centre = prepare(rim_full[0:3], rim_full[3])
    coupling_full = rim_full[4:13].reshape((phases, phases) + rim_full.shape[1:])
    full_set = (trans_x, trans_y, trans_z, centre, coupling_full)
    ext_set = tuple((member[..., 1:-1, 1:-1, :] for member in full_set))
    diag_part = jnp.stack([ext_set[4][member, member] for member in range(phases)])
    inverse_diag = 1.0 / (ext_set[3][None] + diag_part)

    def extended_fn(current):
        rim_x = padded(current, (("wide", 1),), 2)
        rim_xy = padded(rim_x, (("narrow", 2),), 3)
        applied = operate(rim_xy, full_set[0], full_set[1], full_set[2], full_set[3], full_set[4])
        extended = (rim_full[13:] - applied)[..., 1:-1, 1:-1, :]
        return (extended, extended[..., 1:-1, 2:-2, :])

    groups = jnp.arange(AGG_LOC, dtype=jnp.int32)
    member_of = (groups[:, None] == agg_map.reshape(1, -1)).astype(jnp.float32)
    current = start
    for _ in range(SWEEPS):
        extended, owned_misfit = extended_fn(current)
        coarse_rhs = jnp.dot(member_of, owned_misfit[0].reshape(-1), precision=best_precision)
        copies = jnp.broadcast_to(coarse_rhs, (devices, AGG_LOC))
        coarse_all = lax.all_to_all(copies, ("wide", "narrow"), 0, 0).reshape(-1)
        coarse_sol = jnp.dot(coarse_inverse, coarse_all, precision=best_precision)
        update = local_solve(extended, ext_set, inverse_diag, tile_factors)[..., 1:-1, 2:-2, :]
        lifted = jnp.dot(coarse_sol, member_of, precision=best_precision).reshape(accum.shape)
        current = current + update.at[0].add(lifted)
    final_misfit = extended_fn(current)[1]
    return (current, final_misfit)


def solution(mesh):
    return jax.shard_map(
        per_device,
        mesh=mesh,
        in_specs=(
            P(None, "wide", "narrow", None),
            P(None, "wide", "narrow", None),
            P(None, "wide", "narrow", None),
            P("wide", "narrow", None),
            P(None, None, "wide", "narrow", None),
            P("wide", "narrow", None),
            P("wide", "narrow", None),
            P("wide", "narrow", None),
            P("wide", "narrow", None, None),
            P(("wide", "narrow"), None),
        ),
        out_specs=(P(None, "wide", "narrow", None), P(None, "wide", "narrow", None)),
        check_vma=False,
    )
```

```python
import functools

import jax
import jax.numpy as jnp
from jax import lax
from jax.experimental import pallas as pl
from jax.experimental.pallas import tpu as pltpu
from jax.sharding import PartitionSpec as P

AGG_LOC = 32
SWEEPS = 3
PAIRS = 8
ROWS = 16
LANES = 128
FULL = 7
THIN = 13
WIDE_ROWS = FULL * 16 + THIN * 8
NARROW_ROWS = FULL * 24 + THIN * 12
TX, TXW, TY, TYS, TZ, TZM, CENTRE, COUP, INV, RHS = 0, 1, 2, 3, 4, 5, 6, 7, 16, 19
N_COEF = 22
VMEM_LIMIT = 24 * 1024 * 1024

f32 = jnp.float32


def swap_halves(v):
    return pltpu.roll(v, 64, axis=1)


def shifted(v, offset, axis):
    return pltpu.roll(v, (-offset) % v.shape[axis], axis=axis)


def lane_index(shape):
    return lax.broadcasted_iota(jnp.int32, shape, 1)


def box_mask():
    row = lax.broadcasted_iota(jnp.int32, (ROWS, LANES), 0)
    return (row < 10) | (row >= 14)


def operate_pair(values, coef, pair, rolled):
    low = lane_index((ROWS, LANES)) < 64
    mids = [values[c, pair] for c in range(3)]

    def halves(c, p):
        if (c, p) not in rolled:
            rolled[c, p] = swap_halves(values[c, p])
        return rolled[c, p]

    out = []
    for c in range(3):
        v = mids[c]
        own = halves(c, pair)
        inflow = coef[TX, pair - 1] * jnp.where(low, own, halves(c, pair + 1))
        inflow += coef[TXW, pair - 1] * jnp.where(low, halves(c, pair - 1), own)
        inflow += coef[TY, pair - 1] * shifted(v, 1, 0)
        inflow += coef[TYS, pair - 1] * shifted(v, -1, 0)
        inflow += coef[TZ, pair - 1] * shifted(v, 1, 1)
        inflow += coef[TZM, pair - 1] * shifted(v, -1, 1)
        total = coef[CENTRE, pair - 1] * v
        for b in range(3):
            total += coef[COUP + 3 * c + b, pair - 1] * mids[b]
        out.append(total - inflow)
    return out


def add_wells_and_pack(cells, index, accum, trans, start, agg, coupling, rhs, accum_w, east, west):
    where_row = (lax.broadcasted_iota(jnp.int32, (32, 64), 0) == cells[...] // LANES).astype(f32)
    lane_no = lax.broadcasted_iota(jnp.int32, (LANES, 64), 0)
    share = jnp.where(lane_no == cells[...] % LANES, index[...], 0.0)
    added = lax.dot_general(
        where_row, share, (((1,), (1,)), ((), ())), precision=lax.Precision.HIGHEST, preferred_element_type=f32
    )
    for p in range(4):
        accum_w[p] = accum[p] + added[8 * p : 8 * p + 8]
    for out, first, thin in ((east, 2, 3), (west, 0, 0)):
        for f in range(FULL):
            for p in range(2):
                if f < 3:
                    value = trans[f, first + p]
                elif f < 6:
                    value = start[f - 3, first + p]
                else:
                    value = agg[first + p].astype(f32)
                out[f * 16 + p * 8 : f * 16 + p * 8 + 8] = value
        for t in range(THIN):
            at = FULL * 16 + t * 8
            if t == 0:
                value = accum_w[thin]
            elif t < 10:
                value = coupling[(t - 1) // 3, (t - 1) % 3, thin]
            else:
                value = rhs[t - 10, thin]
            out[at : at + 8] = value


def pack_narrow(from_west, from_east, accum_w, trans, start, agg, coupling, rhs, north, south):
    def rows_of_full(f, a):
        if a < 2:
            return from_west[f * 16 + a * 8 : f * 16 + a * 8 + 8]
        if a >= 6:
            return from_east[f * 16 + (a - 6) * 8 : f * 16 + (a - 6) * 8 + 8]
        if f < 3:
            return trans[f, a - 2]
        if f < 6:
            return start[f - 3, a - 2]
        return agg[a - 2].astype(f32)

    def rows_of_thin(t, a):
        at = FULL * 16 + t * 8
        if a < 2:
            return from_west[at : at + 8]
        if a >= 6:
            return from_east[at : at + 8]
        if t == 0:
            return accum_w[a - 2]
        if t < 10:
            return coupling[(t - 1) // 3, (t - 1) % 3, a - 2]
        return rhs[t - 10, a - 2]

    for f in range(FULL):
        for a in range(8):
            v = rows_of_full(f, a)
            at = (f * 8 + a) * 3
            north[at : at + 3] = v[5:8]
            south[at : at + 3] = v[0:3]
    for t in range(THIN):
        for a in range(1, 7):
            v = rows_of_thin(t, a)
            at = FULL * 24 + (t * 6 + a - 1) * 2
            north[at : at + 2] = v[6:8]
            south[at : at + 2] = v[0:2]


def pack_current(current, from_west, from_east, north, south):
    for c in range(3):
        for a in range(8):
            v = from_west[c, a] if a < 2 else from_east[c, a - 6] if a >= 6 else current[c, a - 2]
            at = (c * 8 + a) * 3
            north[at : at + 3] = v[5:8]
            south[at : at + 3] = v[0:3]


def coarse_part(misfit0, agg, coarse, sums, spread, payload):
    for g in range(AGG_LOC):
        picked = jnp.where(agg[0] == g, misfit0[0], 0.0)
        for p in range(1, 4):
            picked += jnp.where(agg[p] == g, misfit0[p], 0.0)
        sums[g : g + 1, :] = jnp.sum(picked, axis=0, keepdims=True)
    weight = jnp.broadcast_to(jnp.sum(sums[...], axis=1, keepdims=True), (AGG_LOC, LANES))
    count = coarse.shape[1] // LANES
    for w in range(count):
        row = jnp.sum(coarse[:, w * LANES : (w + 1) * LANES] * weight, axis=0, keepdims=True)
        spread[1, w + 1 : w + 2, :] = row
    middle = spread[1, 1 : count + 1, :]
    for n in range(4):
        turned = middle if n == 1 else shifted(middle, 32 * (n - 1), 1)
        if n != 1:
            spread[n, 1 : count + 1, :] = turned
        spread[n, 0:1, :] = turned[count - 1 : count]
        spread[n, count + 1 : count + 2, :] = turned[0:1]
    for w in range(count):
        for n in range(4):
            payload[w * 4 + n] = spread[n, w : w + 3, :]


def misfit_part(values, coef, agg, coarse, misfit, payload, sums, spread):
    inside = box_mask()
    rolled = {}
    for c in range(3):
        misfit[c, 0] = jnp.zeros((ROWS, LANES), f32)
        misfit[c, 7] = jnp.zeros((ROWS, LANES), f32)
    for a in range(1, 7):
        applied = operate_pair(values, coef, a, rolled)
        for c in range(3):
            misfit[c, a] = jnp.where(inside, coef[RHS + c, a - 1] - applied[c], 0.0)
    coarse_part([misfit[0, a, 0:8] for a in range(2, 6)], agg, coarse, sums, spread, payload)


def first_misfit(
    from_west,
    from_east,
    from_south,
    from_north,
    accum_w,
    trans,
    start,
    agg,
    coupling,
    rhs,
    coarse,
    coef,
    slots,
    misfit,
    payload,
    rim,
    values,
    sums,
    spread,
):
    blank = jnp.zeros((ROWS, LANES), f32)

    def place(target, rows, at_north, at_south, width):
        target[...] = blank
        target[0:8] = rows
        target[8 : 8 + width] = from_north[at_north : at_north + width]
        target[16 - width : 16] = from_south[at_south : at_south + width]

    for f in range(FULL):
        for a in range(8):
            if a < 2:
                rows = from_west[f * 16 + a * 8 : f * 16 + a * 8 + 8]
            elif a >= 6:
                rows = from_east[f * 16 + (a - 6) * 8 : f * 16 + (a - 6) * 8 + 8]
            elif f < 3:
                rows = trans[f, a - 2]
            elif f < 6:
                rows = start[f - 3, a - 2]
            else:
                rows = agg[a - 2].astype(f32)
            at = (f * 8 + a) * 3
            target = values.at[f - 3, a] if 3 <= f < 6 else rim.at[f if f < 3 else 3, a]
            place(target, rows, at, at, 3)
    for t in range(THIN):
        for a in range(1, 7):
            at = FULL * 16 + t * 8
            if a < 2:
                rows = from_west[at : at + 8]
            elif a >= 6:
                rows = from_east[at : at + 8]
            elif t == 0:
                rows = accum_w[a - 2]
            elif t < 10:
                rows = coupling[(t - 1) // 3, (t - 1) % 3, a - 2]
            else:
                rows = rhs[t - 10, a - 2]
            at = FULL * 24 + (t * 6 + a - 1) * 2
            target = coef.at[CENTRE if t == 0 else COUP + t - 1 if t < 10 else RHS + t - 10, a - 1]
            place(target, rows, at, at, 2)
    row = lax.broadcasted_iota(jnp.int32, (ROWS, LANES), 0)
    lane = lane_index((ROWS, LANES))
    low = lane < 64
    offset = jnp.where(row < 8, 32, jnp.where(row < 12, 64, 0))
    inside = box_mask()
    for a in range(8):
        slots[a] = rim[3, a].astype(jnp.int32) + offset
    for a in range(1, 7):
        tx, ty = rim[0, a], rim[1, a]
        tz = jnp.where((lane % 64) < 63, rim[2, a], 0.0)
        txw = jnp.where(low, swap_halves(rim[0, a - 1]), swap_halves(tx))
        tys = shifted(ty, -1, 0)
        tzm = shifted(tz, -1, 1)
        centre = coef[CENTRE, a - 1] + (tx + txw + ty + tys + tz + tzm)
        coef[TX, a - 1] = tx
        coef[TXW, a - 1] = txw
        coef[TY, a - 1] = ty
        coef[TYS, a - 1] = tys
        coef[TZ, a - 1] = tz
        coef[TZM, a - 1] = tzm
        coef[CENTRE, a - 1] = centre
        for c in range(3):
            diagonal = jnp.where(inside, centre + coef[COUP + 4 * c, a - 1], 1.0)
            coef[INV + c, a - 1] = jnp.where(inside, 1.0 / diagonal, 0.0)
    misfit_part(values, coef, agg, coarse, misfit, payload, sums, spread)


def gather_values(current, from_west, from_east, from_south, from_north, received, slots, values):
    total = jnp.sum(received[...], axis=0)
    blank = jnp.zeros((2, LANES), f32)
    for a in range(8):
        block = 0 if a < 2 else 2 if a >= 6 else 1
        table = jnp.broadcast_to(total[block : block + 1], (8, LANES))
        for c in range(3):
            rows = from_west[c, a] if a < 2 else from_east[c, a - 6] if a >= 6 else current[c, a - 2]
            at = (c * 8 + a) * 3
            values[c, a, 0:8] = rows
            values[c, a, 8:11] = from_north[at : at + 3]
            values[c, a, 11:13] = blank
            values[c, a, 13:16] = from_south[at : at + 3]
        for half in range(2):
            where = slots[a, 8 * half : 8 * half + 8]
            lifted = jnp.take_along_axis(table, where, axis=1, mode="promise_in_bounds")
            values[0, a, 8 * half : 8 * half + 8] += lifted


def next_misfit(
    current,
    from_west,
    from_east,
    from_south,
    from_north,
    received,
    slots,
    coef,
    agg,
    coarse,
    moved,
    misfit,
    payload,
    values,
    sums,
    spread,
):
    gather_values(current, from_west, from_east, from_south, from_north, received, slots, values)
    for c in range(3):
        for p in range(4):
            moved[c, p] = values[c, p + 2, 0:8]
    misfit_part(values, coef, agg, coarse, misfit, payload, sums, spread)


def last_misfit(
    current, from_west, from_east, from_south, from_north, received, slots, coef, iterate, residual, values
):
    gather_values(current, from_west, from_east, from_south, from_north, received, slots, values)
    rolled = {}
    for a in range(2, 6):
        applied = operate_pair(values, coef, a, rolled)
        for c in range(3):
            iterate[c, a - 2] = values[c, a, 0:8]
            residual[c, a - 2] = (coef[RHS + c, a - 1] - applied[c])[0:8]


def local_solve(misfit, coef, current, factors, moved, one, two):
    own_cols = list(range(8))
    row8 = lax.broadcasted_iota(jnp.int32, (24, LANES), 0) % 8

    def tiles(values, pair, cols, half):
        scaled = [coef[INV + c, pair - 1, 8 * half : 8 * half + 8] * values[c] for c in range(3)]
        left = jnp.concatenate(scaled, axis=0).astype(jnp.bfloat16)
        total = jnp.zeros((24, LANES), f32)
        for y in cols:
            product = lax.dot_general(
                left, factors[pair - 1, y + 2], (((1,), (1,)), ((), ())), preferred_element_type=f32
            )
            total = jnp.where(row8 == y % 8, product, total)
        return [total[8 * c : 8 * c + 8] for c in range(3)]

    blank = jnp.zeros((ROWS, LANES), f32)
    for c in range(3):
        for ref in (one, two):
            ref[c, 0] = blank
            ref[c, 7] = blank
    for a in range(1, 7):
        edge = a in (1, 6)
        for half, cols in ((0, own_cols), (1, [8, -1] if edge else [8, 9, -2, -1])):
            part = tiles([misfit[c, a, 8 * half : 8 * half + 8] for c in range(3)], a, cols, half)
            for c in range(3):
                one[c, a, 8 * half : 8 * half + 8] = part[c]
    rolled = {}
    for a in range(1, 7):
        edge = a in (1, 6)
        applied = operate_pair(one, coef, a, rolled)
        left = [misfit[c, a] - applied[c] for c in range(3)]
        for half, cols in ((0, own_cols), (1, [] if edge else [8, -1])):
            if not cols:
                for c in range(3):
                    two[c, a, 8:16] = one[c, a, 8:16]
                continue
            part = tiles([v[8 * half : 8 * half + 8] for v in left], a, cols, half)
            for c in range(3):
                two[c, a, 8 * half : 8 * half + 8] = one[c, a, 8 * half : 8 * half + 8] + part[c]
    rolled = {}
    for a in range(2, 6):
        applied = operate_pair(two, coef, a, rolled)
        part = tiles([(misfit[c, a] - applied[c])[0:8] for c in range(3)], a, own_cols, 0)
        for c in range(3):
            moved[c, a - 2] = current[c, a - 2] + (two[c, a, 0:8] + part[c])


def call(body, name, outs, scratch, *operands, flops=1000000):
    vmem = pl.BlockSpec(memory_space=pltpu.VMEM)
    return pl.pallas_call(
        body,
        out_shape=[jax.ShapeDtypeStruct(shape, dtype) for shape, dtype in outs],
        in_specs=[vmem] * len(operands),
        out_specs=[vmem] * len(outs),
        scratch_shapes=[pltpu.VMEM(shape, f32) for shape in scratch],
        compiler_params=pltpu.CompilerParams(vmem_limit_bytes=VMEM_LIMIT),
        cost_estimate=pl.CostEstimate(flops=flops, bytes_accessed=0, transcendentals=0),
        name=name,
    )(*operands)


def both_ways(axis, up, down):
    count = lax.axis_size(axis)
    from_previous = lax.ppermute(up, axis, [(i, (i + 1) % count) for i in range(count)])
    from_next = lax.ppermute(down, axis, [((i + 1) % count, i) for i in range(count)])
    return from_previous, from_next


def per_device(
    rhs, start, trans, accum, coupling, well_cells, well_index, agg_map, tile_factors, coarse_inverse
):
    devices = lax.axis_size("wide") * lax.axis_size("narrow")
    spread = ((4, devices // 4 + 8, LANES), (AGG_LOC, LANES))
    own = ((3, 4, 8, LANES), f32)
    box = ((3, PAIRS, ROWS, LANES), f32)
    payload_type = ((devices, 3, LANES), f32)
    narrow_type = ((72, LANES), f32)

    accum_w, east, west = call(
        add_wells_and_pack,
        "pack_wide",
        [((4, 8, LANES), f32), ((WIDE_ROWS, LANES), f32), ((WIDE_ROWS, LANES), f32)],
        [],
        well_cells.reshape(1, -1),
        well_index.reshape(1, -1),
        accum,
        trans,
        start,
        agg_map,
        coupling,
        rhs,
    )
    from_west, from_east = both_ways("wide", east, west)
    mine = (accum_w, trans, start, agg_map, coupling, rhs)
    north, south = call(
        pack_narrow,
        "pack_narrow",
        [((NARROW_ROWS, LANES), f32)] * 2,
        [],
        from_west,
        from_east,
        *mine,
    )
    from_south, from_north = both_ways("narrow", north, south)
    coef, slots, misfit, payload = call(
        first_misfit,
        "first_misfit",
        [((N_COEF, 6, ROWS, LANES), f32), ((PAIRS, ROWS, LANES), jnp.int32), box, payload_type],
        [(4, PAIRS, ROWS, LANES), (3, PAIRS, ROWS, LANES), spread[1], spread[0]],
        from_west,
        from_east,
        from_south,
        from_north,
        *mine,
        coarse_inverse,
    )
    current = start
    for sweep in range(SWEEPS):
        received = lax.all_to_all(payload, ("wide", "narrow"), 0, 0)
        (current,) = call(
            local_solve, "local_solve", [own], [box[0], box[0]], misfit, coef, current, tile_factors, flops=30000000
        )
        from_west, from_east = both_ways("wide", current[:, 2:4], current[:, 0:2])
        north, south = call(
            pack_current, "pack_current", [narrow_type] * 2, [], current, from_west, from_east
        )
        from_south, from_north = both_ways("narrow", north, south)
        known = (current, from_west, from_east, from_south, from_north, received, slots, coef)
        if sweep < SWEEPS - 1:
            current, misfit, payload = call(
                next_misfit,
                "next_misfit",
                [own, box, payload_type],
                [box[0], spread[1], spread[0]],
                *known,
                agg_map,
                coarse_inverse,
            )
        else:
            iterate, residual = call(last_misfit, "last_misfit", [own, own], [box[0]], *known)
    return iterate, residual


def solution(mesh):
    return jax.shard_map(
        per_device,
        mesh=mesh,
        in_specs=(
            P(None, "wide", "narrow", None),
            P(None, "wide", "narrow", None),
            P(None, "wide", "narrow", None),
            P("wide", "narrow", None),
            P(None, None, "wide", "narrow", None),
            P("wide", "narrow", None),
            P("wide", "narrow", None),
            P("wide", "narrow", None),
            P("wide", "narrow", None, None),
            P(("wide", "narrow"), None),
        ),
        out_specs=(P(None, "wide", "narrow", None), P(None, "wide", "narrow", None)),
        check_vma=False,
    )
```

```python
import functools

import jax
import jax.numpy as jnp
from jax import lax
from jax.experimental import pallas as pl
from jax.experimental.pallas import tpu as pltpu
from jax.sharding import PartitionSpec as P

AGG_LOC = 32
SWEEPS = 3
PAIRS = 8
ROWS = 16
LANES = 128
FULL = 7
THIN = 13
WIDE_ROWS = FULL * 16 + THIN * 8
NARROW_ROWS = FULL * 24 + THIN * 12
TX, TXW, TY, TYS, TZ, TZM, CENTRE, COUP, INV, RHS = 0, 1, 2, 3, 4, 5, 6, 7, 16, 19
N_COEF = 22
VMEM_LIMIT = 24 * 1024 * 1024

f32 = jnp.float32


def swap_halves(v):
    return pltpu.roll(v, 64, axis=1)


def shifted(v, offset, axis):
    return pltpu.roll(v, (-offset) % v.shape[axis], axis=axis)


def lane_index(shape):
    return lax.broadcasted_iota(jnp.int32, shape, 1)


def box_mask():
    row = lax.broadcasted_iota(jnp.int32, (ROWS, LANES), 0)
    return (row < 10) | (row >= 14)


def operate_pair(values, coef, pair, rolled):
    low = lane_index((ROWS, LANES)) < 64
    mids = [values[c, pair] for c in range(3)]

    def halves(c, p):
        if (c, p) not in rolled:
            rolled[c, p] = swap_halves(values[c, p])
        return rolled[c, p]

    out = []
    for c in range(3):
        v = mids[c]
        own = halves(c, pair)
        inflow = coef[TX, pair - 1] * jnp.where(low, own, halves(c, pair + 1))
        inflow += coef[TXW, pair - 1] * jnp.where(low, halves(c, pair - 1), own)
        inflow += coef[TY, pair - 1] * shifted(v, 1, 0)
        inflow += coef[TYS, pair - 1] * shifted(v, -1, 0)
        inflow += coef[TZ, pair - 1] * shifted(v, 1, 1)
        inflow += coef[TZM, pair - 1] * shifted(v, -1, 1)
        total = coef[CENTRE, pair - 1] * v
        for b in range(3):
            total += coef[COUP + 3 * c + b, pair - 1] * mids[b]
        out.append(total - inflow)
    return out


def pick(odd, when_odd, when_even):
    return jnp.where(odd, when_odd, when_even)


def is_odd(axis):
    return lax.axis_index(axis) % 2 == 1


def add_wells_and_pack(
    cells_in,
    index_in,
    accum,
    trans,
    start,
    agg,
    coupling,
    rhs,
    mine,
    agg_float,
    far,
    near,
    cells,
    index,
    accum_in,
    agg_in,
    sems,
):
    sources = (
        (cells_in, cells),
        (index_in, index),
        (agg, agg_in),
        (accum, accum_in),
        (trans, mine.at[0:3]),
        (start, mine.at[3:6]),
        (coupling, mine.at[8:17]),
        (rhs, mine.at[17:20]),
    )
    copies = [pltpu.make_async_copy(source, target, sems.at[i]) for i, (source, target) in enumerate(sources)]
    for copy in copies:
        copy.start()
    for copy in copies[:2]:
        copy.wait()
    where_row = (lax.broadcasted_iota(jnp.int32, (32, 64), 0) == cells[...] // LANES).astype(f32)
    lane_no = lax.broadcasted_iota(jnp.int32, (LANES, 64), 0)
    share = jnp.where(lane_no == cells[...] % LANES, index[...], 0.0)
    added = lax.dot_general(
        where_row, share, (((1,), (1,)), ((), ())), precision=lax.Precision.HIGHEST, preferred_element_type=f32
    )
    for copy in copies[2:]:
        copy.wait()
    for p in range(4):
        mine[7, p] = accum_in[p] + added[8 * p : 8 * p + 8]
        mine[6, p] = agg_in[p].astype(f32)
        agg_float[p] = agg_in[p].astype(f32)
    odd = is_odd("wide")
    for f in range(FULL):
        for p in range(2):
            east, west = mine[f, 2 + p], mine[f, p]
            at = f * 16 + p * 8
            far[at : at + 8] = pick(odd, east, west)
            near[at : at + 8] = pick(odd, west, east)
    for t in range(THIN):
        east, west = mine[FULL + t, 3], mine[FULL + t, 0]
        at = FULL * 16 + t * 8
        far[at : at + 8] = pick(odd, east, west)
        near[at : at + 8] = pick(odd, west, east)


def rim_rows(odd, far, near, mine, channel_no, at, depth, pair):
    if pair < 2:
        at += 8 * pair if depth == 2 else 0
        return pick(odd, near[at : at + 8], far[at : at + 8])
    if pair >= 6:
        at += 8 * (pair - 6) if depth == 2 else 0
        return pick(odd, far[at : at + 8], near[at : at + 8])
    return mine[channel_no, pair - 2]


def pack_narrow(far, near, mine, low, high):
    odd = is_odd("wide")
    narrow_odd = is_odd("narrow")
    for f in range(FULL):
        for a in range(8):
            v = rim_rows(odd, far, near, mine, f, f * 16, 2, a)
            at = (f * 8 + a) * 3
            low[at : at + 3] = pick(narrow_odd, v[5:8], v[0:3])
            high[at : at + 3] = pick(narrow_odd, v[0:3], v[5:8])
    for t in range(THIN):
        for a in range(1, 7):
            v = rim_rows(odd, far, near, mine, FULL + t, FULL * 16 + t * 8, 1, a)
            at = FULL * 24 + (t * 6 + a - 1) * 2
            low[at : at + 2] = pick(narrow_odd, v[6:8], v[0:2])
            high[at : at + 2] = pick(narrow_odd, v[0:2], v[6:8])


def pack_current(current, far, near, low, high):
    odd = is_odd("wide")
    narrow_odd = is_odd("narrow")
    for c in range(3):
        for a in range(8):
            v = rim_rows(odd, far, near, current, c, c * 16, 2, a)
            at = (c * 8 + a) * 3
            low[at : at + 3] = pick(narrow_odd, v[5:8], v[0:3])
            high[at : at + 3] = pick(narrow_odd, v[0:3], v[5:8])


def coarse_part(misfit0, agg, coarse, fetch, sums, spread, payload):
    for g in range(AGG_LOC):
        picked = jnp.where(agg[0] == float(g), misfit0[0], 0.0)
        for p in range(1, 4):
            picked += jnp.where(agg[p] == float(g), misfit0[p], 0.0)
        sums[g : g + 1, :] = jnp.sum(picked, axis=0, keepdims=True)
    weight = jnp.broadcast_to(jnp.sum(sums[...], axis=1, keepdims=True), (AGG_LOC, LANES))
    count = coarse.shape[1] // LANES
    fetch.wait()
    for w in range(count):
        row = jnp.sum(coarse[:, w * LANES : (w + 1) * LANES] * weight, axis=0, keepdims=True)
        spread[1, w + 1 : w + 2, :] = row
    middle = spread[1, 1 : count + 1, :]
    for n in range(4):
        turned = middle if n == 1 else shifted(middle, 32 * (n - 1), 1)
        if n != 1:
            spread[n, 1 : count + 1, :] = turned
        spread[n, 0:1, :] = turned[count - 1 : count]
        spread[n, count + 1 : count + 2, :] = turned[0:1]
    for w in range(count):
        for n in range(4):
            payload[w * 4 + n] = spread[n, w : w + 3, :]


def misfit_part(values, coef, agg, coarse, fetch, misfit, payload, sums, spread):
    inside = box_mask()
    rolled = {}
    for c in range(3):
        misfit[c, 0] = jnp.zeros((ROWS, LANES), f32)
        misfit[c, 7] = jnp.zeros((ROWS, LANES), f32)
    for a in range(1, 7):
        applied = operate_pair(values, coef, a, rolled)
        for c in range(3):
            misfit[c, a] = jnp.where(inside, coef[RHS + c, a - 1] - applied[c], 0.0)
    coarse_part([misfit[0, a, 0:8] for a in range(2, 6)], agg, coarse, fetch, sums, spread, payload)


def first_misfit(
    far,
    near,
    low,
    high,
    mine,
    agg,
    coarse_hbm,
    coef,
    slots,
    misfit,
    payload,
    rim,
    values,
    sums,
    spread,
    coarse,
    sem,
):
    fetch = pltpu.make_async_copy(coarse_hbm, coarse, sem)
    fetch.start()
    odd = is_odd("wide")
    narrow_odd = is_odd("narrow")
    blank = jnp.zeros((ROWS, LANES), f32)

    def place(target, rows, at, width):
        target[...] = blank
        target[0:8] = rows
        a, b = low[at : at + width], high[at : at + width]
        target[8 : 8 + width] = pick(narrow_odd, a, b)
        target[16 - width : 16] = pick(narrow_odd, b, a)

    for f in range(FULL):
        for a in range(8):
            rows = rim_rows(odd, far, near, mine, f, f * 16, 2, a)
            target = values.at[f - 3, a] if 3 <= f < 6 else rim.at[f if f < 3 else 3, a]
            place(target, rows, (f * 8 + a) * 3, 3)
    for t in range(THIN):
        for a in range(1, 7):
            rows = rim_rows(odd, far, near, mine, FULL + t, FULL * 16 + t * 8, 1, a)
            target = coef.at[CENTRE if t == 0 else COUP + t - 1 if t < 10 else RHS + t - 10, a - 1]
            place(target, rows, FULL * 24 + (t * 6 + a - 1) * 2, 2)
    row = lax.broadcasted_iota(jnp.int32, (ROWS, LANES), 0)
    lane = lane_index((ROWS, LANES))
    low = lane < 64
    offset = jnp.where(row < 8, 32, jnp.where(row < 12, 64, 0))
    inside = box_mask()
    for a in range(8):
        slots[a] = rim[3, a].astype(jnp.int32) + offset
    for a in range(1, 7):
        tx, ty = rim[0, a], rim[1, a]
        tz = jnp.where((lane % 64) < 63, rim[2, a], 0.0)
        txw = jnp.where(low, swap_halves(rim[0, a - 1]), swap_halves(tx))
        tys = shifted(ty, -1, 0)
        tzm = shifted(tz, -1, 1)
        centre = coef[CENTRE, a - 1] + (tx + txw + ty + tys + tz + tzm)
        coef[TX, a - 1] = tx
        coef[TXW, a - 1] = txw
        coef[TY, a - 1] = ty
        coef[TYS, a - 1] = tys
        coef[TZ, a - 1] = tz
        coef[TZM, a - 1] = tzm
        coef[CENTRE, a - 1] = centre
        for c in range(3):
            diagonal = jnp.where(inside, centre + coef[COUP + 4 * c, a - 1], 1.0)
            coef[INV + c, a - 1] = jnp.where(inside, 1.0 / diagonal, 0.0)
    misfit_part(values, coef, agg, coarse, fetch, misfit, payload, sums, spread)


def gather_values(current, far, near, low, high, received, slots, values):
    odd = is_odd("wide")
    narrow_odd = is_odd("narrow")
    total = jnp.sum(received[...], axis=0)
    blank = jnp.zeros((2, LANES), f32)
    for a in range(8):
        block = 0 if a < 2 else 2 if a >= 6 else 1
        table = jnp.broadcast_to(total[block : block + 1], (8, LANES))
        for c in range(3):
            at = (c * 8 + a) * 3
            first, second = low[at : at + 3], high[at : at + 3]
            values[c, a, 0:8] = rim_rows(odd, far, near, current, c, c * 16, 2, a)
            values[c, a, 8:11] = pick(narrow_odd, first, second)
            values[c, a, 11:13] = blank
            values[c, a, 13:16] = pick(narrow_odd, second, first)
        for half in range(2):
            where = slots[a, 8 * half : 8 * half + 8]
            lifted = jnp.take_along_axis(table, where, axis=1, mode="promise_in_bounds")
            values[0, a, 8 * half : 8 * half + 8] += lifted


def next_misfit(
    current,
    far,
    near,
    low,
    high,
    received,
    slots,
    coef,
    agg,
    coarse_hbm,
    moved,
    misfit,
    payload,
    values,
    sums,
    spread,
    coarse,
    sem,
):
    fetch = pltpu.make_async_copy(coarse_hbm, coarse, sem)
    fetch.start()
    gather_values(current, far, near, low, high, received, slots, values)
    for c in range(3):
        for p in range(4):
            moved[c, p] = values[c, p + 2, 0:8]
    misfit_part(values, coef, agg, coarse, fetch, misfit, payload, sums, spread)


def last_misfit(current, far, near, low, high, received, slots, coef, iterate, residual, values):
    gather_values(current, far, near, low, high, received, slots, values)
    rolled = {}
    for a in range(2, 6):
        applied = operate_pair(values, coef, a, rolled)
        for c in range(3):
            iterate[c, a - 2] = values[c, a, 0:8]
            residual[c, a - 2] = (coef[RHS + c, a - 1] - applied[c])[0:8]


def local_solve(misfit, coef, current, factors_hbm, moved, far, near, one, two, factors, sems, first=0):
    fetches = [pltpu.make_async_copy(factors_hbm.at[a], factors.at[a], sems.at[a]) for a in range(6)]
    for fetch in fetches:
        fetch.start()
    own_cols = list(range(8))
    row8 = lax.broadcasted_iota(jnp.int32, (24, LANES), 0) % 8

    def tiles(values, pair, cols, half):
        scaled = [coef[INV + c, pair - 1, 8 * half : 8 * half + 8] * values[c] for c in range(3)]
        left = jnp.concatenate(scaled, axis=0).astype(jnp.bfloat16)
        total = jnp.zeros((24, LANES), f32)
        for y in cols:
            product = lax.dot_general(
                left, factors[pair - 1, y + 2], (((1,), (1,)), ((), ())), preferred_element_type=f32
            )
            total = jnp.where(row8 == y % 8, product, total)
        return [total[8 * c : 8 * c + 8] for c in range(3)]

    blank = jnp.zeros((ROWS, LANES), f32)
    for c in range(3):
        for ref in (one, two):
            ref[c, 0] = blank
            ref[c, 7] = blank
    for a in range(1, 7):
        edge = a in (1, 6)
        fetches[a - 1].wait()
        for half, cols in ((0, own_cols), (1, [8, -1] if edge else [8, 9, -2, -1])):
            part = tiles([misfit[c, a, 8 * half : 8 * half + 8] for c in range(3)], a, cols, half)
            for c in range(3):
                one[c, a, 8 * half : 8 * half + 8] = part[c]
    rolled = {}
    for a in range(1, 7):
        edge = a in (1, 6)
        applied = operate_pair(one, coef, a, rolled)
        left = [misfit[c, a] - applied[c] for c in range(3)]
        for half, cols in ((0, own_cols), (1, [] if edge else [8, -1])):
            if not cols:
                for c in range(3):
                    two[c, a, 8:16] = one[c, a, 8:16]
                continue
            part = tiles([v[8 * half : 8 * half + 8] for v in left], a, cols, half)
            for c in range(3):
                two[c, a, 8 * half : 8 * half + 8] = one[c, a, 8 * half : 8 * half + 8] + part[c]
    rolled = {}
    for a in range(2, 6):
        applied = operate_pair(two, coef, a, rolled)
        part = tiles([(misfit[c, a] - applied[c])[0:8] for c in range(3)], a, own_cols, 0)
        for c in range(3):
            moved[c, a - 2] = current[first + c, a - 2] + (two[c, a, 0:8] + part[c])
    odd = is_odd("wide")
    for c in range(3):
        for p in range(2):
            at = c * 16 + p * 8
            far[at : at + 8] = pick(odd, moved[c, 2 + p], moved[c, p])
            near[at : at + 8] = pick(odd, moved[c, p], moved[c, 2 + p])


def call(body, name, outs, scratch, operands, in_hbm=(), flops=1000000):
    vmem = pl.BlockSpec(memory_space=pltpu.VMEM)
    hbm = pl.BlockSpec(memory_space=pltpu.HBM)
    operands = [pltpu.with_memory_space_constraint(x, pltpu.HBM) if i in in_hbm else x for i, x in enumerate(operands)]
    return pl.pallas_call(
        body,
        out_shape=[jax.ShapeDtypeStruct(shape, dtype) for shape, dtype in outs],
        in_specs=[hbm if i in in_hbm else vmem for i in range(len(operands))],
        out_specs=[vmem] * len(outs),
        scratch_shapes=scratch,
        compiler_params=pltpu.CompilerParams(vmem_limit_bytes=VMEM_LIMIT),
        cost_estimate=pl.CostEstimate(flops=flops, bytes_accessed=0, transcendentals=0),
        name=name,
    )(*operands)


def swaps(axis, far, near):
    count = lax.axis_size(axis)
    with jax.named_scope(axis + "_far"):
        far = lax.ppermute(far, axis, [(i, (i + (1 if i % 2 else -1)) % count) for i in range(count)])
    with jax.named_scope(axis + "_near"):
        near = lax.ppermute(near, axis, [(i, i ^ 1) for i in range(count)])
    return far, near


def per_device(
    rhs, start, trans, accum, coupling, well_cells, well_index, agg_map, tile_factors, coarse_inverse
):
    devices = lax.axis_size("wide") * lax.axis_size("narrow")
    dma = pltpu.SemaphoreType.DMA
    own = ((3, 4, 8, LANES), f32)
    box = ((3, PAIRS, ROWS, LANES), f32)
    wide_type = ((48, LANES), f32)
    narrow_type = ((72, LANES), f32)
    payload_type = ((devices, 3, LANES), f32)
    coarse_scratch = [
        pltpu.VMEM(box[0], f32),
        pltpu.VMEM((AGG_LOC, LANES), f32),
        pltpu.VMEM((4, devices // 4 + 8, LANES), f32),
        pltpu.VMEM(coarse_inverse.shape, f32),
        dma,
    ]

    mine, agg, far, near = call(
        add_wells_and_pack,
        "pack_wide",
        [((FULL + THIN, 4, 8, LANES), f32), ((4, 8, LANES), f32)] + [((WIDE_ROWS, LANES), f32)] * 2,
        [
            pltpu.VMEM((1, 64), jnp.int32),
            pltpu.VMEM((1, 64), f32),
            pltpu.VMEM((4, 8, LANES), f32),
            pltpu.VMEM((4, 8, LANES), jnp.int32),
            dma((8,)),
        ],
        [
            well_cells.reshape(1, -1),
            well_index.reshape(1, -1),
            accum,
            trans,
            start,
            agg_map,
            coupling.reshape((9,) + accum.shape),
            rhs,
        ],
        in_hbm=range(8),
    )
    far, near = swaps("wide", far, near)
    low, high = call(pack_narrow, "pack_narrow", [((NARROW_ROWS, LANES), f32)] * 2, [], [far, near, mine])
    low, high = swaps("narrow", low, high)
    coef, slots, misfit, payload = call(
        first_misfit,
        "first_misfit",
        [((N_COEF, 6, ROWS, LANES), f32), ((PAIRS, ROWS, LANES), jnp.int32), box, payload_type],
        [pltpu.VMEM((4, PAIRS, ROWS, LANES), f32)] + coarse_scratch,
        [far, near, low, high, mine, agg, coarse_inverse],
        in_hbm=(6,),
    )
    current, first = mine, 3
    for sweep in range(SWEEPS):
        received = lax.all_to_all(payload, ("wide", "narrow"), 0, 0)
        current, far, near = call(
            functools.partial(local_solve, first=first),
            "local_solve",
            [own, wide_type, wide_type],
            [pltpu.VMEM(box[0], f32)] * 2 + [pltpu.VMEM(tile_factors.shape, tile_factors.dtype), dma((6,))],
            [misfit, coef, current, tile_factors],
            in_hbm=(3,),
            flops=30000000,
        )
        first = 0
        far, near = swaps("wide", far, near)
        low, high = call(pack_current, "pack_current", [narrow_type] * 2, [], [current, far, near])
        low, high = swaps("narrow", low, high)
        known = [current, far, near, low, high, received, slots, coef]
        if sweep < SWEEPS - 1:
            current, misfit, payload = call(
                next_misfit,
                "next_misfit",
                [own, box, payload_type],
                coarse_scratch,
                known + [agg, coarse_inverse],
                in_hbm=(9,),
            )
        else:
            iterate, residual = call(last_misfit, "last_misfit", [own, own], [pltpu.VMEM(box[0], f32)], known)
    return iterate, residual


def solution(mesh):
    return jax.shard_map(
        per_device,
        mesh=mesh,
        in_specs=(
            P(None, "wide", "narrow", None),
            P(None, "wide", "narrow", None),
            P(None, "wide", "narrow", None),
            P("wide", "narrow", None),
            P(None, None, "wide", "narrow", None),
            P("wide", "narrow", None),
            P("wide", "narrow", None),
            P("wide", "narrow", None),
            P("wide", "narrow", None, None),
            P(("wide", "narrow"), None),
        ),
        out_specs=(P(None, "wide", "narrow", None), P(None, "wide", "narrow", None)),
        check_vma=False,
    )
```

```python
import functools

import jax
import jax.numpy as jnp
from jax import lax
from jax.experimental import pallas as pl
from jax.experimental.pallas import tpu as pltpu
from jax.sharding import PartitionSpec as P

AGG_LOC = 32
SWEEPS = 3
PAIRS = 8
ROWS = 16
LANES = 128
FULL = 7
THIN = 13
WIDE_ROWS = FULL * 16 + THIN * 8
NARROW_ROWS = FULL * 24 + THIN * 12
TX, TXW, TY, TYS, TZ, TZM, CENTRE, COUP, INV, RHS = 0, 1, 2, 3, 4, 5, 6, 7, 16, 19
N_COEF = 22
VMEM_LIMIT = 24 * 1024 * 1024

f32 = jnp.float32


def swap_halves(v):
    return pltpu.roll(v, 64, axis=1)


def shifted(v, offset, axis):
    return pltpu.roll(v, (-offset) % v.shape[axis], axis=axis)


def lane_index(shape):
    return lax.broadcasted_iota(jnp.int32, shape, 1)


def box_mask():
    row = lax.broadcasted_iota(jnp.int32, (ROWS, LANES), 0)
    return (row < 10) | (row >= 14)


def operate_pair(values, coef, pair, rolled):
    low = lane_index((ROWS, LANES)) < 64
    mids = [values[c, pair] for c in range(3)]

    def halves(c, p):
        if (c, p) not in rolled:
            rolled[c, p] = swap_halves(values[c, p])
        return rolled[c, p]

    out = []
    for c in range(3):
        v = mids[c]
        own = halves(c, pair)
        inflow = coef[TX, pair - 1] * jnp.where(low, own, halves(c, pair + 1))
        inflow += coef[TXW, pair - 1] * jnp.where(low, halves(c, pair - 1), own)
        inflow += coef[TY, pair - 1] * shifted(v, 1, 0)
        inflow += coef[TYS, pair - 1] * shifted(v, -1, 0)
        inflow += coef[TZ, pair - 1] * shifted(v, 1, 1)
        inflow += coef[TZM, pair - 1] * shifted(v, -1, 1)
        total = coef[CENTRE, pair - 1] * v
        for b in range(3):
            total += coef[COUP + 3 * c + b, pair - 1] * mids[b]
        out.append(total - inflow)
    return out


def pick(odd, when_odd, when_even):
    return jnp.where(odd, when_odd, when_even)


def is_odd(axis):
    return lax.axis_index(axis) % 2 == 1


def add_wells_and_pack(
    cells_in,
    index_in,
    accum,
    trans,
    start,
    agg,
    coupling,
    rhs,
    mine,
    agg_float,
    far,
    near,
    cells,
    index,
    accum_in,
    agg_in,
    sems,
):
    sources = (
        (cells_in, cells),
        (index_in, index),
        (agg, agg_in),
        (accum, accum_in),
        (trans, mine.at[0:3]),
        (start, mine.at[3:6]),
        (coupling, mine.at[8:17]),
        (rhs, mine.at[17:20]),
    )
    copies = [pltpu.make_async_copy(source, target, sems.at[i]) for i, (source, target) in enumerate(sources)]
    for copy in copies:
        copy.start()
    for copy in copies[:2]:
        copy.wait()
    where_row = (lax.broadcasted_iota(jnp.int32, (32, 64), 0) == cells[...] // LANES).astype(f32)
    lane_no = lax.broadcasted_iota(jnp.int32, (LANES, 64), 0)
    share = jnp.where(lane_no == cells[...] % LANES, index[...], 0.0)
    added = lax.dot_general(
        where_row, share, (((1,), (1,)), ((), ())), precision=lax.Precision.HIGHEST, preferred_element_type=f32
    )
    for copy in copies[2:]:
        copy.wait()
    for p in range(4):
        mine[7, p] = accum_in[p] + added[8 * p : 8 * p + 8]
        mine[6, p] = agg_in[p].astype(f32)
        agg_float[p] = agg_in[p].astype(f32)
    odd = is_odd("wide")
    for f in range(FULL):
        for p in range(2):
            east, west = mine[f, 2 + p], mine[f, p]
            at = f * 16 + p * 8
            far[at : at + 8] = pick(odd, east, west)
            near[at : at + 8] = pick(odd, west, east)
    for t in range(THIN):
        east, west = mine[FULL + t, 3], mine[FULL + t, 0]
        at = FULL * 16 + t * 8
        far[at : at + 8] = pick(odd, east, west)
        near[at : at + 8] = pick(odd, west, east)


def rim_rows(odd, far, near, mine, channel_no, at, depth, pair):
    if pair < 2:
        at += 8 * pair if depth == 2 else 0
        return pick(odd, near[at : at + 8], far[at : at + 8])
    if pair >= 6:
        at += 8 * (pair - 6) if depth == 2 else 0
        return pick(odd, far[at : at + 8], near[at : at + 8])
    return mine[channel_no, pair - 2]


def pack_narrow(far, near, mine, low, high):
    odd = is_odd("wide")
    narrow_odd = is_odd("narrow")
    for f in range(FULL):
        for a in range(8):
            v = rim_rows(odd, far, near, mine, f, f * 16, 2, a)
            at = (f * 8 + a) * 3
            low[at : at + 3] = pick(narrow_odd, v[5:8], v[0:3])
            high[at : at + 3] = pick(narrow_odd, v[0:3], v[5:8])
    for t in range(THIN):
        for a in range(1, 7):
            v = rim_rows(odd, far, near, mine, FULL + t, FULL * 16 + t * 8, 1, a)
            at = FULL * 24 + (t * 6 + a - 1) * 2
            low[at : at + 2] = pick(narrow_odd, v[6:8], v[0:2])
            high[at : at + 2] = pick(narrow_odd, v[0:2], v[6:8])


def pack_current(current, far, near, low, high):
    odd = is_odd("wide")
    narrow_odd = is_odd("narrow")
    for c in range(3):
        for a in range(8):
            v = rim_rows(odd, far, near, current, c, c * 16, 2, a)
            at = (c * 8 + a) * 3
            low[at : at + 3] = pick(narrow_odd, v[5:8], v[0:3])
            high[at : at + 3] = pick(narrow_odd, v[0:3], v[5:8])


def coarse_part(misfit0, agg, coarse, sums, spread, staged):
    for g in range(AGG_LOC):
        picked = jnp.where(agg[0] == float(g), misfit0[0], 0.0)
        for p in range(1, 4):
            picked += jnp.where(agg[p] == float(g), misfit0[p], 0.0)
        sums[g : g + 1, :] = jnp.sum(picked, axis=0, keepdims=True)
    weight = jnp.broadcast_to(jnp.sum(sums[...], axis=1, keepdims=True), (AGG_LOC, LANES))
    count = coarse.shape[1] // LANES
    for w in range(count):
        row = jnp.sum(coarse[:, w * LANES : (w + 1) * LANES] * weight, axis=0, keepdims=True)
        spread[1, w + 1 : w + 2, :] = row
    middle = spread[1, 1 : count + 1, :]
    for n in range(4):
        turned = middle if n == 1 else shifted(middle, 32 * (n - 1), 1)
        if n != 1:
            spread[n, 1 : count + 1, :] = turned
        spread[n, 0:1, :] = turned[count - 1 : count]
        spread[n, count + 1 : count + 2, :] = turned[0:1]
    for w in range(count):
        for n in range(4):
            at = 3 * (4 * w + n)
            staged[at : at + 3, :] = spread[n, w : w + 3, :]


def solve_box(values, coef, agg, coarse, factors_hbm, payload, current, far, near, scratch):
    misfit, sums, spread, staged, one, two, factors, tile_sems, sem = scratch
    inside = box_mask()
    rolled = {}
    for c in range(3):
        misfit[c, 0] = jnp.zeros((ROWS, LANES), f32)
        misfit[c, 7] = jnp.zeros((ROWS, LANES), f32)
    for a in range(1, 7):
        applied = operate_pair(values, coef, a, rolled)
        for c in range(3):
            misfit[c, a] = jnp.where(inside, coef[RHS + c, a - 1] - applied[c], 0.0)
    coarse_part([misfit[0, a, 0:8] for a in range(2, 6)], agg, coarse, sums, spread, staged)
    write = pltpu.make_async_copy(staged, payload, sem)
    write.start()
    local_solve(misfit, coef, values, factors_hbm, factors, tile_sems, current, one, two)
    odd = is_odd("wide")
    for c in range(3):
        for p in range(2):
            at = c * 16 + p * 8
            far[at : at + 8] = pick(odd, current[c, 2 + p], current[c, p])
            near[at : at + 8] = pick(odd, current[c, p], current[c, 2 + p])
    write.wait()


def fetch_tiles(factors_hbm, factors, sems):
    return [pltpu.make_async_copy(factors_hbm.at[a], factors.at[a], sems.at[a]) for a in range(6)]


def first_sweep(
    far,
    near,
    low,
    high,
    mine,
    agg,
    coarse,
    factors_hbm,
    coef,
    slots,
    payload,
    current,
    far_out,
    near_out,
    rim,
    values,
    *scratch,
):
    for fetch in fetch_tiles(factors_hbm, scratch[-3], scratch[-2]):
        fetch.start()
    odd = is_odd("wide")
    narrow_odd = is_odd("narrow")
    blank = jnp.zeros((ROWS, LANES), f32)

    def place(target, rows, at, width):
        target[...] = blank
        target[0:8] = rows
        a, b = low[at : at + width], high[at : at + width]
        target[8 : 8 + width] = pick(narrow_odd, a, b)
        target[16 - width : 16] = pick(narrow_odd, b, a)

    for f in range(FULL):
        for a in range(8):
            rows = rim_rows(odd, far, near, mine, f, f * 16, 2, a)
            target = values.at[f - 3, a] if 3 <= f < 6 else rim.at[f if f < 3 else 3, a]
            place(target, rows, (f * 8 + a) * 3, 3)
    for t in range(THIN):
        for a in range(1, 7):
            rows = rim_rows(odd, far, near, mine, FULL + t, FULL * 16 + t * 8, 1, a)
            target = coef.at[CENTRE if t == 0 else COUP + t - 1 if t < 10 else RHS + t - 10, a - 1]
            place(target, rows, FULL * 24 + (t * 6 + a - 1) * 2, 2)
    row = lax.broadcasted_iota(jnp.int32, (ROWS, LANES), 0)
    lane = lane_index((ROWS, LANES))
    low = lane < 64
    offset = jnp.where(row < 8, 32, jnp.where(row < 12, 64, 0))
    inside = box_mask()
    for a in range(8):
        slots[a] = rim[3, a].astype(jnp.int32) + offset
    for a in range(1, 7):
        tx, ty = rim[0, a], rim[1, a]
        tz = jnp.where((lane % 64) < 63, rim[2, a], 0.0)
        txw = jnp.where(low, swap_halves(rim[0, a - 1]), swap_halves(tx))
        tys = shifted(ty, -1, 0)
        tzm = shifted(tz, -1, 1)
        centre = coef[CENTRE, a - 1] + (tx + txw + ty + tys + tz + tzm)
        coef[TX, a - 1] = tx
        coef[TXW, a - 1] = txw
        coef[TY, a - 1] = ty
        coef[TYS, a - 1] = tys
        coef[TZ, a - 1] = tz
        coef[TZM, a - 1] = tzm
        coef[CENTRE, a - 1] = centre
        for c in range(3):
            diagonal = jnp.where(inside, centre + coef[COUP + 4 * c, a - 1], 1.0)
            coef[INV + c, a - 1] = jnp.where(inside, 1.0 / diagonal, 0.0)
    solve_box(values, coef, agg, coarse, factors_hbm, payload, current, far_out, near_out, scratch)


def gather_values(current, far, near, low, high, received, slots, values):
    odd = is_odd("wide")
    narrow_odd = is_odd("narrow")
    total = received[0:24]
    for i in range(24, received.shape[0], 24):
        total += received[i : i + 24]
    block_of = lax.broadcasted_iota(jnp.int32, (24, LANES), 0) % 3
    totals = [jnp.sum(jnp.where(block_of == k, total, 0.0), axis=0, keepdims=True) for k in range(3)]
    blank = jnp.zeros((2, LANES), f32)
    for a in range(8):
        block = 0 if a < 2 else 2 if a >= 6 else 1
        table = jnp.broadcast_to(totals[block], (8, LANES))
        for c in range(3):
            at = (c * 8 + a) * 3
            first, second = low[at : at + 3], high[at : at + 3]
            values[c, a, 0:8] = rim_rows(odd, far, near, current, c, c * 16, 2, a)
            values[c, a, 8:11] = pick(narrow_odd, first, second)
            values[c, a, 11:13] = blank
            values[c, a, 13:16] = pick(narrow_odd, second, first)
        for half in range(2):
            where = slots[a, 8 * half : 8 * half + 8]
            lifted = jnp.take_along_axis(table, where, axis=1, mode="promise_in_bounds")
            values[0, a, 8 * half : 8 * half + 8] += lifted


def next_sweep(
    current,
    far,
    near,
    low,
    high,
    received,
    slots,
    coef,
    agg,
    coarse,
    factors_hbm,
    payload,
    moved,
    far_out,
    near_out,
    values,
    *scratch,
):
    for fetch in fetch_tiles(factors_hbm, scratch[-3], scratch[-2]):
        fetch.start()
    gather_values(current, far, near, low, high, received, slots, values)
    solve_box(values, coef, agg, coarse, factors_hbm, payload, moved, far_out, near_out, scratch)


def last_misfit(current, far, near, low, high, received, slots, coef, iterate, residual, values):
    gather_values(current, far, near, low, high, received, slots, values)
    rolled = {}
    for a in range(2, 6):
        applied = operate_pair(values, coef, a, rolled)
        for c in range(3):
            iterate[c, a - 2] = values[c, a, 0:8]
            residual[c, a - 2] = (coef[RHS + c, a - 1] - applied[c])[0:8]


def local_solve(misfit, coef, values, factors_hbm, factors, sems, moved, one, two):
    fetches = fetch_tiles(factors_hbm, factors, sems)
    own_cols = list(range(8))
    row8 = lax.broadcasted_iota(jnp.int32, (24, LANES), 0) % 8

    def tiles(values, pair, cols, half):
        scaled = [coef[INV + c, pair - 1, 8 * half : 8 * half + 8] * values[c] for c in range(3)]
        left = jnp.concatenate(scaled, axis=0).astype(jnp.bfloat16)
        total = jnp.zeros((24, LANES), f32)
        for y in cols:
            product = lax.dot_general(
                left, factors[pair - 1, y + 2], (((1,), (1,)), ((), ())), preferred_element_type=f32
            )
            total = jnp.where(row8 == y % 8, product, total)
        return [total[8 * c : 8 * c + 8] for c in range(3)]

    blank = jnp.zeros((ROWS, LANES), f32)
    for c in range(3):
        for ref in (one, two):
            ref[c, 0] = blank
            ref[c, 7] = blank
    for a in range(1, 7):
        edge = a in (1, 6)
        fetches[a - 1].wait()
        for half, cols in ((0, own_cols), (1, [8, -1] if edge else [8, 9, -2, -1])):
            part = tiles([misfit[c, a, 8 * half : 8 * half + 8] for c in range(3)], a, cols, half)
            for c in range(3):
                one[c, a, 8 * half : 8 * half + 8] = part[c]
    rolled = {}
    for a in range(1, 7):
        edge = a in (1, 6)
        applied = operate_pair(one, coef, a, rolled)
        left = [misfit[c, a] - applied[c] for c in range(3)]
        for half, cols in ((0, own_cols), (1, [] if edge else [8, -1])):
            if not cols:
                for c in range(3):
                    two[c, a, 8:16] = one[c, a, 8:16]
                continue
            part = tiles([v[8 * half : 8 * half + 8] for v in left], a, cols, half)
            for c in range(3):
                two[c, a, 8 * half : 8 * half + 8] = one[c, a, 8 * half : 8 * half + 8] + part[c]
    rolled = {}
    for a in range(2, 6):
        applied = operate_pair(two, coef, a, rolled)
        part = tiles([(misfit[c, a] - applied[c])[0:8] for c in range(3)], a, own_cols, 0)
        for c in range(3):
            moved[c, a - 2] = values[c, a, 0:8] + (two[c, a, 0:8] + part[c])


def call(body, name, outs, scratch, operands, in_hbm=(), out_hbm=(), flops=1000000):
    vmem = pl.BlockSpec(memory_space=pltpu.VMEM)
    hbm = pl.BlockSpec(memory_space=pltpu.HBM)
    operands = [pltpu.with_memory_space_constraint(x, pltpu.HBM) if i in in_hbm else x for i, x in enumerate(operands)]
    return pl.pallas_call(
        body,
        out_shape=[
            pltpu.HBM(shape, dtype) if i in out_hbm else jax.ShapeDtypeStruct(shape, dtype)
            for i, (shape, dtype) in enumerate(outs)
        ],
        in_specs=[hbm if i in in_hbm else vmem for i in range(len(operands))],
        out_specs=[hbm if i in out_hbm else vmem for i in range(len(outs))],
        scratch_shapes=scratch,
        compiler_params=pltpu.CompilerParams(vmem_limit_bytes=VMEM_LIMIT),
        cost_estimate=pl.CostEstimate(flops=flops, bytes_accessed=0, transcendentals=0),
        name=name,
    )(*operands)


def swaps(axis, far, near):
    count = lax.axis_size(axis)
    with jax.named_scope(axis + "_far"):
        far = lax.ppermute(far, axis, [(i, (i + (1 if i % 2 else -1)) % count) for i in range(count)])
    with jax.named_scope(axis + "_near"):
        near = lax.ppermute(near, axis, [(i, i ^ 1) for i in range(count)])
    return far, near


def per_device(
    rhs, start, trans, accum, coupling, well_cells, well_index, agg_map, tile_factors, coarse_inverse
):
    devices = lax.axis_size("wide") * lax.axis_size("narrow")
    dma = pltpu.SemaphoreType.DMA
    own = ((3, 4, 8, LANES), f32)
    box = (3, PAIRS, ROWS, LANES)
    wide_type = ((48, LANES), f32)
    narrow_type = ((72, LANES), f32)
    payload_type = ((devices * 3, LANES), f32)
    scratch = [
        pltpu.VMEM(box, f32),
        pltpu.VMEM(box, f32),
        pltpu.VMEM((AGG_LOC, LANES), f32),
        pltpu.VMEM((4, devices // 4 + 8, LANES), f32),
        pltpu.VMEM(payload_type[0], f32),
        pltpu.VMEM(box, f32),
        pltpu.VMEM(box, f32),
        pltpu.VMEM(tile_factors.shape, tile_factors.dtype),
        dma((6,)),
        dma,
    ]

    mine, agg, far, near = call(
        add_wells_and_pack,
        "pack_wide",
        [((FULL + THIN, 4, 8, LANES), f32), ((4, 8, LANES), f32)] + [((WIDE_ROWS, LANES), f32)] * 2,
        [
            pltpu.VMEM((1, 64), jnp.int32),
            pltpu.VMEM((1, 64), f32),
            pltpu.VMEM((4, 8, LANES), f32),
            pltpu.VMEM((4, 8, LANES), jnp.int32),
            dma((8,)),
        ],
        [
            well_cells.reshape(1, -1),
            well_index.reshape(1, -1),
            accum,
            trans,
            start,
            agg_map,
            coupling.reshape((9,) + accum.shape),
            rhs,
        ],
        in_hbm=range(8),
    )
    far, near = swaps("wide", far, near)
    low, high = call(pack_narrow, "pack_narrow", [((NARROW_ROWS, LANES), f32)] * 2, [], [far, near, mine])
    low, high = swaps("narrow", low, high)
    coef, slots, payload, current, far, near = call(
        first_sweep,
        "first_sweep",
        [((N_COEF, 6, ROWS, LANES), f32), ((PAIRS, ROWS, LANES), jnp.int32), payload_type, own, wide_type, wide_type],
        [pltpu.VMEM((4, PAIRS, ROWS, LANES), f32)] + scratch,
        [far, near, low, high, mine, agg, coarse_inverse, tile_factors],
        in_hbm=(7,),
        out_hbm=(2,),
    )
    for sweep in range(SWEEPS):
        blocks = payload.reshape(devices, 1, 3 * LANES)
        received = lax.all_to_all(blocks, ("wide", "narrow"), 0, 0).reshape(payload_type[0])
        far, near = swaps("wide", far, near)
        low, high = call(pack_current, "pack_current", [narrow_type] * 2, [], [current, far, near])
        low, high = swaps("narrow", low, high)
        known = [current, far, near, low, high, received, slots, coef]
        if sweep < SWEEPS - 1:
            payload, current, far, near = call(
                next_sweep,
                "next_sweep",
                [payload_type, own, wide_type, wide_type],
                scratch,
                known + [agg, coarse_inverse, tile_factors],
                in_hbm=(10,),
                out_hbm=(0,),
            )
        else:
            iterate, residual = call(last_misfit, "last_misfit", [own, own], [pltpu.VMEM(box, f32)], known)
    return iterate, residual


def solution(mesh):
    return jax.shard_map(
        per_device,
        mesh=mesh,
        in_specs=(
            P(None, "wide", "narrow", None),
            P(None, "wide", "narrow", None),
            P(None, "wide", "narrow", None),
            P("wide", "narrow", None),
            P(None, None, "wide", "narrow", None),
            P("wide", "narrow", None),
            P("wide", "narrow", None),
            P("wide", "narrow", None),
            P("wide", "narrow", None, None),
            P(("wide", "narrow"), None),
        ),
        out_specs=(P(None, "wide", "narrow", None), P(None, "wide", "narrow", None)),
        check_vma=False,
    )
```

```python
import functools

import jax
import jax.numpy as jnp
from jax import lax
from jax.experimental import pallas as pl
from jax.experimental.pallas import tpu as pltpu
from jax.sharding import PartitionSpec as P

AGG_LOC = 32
SWEEPS = 3
PAIRS = 8
ROWS = 16
LANES = 128
FULL = 7
THIN = 13
WIDE_ROWS = FULL * 16 + THIN * 8
NARROW_ROWS = FULL * 24 + THIN * 12
TX, TXW, TY, TYS, TZ, TZM, CENTRE, COUP, INV, RHS = 0, 1, 2, 3, 4, 5, 6, 7, 16, 19
N_COEF = 22
VMEM_LIMIT = 24 * 1024 * 1024

f32 = jnp.float32


def swap_halves(v):
    return pltpu.roll(v, 64, axis=1)


def shifted(v, offset, axis):
    return pltpu.roll(v, (-offset) % v.shape[axis], axis=axis)


def lane_index(shape):
    return lax.broadcasted_iota(jnp.int32, shape, 1)


def box_mask():
    row = lax.broadcasted_iota(jnp.int32, (ROWS, LANES), 0)
    return (row < 10) | (row >= 14)


def operate_pair(values, coef, pair, rolled):
    low = lane_index((ROWS, LANES)) < 64
    mids = [values[c, pair] for c in range(3)]

    def halves(c, p):
        if (c, p) not in rolled:
            rolled[c, p] = swap_halves(values[c, p])
        return rolled[c, p]

    out = []
    for c in range(3):
        v = mids[c]
        own = halves(c, pair)
        inflow = coef[TX, pair - 1] * jnp.where(low, own, halves(c, pair + 1))
        inflow += coef[TXW, pair - 1] * jnp.where(low, halves(c, pair - 1), own)
        inflow += coef[TY, pair - 1] * shifted(v, 1, 0)
        inflow += coef[TYS, pair - 1] * shifted(v, -1, 0)
        inflow += coef[TZ, pair - 1] * shifted(v, 1, 1)
        inflow += coef[TZM, pair - 1] * shifted(v, -1, 1)
        total = coef[CENTRE, pair - 1] * v
        for b in range(3):
            total += coef[COUP + 3 * c + b, pair - 1] * mids[b]
        out.append(total - inflow)
    return out


def pick(odd, when_odd, when_even):
    return jnp.where(odd, when_odd, when_even)


def is_odd(axis):
    return lax.axis_index(axis) % 2 == 1


def add_wells_and_pack(
    cells_in,
    index_in,
    accum,
    trans,
    start,
    agg,
    coupling,
    rhs,
    mine,
    agg_float,
    far,
    near,
    cells,
    index,
    accum_in,
    agg_in,
    sems,
):
    sources = (
        (cells_in, cells),
        (index_in, index),
        (agg, agg_in),
        (accum, accum_in),
        (trans, mine.at[0:3]),
        (start, mine.at[3:6]),
        (coupling, mine.at[8:17]),
        (rhs, mine.at[17:20]),
    )
    copies = [pltpu.make_async_copy(source, target, sems.at[i]) for i, (source, target) in enumerate(sources)]
    for copy in copies:
        copy.start()
    for copy in copies[:2]:
        copy.wait()
    where_row = (lax.broadcasted_iota(jnp.int32, (32, 64), 0) == cells[...] // LANES).astype(f32)
    lane_no = lax.broadcasted_iota(jnp.int32, (LANES, 64), 0)
    share = jnp.where(lane_no == cells[...] % LANES, index[...], 0.0)
    added = lax.dot_general(
        where_row, share, (((1,), (1,)), ((), ())), precision=lax.Precision.HIGHEST, preferred_element_type=f32
    )
    for copy in copies[2:]:
        copy.wait()
    for p in range(4):
        mine[7, p] = accum_in[p] + added[8 * p : 8 * p + 8]
        mine[6, p] = agg_in[p].astype(f32)
        agg_float[p] = agg_in[p].astype(f32)
    odd = is_odd("wide")
    for f in range(FULL):
        for p in range(2):
            east, west = mine[f, 2 + p], mine[f, p]
            at = f * 16 + p * 8
            far[at : at + 8] = pick(odd, east, west)
            near[at : at + 8] = pick(odd, west, east)
    for t in range(THIN):
        east, west = mine[FULL + t, 3], mine[FULL + t, 0]
        at = FULL * 16 + t * 8
        far[at : at + 8] = pick(odd, east, west)
        near[at : at + 8] = pick(odd, west, east)


def rim_rows(odd, far, near, mine, channel_no, at, depth, pair):
    if pair < 2:
        at += 8 * pair if depth == 2 else 0
        return pick(odd, near[at : at + 8], far[at : at + 8])
    if pair >= 6:
        at += 8 * (pair - 6) if depth == 2 else 0
        return pick(odd, far[at : at + 8], near[at : at + 8])
    return mine[channel_no, pair - 2]


def pack_narrow(far, near, mine, low, high):
    odd = is_odd("wide")
    narrow_odd = is_odd("narrow")
    for f in range(FULL):
        for a in range(8):
            v = rim_rows(odd, far, near, mine, f, f * 16, 2, a)
            at = (f * 8 + a) * 3
            low[at : at + 3] = pick(narrow_odd, v[5:8], v[0:3])
            high[at : at + 3] = pick(narrow_odd, v[0:3], v[5:8])
    for t in range(THIN):
        for a in range(1, 7):
            v = rim_rows(odd, far, near, mine, FULL + t, FULL * 16 + t * 8, 1, a)
            at = FULL * 24 + (t * 6 + a - 1) * 2
            low[at : at + 2] = pick(narrow_odd, v[6:8], v[0:2])
            high[at : at + 2] = pick(narrow_odd, v[0:2], v[6:8])


def pack_current(current, far, near, received, low, high, part):
    total = received[0:24]
    for i in range(24, received.shape[0], 24):
        total += received[i : i + 24]
    block_of = lax.broadcasted_iota(jnp.int32, (24, LANES), 0) % 3
    part[...] = jnp.zeros((8, LANES), f32)
    for k in range(3):
        part[k : k + 1, :] = jnp.sum(jnp.where(block_of == k, total, 0.0), axis=0, keepdims=True)
    high[72:80] = part[...]
    odd = is_odd("wide")
    narrow_odd = is_odd("narrow")
    for c in range(3):
        for a in range(8):
            v = rim_rows(odd, far, near, current, c, c * 16, 2, a)
            at = (c * 8 + a) * 3
            low[at : at + 3] = pick(narrow_odd, v[5:8], v[0:3])
            high[at : at + 3] = pick(narrow_odd, v[0:3], v[5:8])


def coarse_part(misfit0, agg, coarse, sums, spread, staged):
    for g in range(AGG_LOC):
        picked = jnp.where(agg[0] == float(g), misfit0[0], 0.0)
        for p in range(1, 4):
            picked += jnp.where(agg[p] == float(g), misfit0[p], 0.0)
        sums[g : g + 1, :] = jnp.sum(picked, axis=0, keepdims=True)
    weight = jnp.broadcast_to(jnp.sum(sums[...], axis=1, keepdims=True), (AGG_LOC, LANES))
    count = coarse.shape[1] // LANES
    for w in range(count):
        row = jnp.sum(coarse[:, w * LANES : (w + 1) * LANES] * weight, axis=0, keepdims=True)
        spread[w + 1 : w + 2, :] = row
    spread[0:1, :] = spread[count : count + 1, :]
    spread[count + 1 : count + 2, :] = spread[1:2, :]
    for w in range(count):
        rows = spread[w : w + 3, :]
        for half in range(2):
            at = 3 * (2 * w + half)
            staged[at : at + 3, :] = rows


def solve_box(values, coef, agg, coarse, factors_hbm, payload, current, far, near, scratch):
    misfit, sums, spread, staged, one, two, factors, tile_sems, sem = scratch
    inside = box_mask()
    rolled = {}
    for c in range(3):
        misfit[c, 0] = jnp.zeros((ROWS, LANES), f32)
        misfit[c, 7] = jnp.zeros((ROWS, LANES), f32)
    for a in range(1, 7):
        applied = operate_pair(values, coef, a, rolled)
        for c in range(3):
            misfit[c, a] = jnp.where(inside, coef[RHS + c, a - 1] - applied[c], 0.0)
    coarse_part([misfit[0, a, 0:8] for a in range(2, 6)], agg, coarse, sums, spread, staged)
    write = pltpu.make_async_copy(staged, payload, sem)
    write.start()
    local_solve(misfit, coef, values, factors_hbm, factors, tile_sems, current, one, two)
    odd = is_odd("wide")
    for c in range(3):
        for p in range(2):
            at = c * 16 + p * 8
            far[at : at + 8] = pick(odd, current[c, 2 + p], current[c, p])
            near[at : at + 8] = pick(odd, current[c, p], current[c, 2 + p])
    write.wait()


def fetch_tiles(factors_hbm, factors, sems):
    cols = [slice(1, 11) if a in (0, 5) else slice(0, 12) for a in range(6)]
    return [pltpu.make_async_copy(factors_hbm.at[a, cols[a]], factors.at[a, cols[a]], sems.at[a]) for a in range(6)]


def first_sweep(
    far,
    near,
    low,
    high,
    mine,
    agg,
    coarse,
    factors_hbm,
    coef,
    slots,
    payload,
    current,
    far_out,
    near_out,
    rim,
    values,
    *scratch,
):
    for fetch in fetch_tiles(factors_hbm, scratch[-3], scratch[-2]):
        fetch.start()
    odd = is_odd("wide")
    narrow_odd = is_odd("narrow")
    blank = jnp.zeros((ROWS, LANES), f32)

    def place(target, rows, at, width):
        target[...] = blank
        target[0:8] = rows
        a, b = low[at : at + width], high[at : at + width]
        target[8 : 8 + width] = pick(narrow_odd, a, b)
        target[16 - width : 16] = pick(narrow_odd, b, a)

    for f in range(FULL):
        for a in range(8):
            rows = rim_rows(odd, far, near, mine, f, f * 16, 2, a)
            target = values.at[f - 3, a] if 3 <= f < 6 else rim.at[f if f < 3 else 3, a]
            place(target, rows, (f * 8 + a) * 3, 3)
    for t in range(THIN):
        for a in range(1, 7):
            rows = rim_rows(odd, far, near, mine, FULL + t, FULL * 16 + t * 8, 1, a)
            target = coef.at[CENTRE if t == 0 else COUP + t - 1 if t < 10 else RHS + t - 10, a - 1]
            place(target, rows, FULL * 24 + (t * 6 + a - 1) * 2, 2)
    row = lax.broadcasted_iota(jnp.int32, (ROWS, LANES), 0)
    lane = lane_index((ROWS, LANES))
    low = lane < 64
    place_of = lax.axis_index("narrow")
    below, here, above = (32 * ((place_of + i) % 4) for i in (3, 0, 1))
    offset = jnp.where(row < 8, here, jnp.where(row < 12, above, below))
    inside = box_mask()
    for a in range(8):
        slots[a] = rim[3, a].astype(jnp.int32) + offset
    for a in range(1, 7):
        tx, ty = rim[0, a], rim[1, a]
        tz = jnp.where((lane % 64) < 63, rim[2, a], 0.0)
        txw = jnp.where(low, swap_halves(rim[0, a - 1]), swap_halves(tx))
        tys = shifted(ty, -1, 0)
        tzm = shifted(tz, -1, 1)
        centre = coef[CENTRE, a - 1] + (tx + txw + ty + tys + tz + tzm)
        coef[TX, a - 1] = tx
        coef[TXW, a - 1] = txw
        coef[TY, a - 1] = ty
        coef[TYS, a - 1] = tys
        coef[TZ, a - 1] = tz
        coef[TZM, a - 1] = tzm
        coef[CENTRE, a - 1] = centre
        for c in range(3):
            diagonal = jnp.where(inside, centre + coef[COUP + 4 * c, a - 1], 1.0)
            coef[INV + c, a - 1] = jnp.where(inside, 1.0 / diagonal, 0.0)
    solve_box(values, coef, agg, coarse, factors_hbm, payload, current, far_out, near_out, scratch)


def gather_values(current, far, near, low, high, part, slots, values):
    odd = is_odd("wide")
    narrow_odd = is_odd("narrow")
    total = part[...] + high[72:80]
    blank = jnp.zeros((2, LANES), f32)
    for a in range(8):
        block = 0 if a < 2 else 2 if a >= 6 else 1
        table = jnp.broadcast_to(total[block : block + 1], (8, LANES))
        for c in range(3):
            at = (c * 8 + a) * 3
            first, second = low[at : at + 3], high[at : at + 3]
            values[c, a, 0:8] = rim_rows(odd, far, near, current, c, c * 16, 2, a)
            values[c, a, 8:11] = pick(narrow_odd, first, second)
            values[c, a, 11:13] = blank
            values[c, a, 13:16] = pick(narrow_odd, second, first)
        for half in range(2):
            where = slots[a, 8 * half : 8 * half + 8]
            lifted = jnp.take_along_axis(table, where, axis=1, mode="promise_in_bounds")
            values[0, a, 8 * half : 8 * half + 8] += lifted


def next_sweep(
    current,
    far,
    near,
    low,
    high,
    part,
    slots,
    coef,
    agg,
    coarse,
    factors_hbm,
    payload,
    moved,
    far_out,
    near_out,
    values,
    *scratch,
):
    for fetch in fetch_tiles(factors_hbm, scratch[-3], scratch[-2]):
        fetch.start()
    gather_values(current, far, near, low, high, part, slots, values)
    solve_box(values, coef, agg, coarse, factors_hbm, payload, moved, far_out, near_out, scratch)


def last_misfit(current, far, near, low, high, part, slots, coef, iterate, residual, values):
    gather_values(current, far, near, low, high, part, slots, values)
    rolled = {}
    for a in range(2, 6):
        applied = operate_pair(values, coef, a, rolled)
        for c in range(3):
            iterate[c, a - 2] = values[c, a, 0:8]
            residual[c, a - 2] = (coef[RHS + c, a - 1] - applied[c])[0:8]


def local_solve(misfit, coef, values, factors_hbm, factors, sems, moved, one, two):
    fetches = fetch_tiles(factors_hbm, factors, sems)
    own_cols = list(range(8))
    row8 = lax.broadcasted_iota(jnp.int32, (24, LANES), 0) % 8

    def tiles(values, pair, cols, half):
        scaled = [coef[INV + c, pair - 1, 8 * half : 8 * half + 8] * values[c] for c in range(3)]
        left = jnp.concatenate(scaled, axis=0).astype(jnp.bfloat16)
        total = jnp.zeros((24, LANES), f32)
        for y in cols:
            product = lax.dot_general(
                left, factors[pair - 1, y + 2], (((1,), (1,)), ((), ())), preferred_element_type=f32
            )
            total = jnp.where(row8 == y % 8, product, total)
        return [total[8 * c : 8 * c + 8] for c in range(3)]

    blank = jnp.zeros((ROWS, LANES), f32)
    for c in range(3):
        for ref in (one, two):
            ref[c, 0] = blank
            ref[c, 7] = blank
    for a in range(1, 7):
        edge = a in (1, 6)
        fetches[a - 1].wait()
        for half, cols in ((0, own_cols), (1, [8, -1] if edge else [8, 9, -2, -1])):
            part = tiles([misfit[c, a, 8 * half : 8 * half + 8] for c in range(3)], a, cols, half)
            for c in range(3):
                one[c, a, 8 * half : 8 * half + 8] = part[c]
    rolled = {}
    for a in range(1, 7):
        edge = a in (1, 6)
        applied = operate_pair(one, coef, a, rolled)
        left = [misfit[c, a] - applied[c] for c in range(3)]
        for half, cols in ((0, own_cols), (1, [] if edge else [8, -1])):
            if not cols:
                for c in range(3):
                    two[c, a, 8:16] = one[c, a, 8:16]
                continue
            part = tiles([v[8 * half : 8 * half + 8] for v in left], a, cols, half)
            for c in range(3):
                two[c, a, 8 * half : 8 * half + 8] = one[c, a, 8 * half : 8 * half + 8] + part[c]
    rolled = {}
    for a in range(2, 6):
        applied = operate_pair(two, coef, a, rolled)
        part = tiles([(misfit[c, a] - applied[c])[0:8] for c in range(3)], a, own_cols, 0)
        for c in range(3):
            moved[c, a - 2] = values[c, a, 0:8] + (two[c, a, 0:8] + part[c])


def call(body, name, outs, scratch, operands, in_hbm=(), out_hbm=(), flops=1000000):
    vmem = pl.BlockSpec(memory_space=pltpu.VMEM)
    hbm = pl.BlockSpec(memory_space=pltpu.HBM)
    operands = [pltpu.with_memory_space_constraint(x, pltpu.HBM) if i in in_hbm else x for i, x in enumerate(operands)]
    return pl.pallas_call(
        body,
        out_shape=[
            pltpu.HBM(shape, dtype) if i in out_hbm else jax.ShapeDtypeStruct(shape, dtype)
            for i, (shape, dtype) in enumerate(outs)
        ],
        in_specs=[hbm if i in in_hbm else vmem for i in range(len(operands))],
        out_specs=[hbm if i in out_hbm else vmem for i in range(len(outs))],
        scratch_shapes=scratch,
        compiler_params=pltpu.CompilerParams(vmem_limit_bytes=VMEM_LIMIT),
        cost_estimate=pl.CostEstimate(flops=flops, bytes_accessed=0, transcendentals=0),
        name=name,
    )(*operands)


def swaps(axis, far, near):
    count = lax.axis_size(axis)
    with jax.named_scope(axis + "_far"):
        far = lax.ppermute(far, axis, [(i, (i + (1 if i % 2 else -1)) % count) for i in range(count)])
    with jax.named_scope(axis + "_near"):
        near = lax.ppermute(near, axis, [(i, i ^ 1) for i in range(count)])
    return far, near


def per_device(
    rhs, start, trans, accum, coupling, well_cells, well_index, agg_map, tile_factors, coarse_inverse
):
    devices = lax.axis_size("wide") * lax.axis_size("narrow")
    members = devices // 2
    groups = [[4 * w + n for w in range(devices // 4) for n in (parity, parity + 2)] for parity in range(2)]
    dma = pltpu.SemaphoreType.DMA
    own = ((3, 4, 8, LANES), f32)
    box = (3, PAIRS, ROWS, LANES)
    wide_type = ((48, LANES), f32)
    narrow_type = ((72, LANES), f32)
    payload_type = ((members * 3, LANES), f32)
    scratch = [
        pltpu.VMEM(box, f32),
        pltpu.VMEM(box, f32),
        pltpu.VMEM((AGG_LOC, LANES), f32),
        pltpu.VMEM((devices // 4 + 8, LANES), f32),
        pltpu.VMEM(payload_type[0], f32),
        pltpu.VMEM(box, f32),
        pltpu.VMEM(box, f32),
        pltpu.VMEM(tile_factors.shape, tile_factors.dtype),
        dma((6,)),
        dma,
    ]

    mine, agg, far, near = call(
        add_wells_and_pack,
        "pack_wide",
        [((FULL + THIN, 4, 8, LANES), f32), ((4, 8, LANES), f32)] + [((WIDE_ROWS, LANES), f32)] * 2,
        [
            pltpu.VMEM((1, 64), jnp.int32),
            pltpu.VMEM((1, 64), f32),
            pltpu.VMEM((4, 8, LANES), f32),
            pltpu.VMEM((4, 8, LANES), jnp.int32),
            dma((8,)),
        ],
        [
            well_cells.reshape(1, -1),
            well_index.reshape(1, -1),
            accum,
            trans,
            start,
            agg_map,
            coupling.reshape((9,) + accum.shape),
            rhs,
        ],
        in_hbm=range(8),
    )
    far, near = swaps("wide", far, near)
    low, high = call(pack_narrow, "pack_narrow", [((NARROW_ROWS, LANES), f32)] * 2, [], [far, near, mine])
    low, high = swaps("narrow", low, high)
    coef, slots, payload, current, far, near = call(
        first_sweep,
        "first_sweep",
        [((N_COEF, 6, ROWS, LANES), f32), ((PAIRS, ROWS, LANES), jnp.int32), payload_type, own, wide_type, wide_type],
        [pltpu.VMEM((4, PAIRS, ROWS, LANES), f32)] + scratch,
        [far, near, low, high, mine, agg, coarse_inverse, tile_factors],
        in_hbm=(7,),
        out_hbm=(2,),
    )
    for sweep in range(SWEEPS):
        blocks = payload.reshape(members, 1, 3 * LANES)
        received = lax.all_to_all(blocks, ("wide", "narrow"), 0, 0, axis_index_groups=groups).reshape(payload_type[0])
        far, near = swaps("wide", far, near)
        low, high, part = call(
            pack_current,
            "pack_current",
            [narrow_type, ((80, LANES), f32), ((8, LANES), f32)],
            [],
            [current, far, near, received],
        )
        low, high = swaps("narrow", low, high)
        known = [current, far, near, low, high, part, slots, coef]
        if sweep < SWEEPS - 1:
            payload, current, far, near = call(
                next_sweep,
                "next_sweep",
                [payload_type, own, wide_type, wide_type],
                scratch,
                known + [agg, coarse_inverse, tile_factors],
                in_hbm=(10,),
                out_hbm=(0,),
            )
        else:
            iterate, residual = call(last_misfit, "last_misfit", [own, own], [pltpu.VMEM(box, f32)], known)
    return iterate, residual


def solution(mesh):
    return jax.shard_map(
        per_device,
        mesh=mesh,
        in_specs=(
            P(None, "wide", "narrow", None),
            P(None, "wide", "narrow", None),
            P(None, "wide", "narrow", None),
            P("wide", "narrow", None),
            P(None, None, "wide", "narrow", None),
            P("wide", "narrow", None),
            P("wide", "narrow", None),
            P("wide", "narrow", None),
            P("wide", "narrow", None, None),
            P(("wide", "narrow"), None),
        ),
        out_specs=(P(None, "wide", "narrow", None), P(None, "wide", "narrow", None)),
        check_vma=False,
    )
```

```python
import functools

import jax
import jax.numpy as jnp
from jax import lax
from jax.experimental import pallas as pl
from jax.experimental.pallas import tpu as pltpu
from jax.sharding import PartitionSpec as P

AGG_LOC = 32
SWEEPS = 3
PAIRS = 8
ROWS = 16
LANES = 128
FULL = 7
THIN = 13
WIDE_ROWS = FULL * 16 + THIN * 8
NARROW_ROWS = FULL * 24 + THIN * 12
TX, TXW, TY, TYS, TZ, TZM, CENTRE, COUP, INV, RHS = 0, 1, 2, 3, 4, 5, 6, 7, 16, 19
N_COEF = 22
VMEM_LIMIT = 24 * 1024 * 1024

f32 = jnp.float32


def swap_halves(v):
    return pltpu.roll(v, 64, axis=1)


def shifted(v, offset, axis):
    return pltpu.roll(v, (-offset) % v.shape[axis], axis=axis)


def lane_index(shape):
    return lax.broadcasted_iota(jnp.int32, shape, 1)


def box_mask():
    row = lax.broadcasted_iota(jnp.int32, (ROWS, LANES), 0)
    return (row < 10) | (row >= 14)


def operate_pair(values, coef, pair, rolled):
    low = lane_index((ROWS, LANES)) < 64
    mids = [values[c, pair] for c in range(3)]

    def halves(c, p):
        if (c, p) not in rolled:
            rolled[c, p] = swap_halves(values[c, p])
        return rolled[c, p]

    out = []
    for c in range(3):
        v = mids[c]
        own = halves(c, pair)
        inflow = coef[TX, pair - 1] * jnp.where(low, own, halves(c, pair + 1))
        inflow += coef[TXW, pair - 1] * jnp.where(low, halves(c, pair - 1), own)
        inflow += coef[TY, pair - 1] * shifted(v, 1, 0)
        inflow += coef[TYS, pair - 1] * shifted(v, -1, 0)
        inflow += coef[TZ, pair - 1] * shifted(v, 1, 1)
        inflow += coef[TZM, pair - 1] * shifted(v, -1, 1)
        total = coef[CENTRE, pair - 1] * v
        for b in range(3):
            total += coef[COUP + 3 * c + b, pair - 1] * mids[b]
        out.append(total - inflow)
    return out


def pick(odd, when_odd, when_even):
    return jnp.where(odd, when_odd, when_even)


def is_odd(axis):
    return lax.axis_index(axis) % 2 == 1


def add_wells_and_pack(
    cells_in,
    index_in,
    accum,
    trans,
    start,
    agg,
    coupling,
    rhs,
    mine,
    agg_float,
    far,
    near,
    cells,
    index,
    accum_in,
    agg_in,
    sems,
):
    sources = (
        (cells_in, cells),
        (index_in, index),
        (agg, agg_in),
        (accum, accum_in),
        (trans, mine.at[0:3]),
        (start, mine.at[3:6]),
        (coupling, mine.at[8:17]),
        (rhs, mine.at[17:20]),
    )
    copies = [pltpu.make_async_copy(source, target, sems.at[i]) for i, (source, target) in enumerate(sources)]
    for copy in copies:
        copy.start()
    for copy in copies[:2]:
        copy.wait()
    where_row = (lax.broadcasted_iota(jnp.int32, (32, 64), 0) == cells[...] // LANES).astype(f32)
    lane_no = lax.broadcasted_iota(jnp.int32, (LANES, 64), 0)
    share = jnp.where(lane_no == cells[...] % LANES, index[...], 0.0)
    added = lax.dot_general(
        where_row, share, (((1,), (1,)), ((), ())), precision=lax.Precision.HIGHEST, preferred_element_type=f32
    )
    for copy in copies[2:]:
        copy.wait()
    for p in range(4):
        mine[7, p] = accum_in[p] + added[8 * p : 8 * p + 8]
        mine[6, p] = agg_in[p].astype(f32)
        agg_float[p] = agg_in[p].astype(f32)
    odd = is_odd("wide")
    for f in range(FULL):
        for p in range(2):
            east, west = mine[f, 2 + p], mine[f, p]
            at = f * 16 + p * 8
            far[at : at + 8] = pick(odd, east, west)
            near[at : at + 8] = pick(odd, west, east)
    for t in range(THIN):
        east, west = mine[FULL + t, 3], mine[FULL + t, 0]
        at = FULL * 16 + t * 8
        far[at : at + 8] = pick(odd, east, west)
        near[at : at + 8] = pick(odd, west, east)


def rim_rows(odd, far, near, mine, channel_no, at, depth, pair):
    if pair < 2:
        at += 8 * pair if depth == 2 else 0
        return pick(odd, near[at : at + 8], far[at : at + 8])
    if pair >= 6:
        at += 8 * (pair - 6) if depth == 2 else 0
        return pick(odd, far[at : at + 8], near[at : at + 8])
    return mine[channel_no, pair - 2]


def pack_narrow(far, near, mine, low, high):
    odd = is_odd("wide")
    narrow_odd = is_odd("narrow")
    for f in range(FULL):
        for a in range(8):
            v = rim_rows(odd, far, near, mine, f, f * 16, 2, a)
            at = (f * 8 + a) * 3
            low[at : at + 3] = pick(narrow_odd, v[5:8], v[0:3])
            high[at : at + 3] = pick(narrow_odd, v[0:3], v[5:8])
    for t in range(THIN):
        for a in range(1, 7):
            v = rim_rows(odd, far, near, mine, FULL + t, FULL * 16 + t * 8, 1, a)
            at = FULL * 24 + (t * 6 + a - 1) * 2
            low[at : at + 2] = pick(narrow_odd, v[6:8], v[0:2])
            high[at : at + 2] = pick(narrow_odd, v[0:2], v[6:8])


def pack_current(current, far, near, received, low, high, part):
    total = received[0:24]
    for i in range(24, received.shape[0], 24):
        total += received[i : i + 24]
    block_of = lax.broadcasted_iota(jnp.int32, (24, LANES), 0) % 3
    part[...] = jnp.zeros((8, LANES), f32)
    for k in range(3):
        part[k : k + 1, :] = jnp.sum(jnp.where(block_of == k, total, 0.0), axis=0, keepdims=True)
    high[72:80] = part[...]
    odd = is_odd("wide")
    narrow_odd = is_odd("narrow")
    for c in range(3):
        for a in range(8):
            v = rim_rows(odd, far, near, current, c, c * 16, 2, a)
            at = (c * 8 + a) * 3
            low[at : at + 3] = pick(narrow_odd, v[5:8], v[0:3])
            high[at : at + 3] = pick(narrow_odd, v[0:3], v[5:8])


def coarse_part(misfit0, agg, coarse, sums, spread, staged, payload, sems):
    for g in range(AGG_LOC):
        picked = jnp.where(agg[0] == float(g), misfit0[0], 0.0)
        for p in range(1, 4):
            picked += jnp.where(agg[p] == float(g), misfit0[p], 0.0)
        sums[g : g + 1, :] = jnp.sum(picked, axis=0, keepdims=True)
    weight = jnp.broadcast_to(jnp.sum(sums[...], axis=1, keepdims=True), (AGG_LOC, LANES))
    count = coarse.shape[1] // LANES
    for w in range(count):
        row = jnp.sum(coarse[:, w * LANES : (w + 1) * LANES] * weight, axis=0, keepdims=True)
        spread[w + 1 : w + 2, :] = row
    spread[0:1, :] = spread[count : count + 1, :]
    spread[count + 1 : count + 2, :] = spread[1:2, :]
    pieces = [slice(0, 3 * count), slice(3 * count, 6 * count)]
    writes = [pltpu.make_async_copy(staged.at[piece], payload.at[piece], sems.at[i]) for i, piece in enumerate(pieces)]
    for w in range(count):
        rows = spread[w : w + 3, :]
        for half in range(2):
            at = 3 * (2 * w + half)
            staged[at : at + 3, :] = rows
        if w == count // 2 - 1:
            writes[0].start()
    writes[1].start()
    for write in writes:
        write.wait()


def misfit_part(values, coef, agg, coarse, misfit, payload, scratch, fetch=None):
    sums, spread, staged, write_sems = scratch
    inside = box_mask()
    rolled = {}
    for c in range(3):
        misfit[c, 0] = jnp.zeros((ROWS, LANES), f32)
        misfit[c, 7] = jnp.zeros((ROWS, LANES), f32)
    for a in range(1, 7):
        applied = operate_pair(values, coef, a, rolled)
        for c in range(3):
            misfit[c, a] = jnp.where(inside, coef[RHS + c, a - 1] - applied[c], 0.0)
    if fetch is not None:
        fetch.wait()
    coarse_part([misfit[0, a, 0:8] for a in range(2, 6)], agg, coarse, sums, spread, staged, payload, write_sems)


def fetch_tiles(factors_hbm, factors, sems):
    cols = [slice(1, 11) if a in (0, 5) else slice(0, 12) for a in range(6)]
    return [pltpu.make_async_copy(factors_hbm.at[a, cols[a]], factors.at[a, cols[a]], sems.at[a]) for a in range(6)]


def first_misfit(
    far,
    near,
    low,
    high,
    mine,
    agg,
    coarse_hbm,
    coef,
    slots,
    moved,
    misfit,
    payload,
    rim,
    coarse,
    sem,
    values,
    *scratch,
):
    fetch = pltpu.make_async_copy(coarse_hbm, coarse, sem)
    fetch.start()
    odd = is_odd("wide")
    narrow_odd = is_odd("narrow")
    blank = jnp.zeros((ROWS, LANES), f32)

    def place(target, rows, at, width):
        target[...] = blank
        target[0:8] = rows
        a, b = low[at : at + width], high[at : at + width]
        target[8 : 8 + width] = pick(narrow_odd, a, b)
        target[16 - width : 16] = pick(narrow_odd, b, a)

    for f in range(FULL):
        for a in range(8):
            rows = rim_rows(odd, far, near, mine, f, f * 16, 2, a)
            target = values.at[f - 3, a] if 3 <= f < 6 else rim.at[f if f < 3 else 3, a]
            place(target, rows, (f * 8 + a) * 3, 3)
    for t in range(THIN):
        for a in range(1, 7):
            rows = rim_rows(odd, far, near, mine, FULL + t, FULL * 16 + t * 8, 1, a)
            target = coef.at[CENTRE if t == 0 else COUP + t - 1 if t < 10 else RHS + t - 10, a - 1]
            place(target, rows, FULL * 24 + (t * 6 + a - 1) * 2, 2)
    row = lax.broadcasted_iota(jnp.int32, (ROWS, LANES), 0)
    lane = lane_index((ROWS, LANES))
    low = lane < 64
    place_of = lax.axis_index("narrow")
    below, here, above = (32 * ((place_of + i) % 4) for i in (3, 0, 1))
    offset = jnp.where(row < 8, here, jnp.where(row < 12, above, below))
    inside = box_mask()
    for a in range(8):
        slots[a] = rim[3, a].astype(jnp.int32) + offset
    for a in range(1, 7):
        tx, ty = rim[0, a], rim[1, a]
        tz = jnp.where((lane % 64) < 63, rim[2, a], 0.0)
        txw = jnp.where(low, swap_halves(rim[0, a - 1]), swap_halves(tx))
        tys = shifted(ty, -1, 0)
        tzm = shifted(tz, -1, 1)
        centre = coef[CENTRE, a - 1] + (tx + txw + ty + tys + tz + tzm)
        coef[TX, a - 1] = tx
        coef[TXW, a - 1] = txw
        coef[TY, a - 1] = ty
        coef[TYS, a - 1] = tys
        coef[TZ, a - 1] = tz
        coef[TZM, a - 1] = tzm
        coef[CENTRE, a - 1] = centre
        for c in range(3):
            diagonal = jnp.where(inside, centre + coef[COUP + 4 * c, a - 1], 1.0)
            coef[INV + c, a - 1] = jnp.where(inside, 1.0 / diagonal, 0.0)
    for c in range(3):
        for p in range(4):
            moved[c, p] = mine[3 + c, p]
    misfit_part(values, coef, agg, coarse, misfit, payload, scratch, fetch)


def gather_values(current, far, near, low, high, part, slots, values):
    odd = is_odd("wide")
    narrow_odd = is_odd("narrow")
    total = part[...] + high[72:80]
    blank = jnp.zeros((2, LANES), f32)
    for a in range(8):
        block = 0 if a < 2 else 2 if a >= 6 else 1
        table = jnp.broadcast_to(total[block : block + 1], (8, LANES))
        for c in range(3):
            at = (c * 8 + a) * 3
            first, second = low[at : at + 3], high[at : at + 3]
            values[c, a, 0:8] = rim_rows(odd, far, near, current, c, c * 16, 2, a)
            values[c, a, 8:11] = pick(narrow_odd, first, second)
            values[c, a, 11:13] = blank
            values[c, a, 13:16] = pick(narrow_odd, second, first)
        for half in range(2):
            where = slots[a, 8 * half : 8 * half + 8]
            lifted = jnp.take_along_axis(table, where, axis=1, mode="promise_in_bounds")
            values[0, a, 8 * half : 8 * half + 8] += lifted


def next_misfit(
    current, far, near, low, high, part, slots, coef, agg, coarse, moved, misfit, payload, values, *scratch
):
    gather_values(current, far, near, low, high, part, slots, values)
    for c in range(3):
        for p in range(4):
            moved[c, p] = values[c, p + 2, 0:8]
    misfit_part(values, coef, agg, coarse, misfit, payload, scratch)


def last_misfit(current, far, near, low, high, part, slots, coef, iterate, residual, values):
    gather_values(current, far, near, low, high, part, slots, values)
    rolled = {}
    for a in range(2, 6):
        applied = operate_pair(values, coef, a, rolled)
        for c in range(3):
            iterate[c, a - 2] = values[c, a, 0:8]
            residual[c, a - 2] = (coef[RHS + c, a - 1] - applied[c])[0:8]


def local_solve(misfit, coef, current, factors_hbm, moved, far, near, one, two, factors, sems):
    fetches = fetch_tiles(factors_hbm, factors, sems)
    for fetch in fetches:
        fetch.start()
    own_cols = list(range(8))
    row8 = lax.broadcasted_iota(jnp.int32, (24, LANES), 0) % 8

    def tiles(values, pair, cols, half):
        scaled = [coef[INV + c, pair - 1, 8 * half : 8 * half + 8] * values[c] for c in range(3)]
        left = jnp.concatenate(scaled, axis=0).astype(jnp.bfloat16)
        total = jnp.zeros((24, LANES), f32)
        for y in cols:
            product = lax.dot_general(
                left, factors[pair - 1, y + 2], (((1,), (1,)), ((), ())), preferred_element_type=f32
            )
            total = jnp.where(row8 == y % 8, product, total)
        return [total[8 * c : 8 * c + 8] for c in range(3)]

    blank = jnp.zeros((ROWS, LANES), f32)
    for c in range(3):
        for ref in (one, two):
            ref[c, 0] = blank
            ref[c, 7] = blank
    rolled_one, rolled_two = {}, {}

    def first(a):
        fetches[a - 1].wait()
        for half, cols in ((0, own_cols), (1, [8, -1] if a in (1, 6) else [8, 9, -2, -1])):
            part = tiles([misfit[c, a, 8 * half : 8 * half + 8] for c in range(3)], a, cols, half)
            for c in range(3):
                one[c, a, 8 * half : 8 * half + 8] = part[c]

    def second(a):
        applied = operate_pair(one, coef, a, rolled_one)
        left = [misfit[c, a] - applied[c] for c in range(3)]
        for half, cols in ((0, own_cols), (1, [] if a in (1, 6) else [8, -1])):
            if not cols:
                for c in range(3):
                    two[c, a, 8:16] = one[c, a, 8:16]
                continue
            part = tiles([v[8 * half : 8 * half + 8] for v in left], a, cols, half)
            for c in range(3):
                two[c, a, 8 * half : 8 * half + 8] = one[c, a, 8 * half : 8 * half + 8] + part[c]

    def third(a):
        applied = operate_pair(two, coef, a, rolled_two)
        part = tiles([(misfit[c, a] - applied[c])[0:8] for c in range(3)], a, own_cols, 0)
        for c in range(3):
            moved[c, a - 2] = current[c, a - 2] + (two[c, a, 0:8] + part[c])

    for a in range(1, 8):
        if a <= 6:
            first(a)
        if a >= 2:
            second(a - 1)
        if a >= 4:
            third(a - 2)
    odd = is_odd("wide")
    for c in range(3):
        for p in range(2):
            at = c * 16 + p * 8
            far[at : at + 8] = pick(odd, moved[c, 2 + p], moved[c, p])
            near[at : at + 8] = pick(odd, moved[c, p], moved[c, 2 + p])


def call(body, name, outs, scratch, operands, in_hbm=(), out_hbm=(), flops=1000000):
    vmem = pl.BlockSpec(memory_space=pltpu.VMEM)
    hbm = pl.BlockSpec(memory_space=pltpu.HBM)
    operands = [pltpu.with_memory_space_constraint(x, pltpu.HBM) if i in in_hbm else x for i, x in enumerate(operands)]
    return pl.pallas_call(
        body,
        out_shape=[
            pltpu.HBM(shape, dtype) if i in out_hbm else jax.ShapeDtypeStruct(shape, dtype)
            for i, (shape, dtype) in enumerate(outs)
        ],
        in_specs=[hbm if i in in_hbm else vmem for i in range(len(operands))],
        out_specs=[hbm if i in out_hbm else vmem for i in range(len(outs))],
        scratch_shapes=scratch,
        compiler_params=pltpu.CompilerParams(vmem_limit_bytes=VMEM_LIMIT),
        cost_estimate=pl.CostEstimate(flops=flops, bytes_accessed=0, transcendentals=0),
        name=name,
    )(*operands)


def swaps(axis, far, near):
    count = lax.axis_size(axis)
    with jax.named_scope(axis + "_far"):
        far = lax.ppermute(far, axis, [(i, (i + (1 if i % 2 else -1)) % count) for i in range(count)])
    with jax.named_scope(axis + "_near"):
        near = lax.ppermute(near, axis, [(i, i ^ 1) for i in range(count)])
    return far, near


def per_device(
    rhs, start, trans, accum, coupling, well_cells, well_index, agg_map, tile_factors, coarse_inverse
):
    devices = lax.axis_size("wide") * lax.axis_size("narrow")
    members = devices // 2
    groups = [[4 * w + n for w in range(devices // 4) for n in (parity, parity + 2)] for parity in range(2)]
    dma = pltpu.SemaphoreType.DMA
    own = ((3, 4, 8, LANES), f32)
    box = (3, PAIRS, ROWS, LANES)
    wide_type = ((48, LANES), f32)
    narrow_type = ((72, LANES), f32)
    payload_type = ((members * 3, LANES), f32)
    scratch = [
        pltpu.VMEM(box, f32),
        pltpu.VMEM((AGG_LOC, LANES), f32),
        pltpu.VMEM((devices // 4 + 8, LANES), f32),
        pltpu.VMEM(payload_type[0], f32),
        dma((2,)),
    ]
    solve_scratch = [
        pltpu.VMEM(box, f32),
        pltpu.VMEM(box, f32),
        pltpu.VMEM(tile_factors.shape, tile_factors.dtype),
        dma((6,)),
    ]

    mine, agg, far, near = call(
        add_wells_and_pack,
        "pack_wide",
        [((FULL + THIN, 4, 8, LANES), f32), ((4, 8, LANES), f32)] + [((WIDE_ROWS, LANES), f32)] * 2,
        [
            pltpu.VMEM((1, 64), jnp.int32),
            pltpu.VMEM((1, 64), f32),
            pltpu.VMEM((4, 8, LANES), f32),
            pltpu.VMEM((4, 8, LANES), jnp.int32),
            dma((8,)),
        ],
        [
            well_cells.reshape(1, -1),
            well_index.reshape(1, -1),
            accum,
            trans,
            start,
            agg_map,
            coupling.reshape((9,) + accum.shape),
            rhs,
        ],
        in_hbm=range(8),
    )
    far, near = swaps("wide", far, near)
    low, high = call(pack_narrow, "pack_narrow", [((NARROW_ROWS, LANES), f32)] * 2, [], [far, near, mine])
    low, high = swaps("narrow", low, high)
    coef, slots, current, misfit, payload = call(
        first_misfit,
        "first_misfit",
        [
            ((N_COEF, 6, ROWS, LANES), f32),
            ((PAIRS, ROWS, LANES), jnp.int32),
            own,
            (box, f32),
            payload_type,
        ],
        [pltpu.VMEM((4, PAIRS, ROWS, LANES), f32), pltpu.VMEM(coarse_inverse.shape, f32), dma] + scratch,
        [far, near, low, high, mine, agg, coarse_inverse],
        in_hbm=(6,),
        out_hbm=(4,),
    )
    for sweep in range(SWEEPS):
        blocks = payload.reshape(members, 1, 3 * LANES)
        received = lax.all_to_all(blocks, ("wide", "narrow"), 0, 0, axis_index_groups=groups).reshape(payload_type[0])
        current, far, near = call(
            local_solve,
            "local_solve",
            [own, wide_type, wide_type],
            solve_scratch,
            [misfit, coef, current, tile_factors],
            in_hbm=(3,),
            flops=30000000,
        )
        far, near = swaps("wide", far, near)
        low, high, part = call(
            pack_current,
            "pack_current",
            [narrow_type, ((80, LANES), f32), ((8, LANES), f32)],
            [],
            [current, far, near, received],
        )
        low, high = swaps("narrow", low, high)
        known = [current, far, near, low, high, part, slots, coef]
        if sweep < SWEEPS - 1:
            current, misfit, payload = call(
                next_misfit,
                "next_misfit",
                [own, (box, f32), payload_type],
                scratch,
                known + [agg, coarse_inverse],
                out_hbm=(2,),
            )
        else:
            iterate, residual = call(last_misfit, "last_misfit", [own, own], [pltpu.VMEM(box, f32)], known)
    return iterate, residual


def solution(mesh):
    return jax.shard_map(
        per_device,
        mesh=mesh,
        in_specs=(
            P(None, "wide", "narrow", None),
            P(None, "wide", "narrow", None),
            P(None, "wide", "narrow", None),
            P("wide", "narrow", None),
            P(None, None, "wide", "narrow", None),
            P("wide", "narrow", None),
            P("wide", "narrow", None),
            P("wide", "narrow", None),
            P("wide", "narrow", None, None),
            P(("wide", "narrow"), None),
        ),
        out_specs=(P(None, "wide", "narrow", None), P(None, "wide", "narrow", None)),
        check_vma=False,
    )
```

```python
import jax
import jax.numpy as jnp
from jax import lax
from jax.experimental import pallas as pl
from jax.experimental.pallas import tpu as pltpu
from jax.sharding import PartitionSpec as P


AGG_LOC = 32
SWEEPS = 3
PAIRS = 8
ROWS = 16
LANES = 128
FULL = 7
THIN = 13
WIDE_ROWS = FULL * 16 + THIN * 8
NARROW_ROWS = FULL * 24 + THIN * 12
TX, TXW, TY, TYS, TZ, TZM, CENTRE, COUP, INV, RHS = 0, 1, 2, 3, 4, 5, 6, 7, 16, 19
N_COEF = 22
VMEM_LIMIT = 24 * 1024 * 1024

f32 = jnp.float32


def swap_halves(v):
    return pltpu.roll(v, 64, axis=1)


def shifted(v, offset, axis):
    return pltpu.roll(v, (-offset) % v.shape[axis], axis=axis)


def lane_index(shape):
    return lax.broadcasted_iota(jnp.int32, shape, 1)


def box_mask():
    row = lax.broadcasted_iota(jnp.int32, (ROWS, LANES), 0)
    return (row < 10) | (row >= 14)


def operate_pair(values, coef, pair, rolled):
    low = lane_index((ROWS, LANES)) < 64
    mids = [values[c, pair] for c in range(3)]

    def halves(c, p):
        if (c, p) not in rolled:
            rolled[c, p] = swap_halves(values[c, p])
        return rolled[c, p]

    out = []
    for c in range(3):
        v = mids[c]
        own = halves(c, pair)
        inflow = coef[TX, pair - 1] * jnp.where(low, own, halves(c, pair + 1))
        inflow += coef[TXW, pair - 1] * jnp.where(low, halves(c, pair - 1), own)
        inflow += coef[TY, pair - 1] * shifted(v, 1, 0)
        inflow += coef[TYS, pair - 1] * shifted(v, -1, 0)
        inflow += coef[TZ, pair - 1] * shifted(v, 1, 1)
        inflow += coef[TZM, pair - 1] * shifted(v, -1, 1)
        total = coef[CENTRE, pair - 1] * v
        for b in range(3):
            total += coef[COUP + 3 * c + b, pair - 1] * mids[b]
        out.append(total - inflow)
    return out


def pick(odd, when_odd, when_even):
    return jnp.where(odd, when_odd, when_even)


def is_odd(axis):
    return lax.axis_index(axis) % 2 == 1


def add_wells_and_pack(
    cells_in,
    index_in,
    accum,
    trans,
    start,
    agg,
    coupling,
    rhs,
    mine,
    agg_float,
    far,
    near,
    cells,
    index,
    accum_in,
    agg_in,
    sems,
):
    sources = (
        (cells_in, cells),
        (index_in, index),
        (agg, agg_in),
        (accum, accum_in),
        (trans, mine.at[0:3]),
        (start, mine.at[3:6]),
        (coupling, mine.at[8:17]),
        (rhs, mine.at[17:20]),
    )
    copies = [pltpu.make_async_copy(source, target, sems.at[i]) for i, (source, target) in enumerate(sources)]
    for copy in copies:
        copy.start()
    for copy in copies[:2]:
        copy.wait()
    where_row = (lax.broadcasted_iota(jnp.int32, (32, 64), 0) == cells[...] // LANES).astype(f32)
    lane_no = lax.broadcasted_iota(jnp.int32, (LANES, 64), 0)
    share = jnp.where(lane_no == cells[...] % LANES, index[...], 0.0)
    added = lax.dot_general(
        where_row, share, (((1,), (1,)), ((), ())), precision=lax.Precision.HIGHEST, preferred_element_type=f32
    )
    for copy in copies[2:]:
        copy.wait()
    for p in range(4):
        mine[7, p] = accum_in[p] + added[8 * p : 8 * p + 8]
        mine[6, p] = agg_in[p].astype(f32)
        agg_float[p] = agg_in[p].astype(f32)
    odd = is_odd("wide")
    for f in range(FULL):
        for p in range(2):
            east, west = mine[f, 2 + p], mine[f, p]
            at = f * 16 + p * 8
            far[at : at + 8] = pick(odd, east, west)
            near[at : at + 8] = pick(odd, west, east)
    for t in range(THIN):
        east, west = mine[FULL + t, 3], mine[FULL + t, 0]
        at = FULL * 16 + t * 8
        far[at : at + 8] = pick(odd, east, west)
        near[at : at + 8] = pick(odd, west, east)


def rim_rows(odd, far, near, mine, channel_no, at, depth, pair):
    if pair < 2:
        at += 8 * pair if depth == 2 else 0
        return pick(odd, near[at : at + 8], far[at : at + 8])
    if pair >= 6:
        at += 8 * (pair - 6) if depth == 2 else 0
        return pick(odd, far[at : at + 8], near[at : at + 8])
    return mine[channel_no, pair - 2]


def pack_narrow(far, near, mine, low, high):
    odd = is_odd("wide")
    narrow_odd = is_odd("narrow")
    for f in range(FULL):
        for a in range(8):
            v = rim_rows(odd, far, near, mine, f, f * 16, 2, a)
            at = (f * 8 + a) * 3
            low[at : at + 3] = pick(narrow_odd, v[5:8], v[0:3])
            high[at : at + 3] = pick(narrow_odd, v[0:3], v[5:8])
    for t in range(THIN):
        for a in range(1, 7):
            v = rim_rows(odd, far, near, mine, FULL + t, FULL * 16 + t * 8, 1, a)
            at = FULL * 24 + (t * 6 + a - 1) * 2
            low[at : at + 2] = pick(narrow_odd, v[6:8], v[0:2])
            high[at : at + 2] = pick(narrow_odd, v[0:2], v[6:8])


def pack_current(current, far, near, received, low, high, part):
    total = received[0:8]
    for i in range(8, received.shape[0], 8):
        total += received[i : i + 8]
    part[...] = jnp.broadcast_to(jnp.sum(total, axis=0, keepdims=True), (8, LANES))
    low[72:80] = part[...]
    high[72:80] = part[...]
    odd = is_odd("wide")
    narrow_odd = is_odd("narrow")
    for c in range(3):
        for a in range(8):
            v = rim_rows(odd, far, near, current, c, c * 16, 2, a)
            at = (c * 8 + a) * 3
            low[at : at + 3] = pick(narrow_odd, v[5:8], v[0:3])
            high[at : at + 3] = pick(narrow_odd, v[0:3], v[5:8])


def coarse_part(misfit0, agg, coarse, sums, spread, staged):
    for g in range(AGG_LOC):
        picked = jnp.where(agg[0] == float(g), misfit0[0], 0.0)
        for p in range(1, 4):
            picked += jnp.where(agg[p] == float(g), misfit0[p], 0.0)
        sums[g : g + 1, :] = jnp.sum(picked, axis=0, keepdims=True)
    weight = jnp.broadcast_to(jnp.sum(sums[...], axis=1, keepdims=True), (AGG_LOC, LANES))
    count = coarse.shape[1] // LANES
    for w in range(count):
        row = jnp.sum(coarse[:, w * LANES : (w + 1) * LANES] * weight, axis=0, keepdims=True)
        spread[0, w + 1 : w + 2, :] = row
    middle = spread[0, 1 : count + 1, :]
    for turn in range(4):
        turned = shifted(middle, -32 * turn, 1) if turn else middle
        if turn:
            spread[turn, 1 : count + 1, :] = turned
        spread[turn, 0:1, :] = turned[count - 1 : count]
        spread[turn, count + 1 : count + 2, :] = turned[0:1]
    lane = lane_index((count, LANES))
    for n in range(4):
        before, own, after = (spread[(k - n) % 4, k : k + count, :] for k in range(3))
        staged[pl.ds(n, count, stride=4), :] = jnp.where(lane < 32, before, jnp.where(lane < 64, own, after))


def solve_box(values, coef, agg, coarse, factors_hbm, payload, current, far, near, scratch, coarse_fetch=None):
    misfit, sums, spread, staged, one, two, factors, tile_sems, sem = scratch
    inside = box_mask()
    rolled = {}
    for c in range(3):
        misfit[c, 0] = jnp.zeros((ROWS, LANES), f32)
        misfit[c, 7] = jnp.zeros((ROWS, LANES), f32)
    for a in range(1, 7):
        applied = operate_pair(values, coef, a, rolled)
        for c in range(3):
            misfit[c, a] = jnp.where(inside, coef[RHS + c, a - 1] - applied[c], 0.0)
    if coarse_fetch is not None:
        coarse_fetch.wait()
    coarse_part([misfit[0, a, 0:8] for a in range(2, 6)], agg, coarse, sums, spread, staged)
    write = pltpu.make_async_copy(staged, payload, sem)
    write.start()
    local_solve(misfit, coef, values, factors_hbm, factors, tile_sems, current, one, two)
    odd = is_odd("wide")
    for c in range(3):
        for p in range(2):
            at = c * 16 + p * 8
            far[at : at + 8] = pick(odd, current[c, 2 + p], current[c, p])
            near[at : at + 8] = pick(odd, current[c, p], current[c, 2 + p])
    write.wait()


def fetch_tiles(factors_hbm, factors, sems):
    cols = [slice(1, 11) if a in (0, 5) else slice(0, 12) for a in range(6)]
    return [pltpu.make_async_copy(factors_hbm.at[a, cols[a]], factors.at[a, cols[a]], sems.at[a]) for a in range(6)]


def first_sweep(
    far,
    near,
    low,
    high,
    mine,
    agg,
    coarse_hbm,
    factors_hbm,
    coef,
    slots,
    payload,
    current,
    far_out,
    near_out,
    rim,
    coarse,
    coarse_sem,
    values,
    *scratch,
):
    coarse_fetch = pltpu.make_async_copy(coarse_hbm, coarse, coarse_sem)
    coarse_fetch.start()
    for fetch in fetch_tiles(factors_hbm, scratch[-3], scratch[-2]):
        fetch.start()
    odd = is_odd("wide")
    narrow_odd = is_odd("narrow")
    blank = jnp.zeros((ROWS, LANES), f32)

    def place(target, rows, at, width):
        target[...] = blank
        target[0:8] = rows
        a, b = low[at : at + width], high[at : at + width]
        target[8 : 8 + width] = pick(narrow_odd, a, b)
        target[16 - width : 16] = pick(narrow_odd, b, a)

    for f in range(FULL):
        for a in range(8):
            rows = rim_rows(odd, far, near, mine, f, f * 16, 2, a)
            target = values.at[f - 3, a] if 3 <= f < 6 else rim.at[f if f < 3 else 3, a]
            place(target, rows, (f * 8 + a) * 3, 3)
    for t in range(THIN):
        for a in range(1, 7):
            rows = rim_rows(odd, far, near, mine, FULL + t, FULL * 16 + t * 8, 1, a)
            target = coef.at[CENTRE if t == 0 else COUP + t - 1 if t < 10 else RHS + t - 10, a - 1]
            place(target, rows, FULL * 24 + (t * 6 + a - 1) * 2, 2)
    row = lax.broadcasted_iota(jnp.int32, (ROWS, LANES), 0)
    lane = lane_index((ROWS, LANES))
    low = lane < 64
    inside = box_mask()
    for a in range(8):
        slots[a] = rim[3, a].astype(jnp.int32) + (0 if a < 2 else 64 if a >= 6 else 32)
    for a in range(1, 7):
        tx, ty = rim[0, a], rim[1, a]
        tz = jnp.where((lane % 64) < 63, rim[2, a], 0.0)
        txw = jnp.where(low, swap_halves(rim[0, a - 1]), swap_halves(tx))
        tys = shifted(ty, -1, 0)
        tzm = shifted(tz, -1, 1)
        centre = coef[CENTRE, a - 1] + (tx + txw + ty + tys + tz + tzm)
        coef[TX, a - 1] = tx
        coef[TXW, a - 1] = txw
        coef[TY, a - 1] = ty
        coef[TYS, a - 1] = tys
        coef[TZ, a - 1] = tz
        coef[TZM, a - 1] = tzm
        coef[CENTRE, a - 1] = centre
        for c in range(3):
            diagonal = jnp.where(inside, centre + coef[COUP + 4 * c, a - 1], 1.0)
            coef[INV + c, a - 1] = jnp.where(inside, 1.0 / diagonal, 0.0)
    solve_box(values, coef, agg, coarse, factors_hbm, payload, current, far_out, near_out, scratch, coarse_fetch)


def gather_values(current, far, near, low, high, part, slots, values):
    odd = is_odd("wide")
    narrow_odd = is_odd("narrow")
    a_part, b_part = low[72:80], high[72:80]
    upper_rows = lax.broadcasted_iota(jnp.int32, (8, LANES), 0) < 4
    from_above, from_below = pick(narrow_odd, a_part, b_part), pick(narrow_odd, b_part, a_part)
    tables = (part[...], jnp.where(upper_rows, from_above, from_below))
    blank = jnp.zeros((2, LANES), f32)
    for a in range(8):
        for c in range(3):
            at = (c * 8 + a) * 3
            first, second = low[at : at + 3], high[at : at + 3]
            values[c, a, 0:8] = rim_rows(odd, far, near, current, c, c * 16, 2, a)
            values[c, a, 8:11] = pick(narrow_odd, first, second)
            values[c, a, 11:13] = blank
            values[c, a, 13:16] = pick(narrow_odd, second, first)
        for half in range(2):
            where = slots[a, 8 * half : 8 * half + 8]
            lifted = jnp.take_along_axis(tables[half], where, axis=1, mode="promise_in_bounds")
            values[0, a, 8 * half : 8 * half + 8] += lifted


def next_sweep(
    current,
    far,
    near,
    low,
    high,
    part,
    slots,
    coef,
    agg,
    coarse,
    factors_hbm,
    payload,
    moved,
    far_out,
    near_out,
    values,
    *scratch,
):
    for fetch in fetch_tiles(factors_hbm, scratch[-3], scratch[-2]):
        fetch.start()
    gather_values(current, far, near, low, high, part, slots, values)
    solve_box(values, coef, agg, coarse, factors_hbm, payload, moved, far_out, near_out, scratch)


def last_misfit(current, far, near, low, high, part, slots, coef, iterate, residual, values):
    gather_values(current, far, near, low, high, part, slots, values)
    rolled = {}
    for a in range(2, 6):
        applied = operate_pair(values, coef, a, rolled)
        for c in range(3):
            iterate[c, a - 2] = values[c, a, 0:8]
            residual[c, a - 2] = (coef[RHS + c, a - 1] - applied[c])[0:8]


def local_solve(misfit, coef, values, factors_hbm, factors, sems, moved, one, two):
    fetches = fetch_tiles(factors_hbm, factors, sems)
    own_cols = list(range(8))
    row8 = lax.broadcasted_iota(jnp.int32, (24, LANES), 0) % 8

    def tiles(values, pair, cols, half):
        scaled = [coef[INV + c, pair - 1, 8 * half : 8 * half + 8] * values[c] for c in range(3)]
        left = jnp.concatenate(scaled, axis=0).astype(jnp.bfloat16)
        total = jnp.zeros((24, LANES), f32)
        for y in cols:
            product = lax.dot_general(
                left, factors[pair - 1, y + 2], (((1,), (1,)), ((), ())), preferred_element_type=f32
            )
            total = jnp.where(row8 == y % 8, product, total)
        return [total[8 * c : 8 * c + 8] for c in range(3)]

    blank = jnp.zeros((ROWS, LANES), f32)
    for c in range(3):
        for ref in (one, two):
            ref[c, 0] = blank
            ref[c, 7] = blank
    for a in range(1, 7):
        edge = a in (1, 6)
        if a in (1, 4):
            for fetch in fetches[a - 1 : a + 2]:
                fetch.wait()
        for half, cols in ((0, own_cols), (1, [8, -1] if edge else [8, 9, -2, -1])):
            part = tiles([misfit[c, a, 8 * half : 8 * half + 8] for c in range(3)], a, cols, half)
            for c in range(3):
                one[c, a, 8 * half : 8 * half + 8] = part[c]
    rolled = {}
    for a in range(1, 7):
        edge = a in (1, 6)
        applied = operate_pair(one, coef, a, rolled)
        left = [misfit[c, a] - applied[c] for c in range(3)]
        for half, cols in ((0, own_cols), (1, [] if edge else [8, -1])):
            if not cols:
                for c in range(3):
                    two[c, a, 8:16] = one[c, a, 8:16]
                continue
            part = tiles([v[8 * half : 8 * half + 8] for v in left], a, cols, half)
            for c in range(3):
                two[c, a, 8 * half : 8 * half + 8] = one[c, a, 8 * half : 8 * half + 8] + part[c]
    rolled = {}
    for a in range(2, 6):
        applied = operate_pair(two, coef, a, rolled)
        part = tiles([(misfit[c, a] - applied[c])[0:8] for c in range(3)], a, own_cols, 0)
        for c in range(3):
            moved[c, a - 2] = values[c, a, 0:8] + (two[c, a, 0:8] + part[c])


def call(body, outs, scratch, operands, in_hbm=(), out_hbm=(), flops=1000000):
    vmem = pl.BlockSpec(memory_space=pltpu.VMEM)
    hbm = pl.BlockSpec(memory_space=pltpu.HBM)
    operands = [pltpu.with_memory_space_constraint(x, pltpu.HBM) if i in in_hbm else x for i, x in enumerate(operands)]
    return pl.pallas_call(
        body,
        out_shape=[
            pltpu.HBM(shape, dtype) if i in out_hbm else jax.ShapeDtypeStruct(shape, dtype)
            for i, (shape, dtype) in enumerate(outs)
        ],
        in_specs=[hbm if i in in_hbm else vmem for i in range(len(operands))],
        out_specs=[hbm if i in out_hbm else vmem for i in range(len(outs))],
        scratch_shapes=scratch,
        compiler_params=pltpu.CompilerParams(vmem_limit_bytes=VMEM_LIMIT),
        cost_estimate=pl.CostEstimate(flops=flops, bytes_accessed=0, transcendentals=0),
    )(*operands)


def swaps(axis, far, near):
    count = lax.axis_size(axis)
    far = lax.ppermute(far, axis, [(i, (i + (1 if i % 2 else -1)) % count) for i in range(count)])
    near = lax.ppermute(near, axis, [(i, i ^ 1) for i in range(count)])
    return far, near


def per_device(
    rhs, start, trans, accum, coupling, well_cells, well_index, agg_map, tile_factors, coarse_inverse
):
    devices = lax.axis_size("wide") * lax.axis_size("narrow")
    dma = pltpu.SemaphoreType.DMA
    own = ((3, 4, 8, LANES), f32)
    box = (3, PAIRS, ROWS, LANES)
    wide_type = ((48, LANES), f32)
    narrow_type = ((80, LANES), f32)
    payload_type = ((devices, LANES), f32)
    scratch = [
        pltpu.VMEM(box, f32),
        pltpu.VMEM(box, f32),
        pltpu.VMEM((AGG_LOC, LANES), f32),
        pltpu.VMEM((4, devices // 4 + 8, LANES), f32),
        pltpu.VMEM(payload_type[0], f32),
        pltpu.VMEM(box, f32),
        pltpu.VMEM(box, f32),
        pltpu.VMEM(tile_factors.shape, tile_factors.dtype),
        dma((6,)),
        dma,
    ]

    mine, agg, far, near = call(
        add_wells_and_pack,
        [((FULL + THIN, 4, 8, LANES), f32), ((4, 8, LANES), f32)] + [((WIDE_ROWS, LANES), f32)] * 2,
        [
            pltpu.VMEM((1, 64), jnp.int32),
            pltpu.VMEM((1, 64), f32),
            pltpu.VMEM((4, 8, LANES), f32),
            pltpu.VMEM((4, 8, LANES), jnp.int32),
            dma((8,)),
        ],
        [
            well_cells.reshape(1, -1),
            well_index.reshape(1, -1),
            accum,
            trans,
            start,
            agg_map,
            coupling.reshape((9,) + accum.shape),
            rhs,
        ],
        in_hbm=range(8),
    )
    far, near = swaps("wide", far, near)
    low, high = call(pack_narrow, [((NARROW_ROWS, LANES), f32)] * 2, [], [far, near, mine])
    low, high = swaps("narrow", low, high)
    coef, slots, payload, current, far, near = call(
        first_sweep,
        [((N_COEF, 6, ROWS, LANES), f32), ((PAIRS, ROWS, LANES), jnp.int32), payload_type, own, wide_type, wide_type],
        [pltpu.VMEM((4, PAIRS, ROWS, LANES), f32), pltpu.VMEM(coarse_inverse.shape, f32), dma] + scratch,
        [far, near, low, high, mine, agg, coarse_inverse, tile_factors],
        in_hbm=(6, 7),
        out_hbm=(2,),
    )
    for sweep in range(SWEEPS):
        blocks = payload.reshape(devices, 1, LANES)
        received = lax.all_to_all(blocks, ("wide", "narrow"), 0, 0).reshape(payload_type[0])
        far, near = swaps("wide", far, near)
        low, high, part = call(
            pack_current, [narrow_type, narrow_type, ((8, LANES), f32)], [], [current, far, near, received]
        )
        low, high = swaps("narrow", low, high)
        known = [current, far, near, low, high, part, slots, coef]
        if sweep < SWEEPS - 1:
            payload, current, far, near = call(
                next_sweep,
                [payload_type, own, wide_type, wide_type],
                scratch,
                known + [agg, coarse_inverse, tile_factors],
                in_hbm=(10,),
                out_hbm=(0,),
            )
        else:
            iterate, residual = call(last_misfit, [own, own], [pltpu.VMEM(box, f32)], known)
    return iterate, residual


def solution(mesh):
    return jax.shard_map(
        per_device,
        mesh=mesh,
        in_specs=(
            P(None, "wide", "narrow", None),
            P(None, "wide", "narrow", None),
            P(None, "wide", "narrow", None),
            P("wide", "narrow", None),
            P(None, None, "wide", "narrow", None),
            P("wide", "narrow", None),
            P("wide", "narrow", None),
            P("wide", "narrow", None),
            P("wide", "narrow", None, None),
            P(("wide", "narrow"), None),
        ),
        out_specs=(P(None, "wide", "narrow", None), P(None, "wide", "narrow", None)),
        check_vma=False,
    )
```

```python
import jax
import jax.numpy as jnp
from jax import lax
from jax.experimental import pallas as pl
from jax.experimental.pallas import tpu as pltpu
from jax.sharding import PartitionSpec as P


AGG_LOC = 32
SWEEPS = 3
PAIRS = 8
ROWS = 16
LANES = 128
FULL = 7
THIN = 13
WIDE_ROWS = FULL * 16 + THIN * 8
NARROW_ROWS = FULL * 24 + THIN * 12
TX, TXW, TY, TYS, TZ, TZM, CENTRE, COUP, INV, RHS = 0, 1, 2, 3, 4, 5, 6, 7, 16, 19
N_COEF = 22
VMEM_LIMIT = 24 * 1024 * 1024

f32 = jnp.float32


def swap_halves(v):
    return pltpu.roll(v, 64, axis=1)


def shifted(v, offset, axis):
    return pltpu.roll(v, (-offset) % v.shape[axis], axis=axis)


def lane_index(shape):
    return lax.broadcasted_iota(jnp.int32, shape, 1)


def box_mask():
    row = lax.broadcasted_iota(jnp.int32, (ROWS, LANES), 0)
    return (row < 10) | (row >= 14)


def operate_pair(values, coef, pair, rolled):
    low = lane_index((ROWS, LANES)) < 64
    mids = [values[c, pair] for c in range(3)]

    def halves(c, p):
        if (c, p) not in rolled:
            rolled[c, p] = swap_halves(values[c, p])
        return rolled[c, p]

    out = []
    for c in range(3):
        v = mids[c]
        own = halves(c, pair)
        inflow = coef[TX, pair - 1] * jnp.where(low, own, halves(c, pair + 1))
        inflow += coef[TXW, pair - 1] * jnp.where(low, halves(c, pair - 1), own)
        inflow += coef[TY, pair - 1] * shifted(v, 1, 0)
        inflow += coef[TYS, pair - 1] * shifted(v, -1, 0)
        inflow += coef[TZ, pair - 1] * shifted(v, 1, 1)
        inflow += coef[TZM, pair - 1] * shifted(v, -1, 1)
        total = coef[CENTRE, pair - 1] * v
        for b in range(3):
            total += coef[COUP + 3 * c + b, pair - 1] * mids[b]
        out.append(total - inflow)
    return out


def pick(odd, when_odd, when_even):
    return jnp.where(odd, when_odd, when_even)


def is_odd(axis):
    return lax.axis_index(axis) % 2 == 1


def add_wells_and_pack(
    cells_in,
    index_in,
    accum,
    trans,
    start,
    agg,
    coupling,
    rhs,
    mine,
    agg_float,
    far,
    near,
    cells,
    index,
    accum_in,
    agg_in,
    sems,
):
    sources = (
        (cells_in, cells),
        (index_in, index),
        (agg, agg_in),
        (accum, accum_in),
        (trans, mine.at[0:3]),
        (start, mine.at[3:6]),
        (coupling, mine.at[8:17]),
        (rhs, mine.at[17:20]),
    )
    copies = [pltpu.make_async_copy(source, target, sems.at[i]) for i, (source, target) in enumerate(sources)]
    for copy in copies:
        copy.start()
    for copy in copies[:2]:
        copy.wait()
    where_row = (lax.broadcasted_iota(jnp.int32, (32, 64), 0) == cells[...] // LANES).astype(f32)
    lane_no = lax.broadcasted_iota(jnp.int32, (LANES, 64), 0)
    share = jnp.where(lane_no == cells[...] % LANES, index[...], 0.0)
    added = lax.dot_general(
        where_row, share, (((1,), (1,)), ((), ())), precision=lax.Precision.HIGHEST, preferred_element_type=f32
    )
    for copy in copies[2:]:
        copy.wait()
    for p in range(4):
        mine[7, p] = accum_in[p] + added[8 * p : 8 * p + 8]
        mine[6, p] = agg_in[p].astype(f32)
        agg_float[p] = agg_in[p].astype(f32)
    odd = is_odd("wide")
    for f in range(FULL):
        for p in range(2):
            east, west = mine[f, 2 + p], mine[f, p]
            at = f * 16 + p * 8
            far[at : at + 8] = pick(odd, east, west)
            near[at : at + 8] = pick(odd, west, east)
    for t in range(THIN):
        east, west = mine[FULL + t, 3], mine[FULL + t, 0]
        at = FULL * 16 + t * 8
        far[at : at + 8] = pick(odd, east, west)
        near[at : at + 8] = pick(odd, west, east)


def rim_rows(odd, far, near, mine, channel_no, at, depth, pair):
    if pair < 2:
        at += 8 * pair if depth == 2 else 0
        return pick(odd, near[at : at + 8], far[at : at + 8])
    if pair >= 6:
        at += 8 * (pair - 6) if depth == 2 else 0
        return pick(odd, far[at : at + 8], near[at : at + 8])
    return mine[channel_no, pair - 2]


def pack_narrow(far, near, mine, low, high):
    odd = is_odd("wide")
    narrow_odd = is_odd("narrow")
    for f in range(FULL):
        for a in range(8):
            v = rim_rows(odd, far, near, mine, f, f * 16, 2, a)
            at = (f * 8 + a) * 3
            low[at : at + 3] = pick(narrow_odd, v[5:8], v[0:3])
            high[at : at + 3] = pick(narrow_odd, v[0:3], v[5:8])
    for t in range(THIN):
        for a in range(1, 7):
            v = rim_rows(odd, far, near, mine, FULL + t, FULL * 16 + t * 8, 1, a)
            at = FULL * 24 + (t * 6 + a - 1) * 2
            low[at : at + 2] = pick(narrow_odd, v[6:8], v[0:2])
            high[at : at + 2] = pick(narrow_odd, v[0:2], v[6:8])


def pack_current(current, far, near, received, low, high, part):
    total = received[0:24]
    for i in range(24, received.shape[0], 24):
        total += received[i : i + 24]
    block_of = lax.broadcasted_iota(jnp.int32, (24, LANES), 0) % 3
    part[...] = jnp.zeros((8, LANES), f32)
    for k in range(3):
        part[k : k + 1, :] = jnp.sum(jnp.where(block_of == k, total, 0.0), axis=0, keepdims=True)
    high[72:80] = part[...]
    odd = is_odd("wide")
    narrow_odd = is_odd("narrow")
    for c in range(3):
        for a in range(8):
            v = rim_rows(odd, far, near, current, c, c * 16, 2, a)
            at = (c * 8 + a) * 3
            low[at : at + 3] = pick(narrow_odd, v[5:8], v[0:3])
            high[at : at + 3] = pick(narrow_odd, v[0:3], v[5:8])


def coarse_part(misfit0, agg, coarse, sums, spread, staged):
    for g in range(AGG_LOC):
        picked = jnp.where(agg[0] == float(g), misfit0[0], 0.0)
        for p in range(1, 4):
            picked += jnp.where(agg[p] == float(g), misfit0[p], 0.0)
        sums[g : g + 1, :] = jnp.sum(picked, axis=0, keepdims=True)
    weight = jnp.broadcast_to(jnp.sum(sums[...], axis=1, keepdims=True), (AGG_LOC, LANES))
    count = coarse.shape[1] // LANES
    for w in range(count):
        row = jnp.sum(coarse[:, w * LANES : (w + 1) * LANES] * weight, axis=0, keepdims=True)
        spread[w + 1 : w + 2, :] = row
    spread[0:1, :] = spread[count : count + 1, :]
    spread[count + 1 : count + 2, :] = spread[1:2, :]
    for w in range(count):
        rows = spread[w : w + 3, :]
        for half in range(2):
            at = 3 * (2 * w + half)
            staged[at : at + 3, :] = rows


def solve_box(values, coef, agg, coarse, factors_hbm, payload, current, far, near, scratch, coarse_fetch=None):
    misfit, sums, spread, staged, one, two, factors, tile_sems, sem = scratch
    inside = box_mask()
    rolled = {}
    for c in range(3):
        misfit[c, 0] = jnp.zeros((ROWS, LANES), f32)
        misfit[c, 7] = jnp.zeros((ROWS, LANES), f32)
    for a in range(1, 7):
        applied = operate_pair(values, coef, a, rolled)
        for c in range(3):
            misfit[c, a] = jnp.where(inside, coef[RHS + c, a - 1] - applied[c], 0.0)
    if coarse_fetch is not None:
        coarse_fetch.wait()
    coarse_part([misfit[0, a, 0:8] for a in range(2, 6)], agg, coarse, sums, spread, staged)
    write = pltpu.make_async_copy(staged, payload, sem)
    write.start()
    local_solve(misfit, coef, values, factors_hbm, factors, tile_sems, current, one, two)
    odd = is_odd("wide")
    for c in range(3):
        for p in range(2):
            at = c * 16 + p * 8
            far[at : at + 8] = pick(odd, current[c, 2 + p], current[c, p])
            near[at : at + 8] = pick(odd, current[c, p], current[c, 2 + p])
    write.wait()


def fetch_tiles(factors_hbm, factors, sems):
    cols = [slice(1, 11) if a in (0, 5) else slice(0, 12) for a in range(6)]
    return [pltpu.make_async_copy(factors_hbm.at[a, cols[a]], factors.at[a, cols[a]], sems.at[a]) for a in range(6)]


def first_sweep(
    far,
    near,
    low,
    high,
    mine,
    agg,
    coarse_hbm,
    factors_hbm,
    coef,
    slots,
    payload,
    current,
    far_out,
    near_out,
    rim,
    coarse,
    coarse_sem,
    values,
    *scratch,
):
    coarse_fetch = pltpu.make_async_copy(coarse_hbm, coarse, coarse_sem)
    coarse_fetch.start()
    for fetch in fetch_tiles(factors_hbm, scratch[-3], scratch[-2]):
        fetch.start()
    odd = is_odd("wide")
    narrow_odd = is_odd("narrow")
    blank = jnp.zeros((ROWS, LANES), f32)

    def place(target, rows, at, width):
        target[...] = blank
        target[0:8] = rows
        a, b = low[at : at + width], high[at : at + width]
        target[8 : 8 + width] = pick(narrow_odd, a, b)
        target[16 - width : 16] = pick(narrow_odd, b, a)

    for f in range(FULL):
        for a in range(8):
            rows = rim_rows(odd, far, near, mine, f, f * 16, 2, a)
            target = values.at[f - 3, a] if 3 <= f < 6 else rim.at[f if f < 3 else 3, a]
            place(target, rows, (f * 8 + a) * 3, 3)
    for t in range(THIN):
        for a in range(1, 7):
            rows = rim_rows(odd, far, near, mine, FULL + t, FULL * 16 + t * 8, 1, a)
            target = coef.at[CENTRE if t == 0 else COUP + t - 1 if t < 10 else RHS + t - 10, a - 1]
            place(target, rows, FULL * 24 + (t * 6 + a - 1) * 2, 2)
    row = lax.broadcasted_iota(jnp.int32, (ROWS, LANES), 0)
    lane = lane_index((ROWS, LANES))
    low = lane < 64
    place_of = lax.axis_index("narrow")
    below, here, above = (32 * ((place_of + i) % 4) for i in (3, 0, 1))
    offset = jnp.where(row < 8, here, jnp.where(row < 12, above, below))
    inside = box_mask()
    for a in range(8):
        slots[a] = rim[3, a].astype(jnp.int32) + offset
    for a in range(1, 7):
        tx, ty = rim[0, a], rim[1, a]
        tz = jnp.where((lane % 64) < 63, rim[2, a], 0.0)
        txw = jnp.where(low, swap_halves(rim[0, a - 1]), swap_halves(tx))
        tys = shifted(ty, -1, 0)
        tzm = shifted(tz, -1, 1)
        centre = coef[CENTRE, a - 1] + (tx + txw + ty + tys + tz + tzm)
        coef[TX, a - 1] = tx
        coef[TXW, a - 1] = txw
        coef[TY, a - 1] = ty
        coef[TYS, a - 1] = tys
        coef[TZ, a - 1] = tz
        coef[TZM, a - 1] = tzm
        coef[CENTRE, a - 1] = centre
        for c in range(3):
            diagonal = jnp.where(inside, centre + coef[COUP + 4 * c, a - 1], 1.0)
            coef[INV + c, a - 1] = jnp.where(inside, 1.0 / diagonal, 0.0)
    solve_box(values, coef, agg, coarse, factors_hbm, payload, current, far_out, near_out, scratch, coarse_fetch)


def gather_values(current, far, near, low, high, part, slots, values):
    odd = is_odd("wide")
    narrow_odd = is_odd("narrow")
    total = part[...] + high[72:80]
    blank = jnp.zeros((2, LANES), f32)
    for a in range(8):
        block = 0 if a < 2 else 2 if a >= 6 else 1
        table = jnp.broadcast_to(total[block : block + 1], (8, LANES))
        for c in range(3):
            at = (c * 8 + a) * 3
            first, second = low[at : at + 3], high[at : at + 3]
            values[c, a, 0:8] = rim_rows(odd, far, near, current, c, c * 16, 2, a)
            values[c, a, 8:11] = pick(narrow_odd, first, second)
            values[c, a, 11:13] = blank
            values[c, a, 13:16] = pick(narrow_odd, second, first)
        for half in range(2):
            where = slots[a, 8 * half : 8 * half + 8]
            lifted = jnp.take_along_axis(table, where, axis=1, mode="promise_in_bounds")
            values[0, a, 8 * half : 8 * half + 8] += lifted


def next_sweep(
    current,
    far,
    near,
    low,
    high,
    part,
    slots,
    coef,
    agg,
    coarse,
    factors_hbm,
    payload,
    moved,
    far_out,
    near_out,
    values,
    *scratch,
):
    for fetch in fetch_tiles(factors_hbm, scratch[-3], scratch[-2]):
        fetch.start()
    gather_values(current, far, near, low, high, part, slots, values)
    solve_box(values, coef, agg, coarse, factors_hbm, payload, moved, far_out, near_out, scratch)


def last_misfit(current, far, near, low, high, part, slots, coef, iterate, residual, values):
    gather_values(current, far, near, low, high, part, slots, values)
    rolled = {}
    for a in range(2, 6):
        applied = operate_pair(values, coef, a, rolled)
        for c in range(3):
            iterate[c, a - 2] = values[c, a, 0:8]
            residual[c, a - 2] = (coef[RHS + c, a - 1] - applied[c])[0:8]


def local_solve(misfit, coef, values, factors_hbm, factors, sems, moved, one, two):
    fetches = fetch_tiles(factors_hbm, factors, sems)
    own_cols = list(range(8))
    row8 = lax.broadcasted_iota(jnp.int32, (24, LANES), 0) % 8

    def tiles(values, pair, cols, half):
        scaled = [coef[INV + c, pair - 1, 8 * half : 8 * half + 8] * values[c] for c in range(3)]
        left = jnp.concatenate(scaled, axis=0).astype(jnp.bfloat16)
        total = jnp.zeros((24, LANES), f32)
        for y in cols:
            product = lax.dot_general(
                left, factors[pair - 1, y + 2], (((1,), (1,)), ((), ())), preferred_element_type=f32
            )
            total = jnp.where(row8 == y % 8, product, total)
        return [total[8 * c : 8 * c + 8] for c in range(3)]

    blank = jnp.zeros((ROWS, LANES), f32)
    for c in range(3):
        for ref in (one, two):
            ref[c, 0] = blank
            ref[c, 7] = blank
    for a in range(1, 7):
        edge = a in (1, 6)
        if a in (1, 4):
            for fetch in fetches[a - 1 : a + 2]:
                fetch.wait()
        for half, cols in ((0, own_cols), (1, [8, -1] if edge else [8, 9, -2, -1])):
            part = tiles([misfit[c, a, 8 * half : 8 * half + 8] for c in range(3)], a, cols, half)
            for c in range(3):
                one[c, a, 8 * half : 8 * half + 8] = part[c]
    rolled = {}
    for a in range(1, 7):
        edge = a in (1, 6)
        applied = operate_pair(one, coef, a, rolled)
        left = [misfit[c, a] - applied[c] for c in range(3)]
        for half, cols in ((0, own_cols), (1, [] if edge else [8, -1])):
            if not cols:
                for c in range(3):
                    two[c, a, 8:16] = one[c, a, 8:16]
                continue
            part = tiles([v[8 * half : 8 * half + 8] for v in left], a, cols, half)
            for c in range(3):
                two[c, a, 8 * half : 8 * half + 8] = one[c, a, 8 * half : 8 * half + 8] + part[c]
    rolled = {}
    for a in range(2, 6):
        applied = operate_pair(two, coef, a, rolled)
        part = tiles([(misfit[c, a] - applied[c])[0:8] for c in range(3)], a, own_cols, 0)
        for c in range(3):
            moved[c, a - 2] = values[c, a, 0:8] + (two[c, a, 0:8] + part[c])


def call(body, outs, scratch, operands, in_hbm=(), out_hbm=(), flops=1000000):
    vmem = pl.BlockSpec(memory_space=pltpu.VMEM)
    hbm = pl.BlockSpec(memory_space=pltpu.HBM)
    operands = [pltpu.with_memory_space_constraint(x, pltpu.HBM) if i in in_hbm else x for i, x in enumerate(operands)]
    return pl.pallas_call(
        body,
        out_shape=[
            pltpu.HBM(shape, dtype) if i in out_hbm else jax.ShapeDtypeStruct(shape, dtype)
            for i, (shape, dtype) in enumerate(outs)
        ],
        in_specs=[hbm if i in in_hbm else vmem for i in range(len(operands))],
        out_specs=[hbm if i in out_hbm else vmem for i in range(len(outs))],
        scratch_shapes=scratch,
        compiler_params=pltpu.CompilerParams(vmem_limit_bytes=VMEM_LIMIT),
        cost_estimate=pl.CostEstimate(flops=flops, bytes_accessed=0, transcendentals=0),
    )(*operands)


def swaps(axis, far, near):
    count = lax.axis_size(axis)
    far = lax.ppermute(far, axis, [(i, (i + (1 if i % 2 else -1)) % count) for i in range(count)])
    near = lax.ppermute(near, axis, [(i, i ^ 1) for i in range(count)])
    return far, near


def per_device(
    rhs, start, trans, accum, coupling, well_cells, well_index, agg_map, tile_factors, coarse_inverse
):
    devices = lax.axis_size("wide") * lax.axis_size("narrow")
    members = devices // 2
    groups = [[4 * w + n for w in range(devices // 4) for n in (parity, parity + 2)] for parity in range(2)]
    dma = pltpu.SemaphoreType.DMA
    own = ((3, 4, 8, LANES), f32)
    box = (3, PAIRS, ROWS, LANES)
    wide_type = ((48, LANES), f32)
    narrow_type = ((72, LANES), f32)
    payload_type = ((members * 3, LANES), f32)
    scratch = [
        pltpu.VMEM(box, f32),
        pltpu.VMEM(box, f32),
        pltpu.VMEM((AGG_LOC, LANES), f32),
        pltpu.VMEM((devices // 4 + 8, LANES), f32),
        pltpu.VMEM(payload_type[0], f32),
        pltpu.VMEM(box, f32),
        pltpu.VMEM(box, f32),
        pltpu.VMEM(tile_factors.shape, tile_factors.dtype),
        dma((6,)),
        dma,
    ]

    mine, agg, far, near = call(
        add_wells_and_pack,
        [((FULL + THIN, 4, 8, LANES), f32), ((4, 8, LANES), f32)] + [((WIDE_ROWS, LANES), f32)] * 2,
        [
            pltpu.VMEM((1, 64), jnp.int32),
            pltpu.VMEM((1, 64), f32),
            pltpu.VMEM((4, 8, LANES), f32),
            pltpu.VMEM((4, 8, LANES), jnp.int32),
            dma((8,)),
        ],
        [
            well_cells.reshape(1, -1),
            well_index.reshape(1, -1),
            accum,
            trans,
            start,
            agg_map,
            coupling.reshape((9,) + accum.shape),
            rhs,
        ],
        in_hbm=range(8),
    )
    far, near = swaps("wide", far, near)
    low, high = call(pack_narrow, [((NARROW_ROWS, LANES), f32)] * 2, [], [far, near, mine])
    low, high = swaps("narrow", low, high)
    coef, slots, payload, current, far, near = call(
        first_sweep,
        [((N_COEF, 6, ROWS, LANES), f32), ((PAIRS, ROWS, LANES), jnp.int32), payload_type, own, wide_type, wide_type],
        [pltpu.VMEM((4, PAIRS, ROWS, LANES), f32), pltpu.VMEM(coarse_inverse.shape, f32), dma] + scratch,
        [far, near, low, high, mine, agg, coarse_inverse, tile_factors],
        in_hbm=(6, 7),
        out_hbm=(2,),
    )
    for sweep in range(SWEEPS):
        blocks = payload.reshape(members, 1, 3 * LANES)
        received = lax.all_to_all(blocks, ("wide", "narrow"), 0, 0, axis_index_groups=groups).reshape(payload_type[0])
        far, near = swaps("wide", far, near)
        low, high, part = call(
            pack_current, [narrow_type, ((80, LANES), f32), ((8, LANES), f32)], [], [current, far, near, received]
        )
        low, high = swaps("narrow", low, high)
        known = [current, far, near, low, high, part, slots, coef]
        if sweep < SWEEPS - 1:
            payload, current, far, near = call(
                next_sweep,
                [payload_type, own, wide_type, wide_type],
                scratch,
                known + [agg, coarse_inverse, tile_factors],
                in_hbm=(10,),
                out_hbm=(0,),
            )
        else:
            iterate, residual = call(last_misfit, [own, own], [pltpu.VMEM(box, f32)], known)
    return iterate, residual


def solution(mesh):
    return jax.shard_map(
        per_device,
        mesh=mesh,
        in_specs=(
            P(None, "wide", "narrow", None),
            P(None, "wide", "narrow", None),
            P(None, "wide", "narrow", None),
            P("wide", "narrow", None),
            P(None, None, "wide", "narrow", None),
            P("wide", "narrow", None),
            P("wide", "narrow", None),
            P("wide", "narrow", None),
            P("wide", "narrow", None, None),
            P(("wide", "narrow"), None),
        ),
        out_specs=(P(None, "wide", "narrow", None), P(None, "wide", "narrow", None)),
        check_vma=False,
    )
```

```python
import jax
import jax.numpy as jnp
from jax import lax
from jax.experimental import pallas as pl
from jax.experimental.pallas import tpu as pltpu
from jax.sharding import PartitionSpec as P


AGG_LOC = 32
SWEEPS = 3
PAIRS = 8
ROWS = 16
LANES = 128
FULL = 7
THIN = 13
WIDE_ROWS = FULL * 16 + THIN * 8
NARROW_ROWS = FULL * 24 + THIN * 12
TX, TXW, TY, TYS, TZ, TZM, CENTRE, COUP, INV, RHS = 0, 1, 2, 3, 4, 5, 6, 7, 16, 19
N_COEF = 22
VMEM_LIMIT = 24 * 1024 * 1024

f32 = jnp.float32


def swap_halves(v):
    return pltpu.roll(v, 64, axis=1)


def shifted(v, offset, axis):
    return pltpu.roll(v, (-offset) % v.shape[axis], axis=axis)


def lane_index(shape):
    return lax.broadcasted_iota(jnp.int32, shape, 1)


def box_mask():
    row = lax.broadcasted_iota(jnp.int32, (ROWS, LANES), 0)
    return (row < 10) | (row >= 14)


def operate_pair(values, coef, pair, rolled):
    low = lane_index((ROWS, LANES)) < 64
    mids = [values[c, pair] for c in range(3)]

    def halves(c, p):
        if (c, p) not in rolled:
            rolled[c, p] = swap_halves(values[c, p])
        return rolled[c, p]

    out = []
    for c in range(3):
        v = mids[c]
        own = halves(c, pair)
        inflow = coef[TX, pair - 1] * jnp.where(low, own, halves(c, pair + 1))
        inflow += coef[TXW, pair - 1] * jnp.where(low, halves(c, pair - 1), own)
        inflow += coef[TY, pair - 1] * shifted(v, 1, 0)
        inflow += coef[TYS, pair - 1] * shifted(v, -1, 0)
        inflow += coef[TZ, pair - 1] * shifted(v, 1, 1)
        inflow += coef[TZM, pair - 1] * shifted(v, -1, 1)
        total = coef[CENTRE, pair - 1] * v
        for b in range(3):
            total += coef[COUP + 3 * c + b, pair - 1] * mids[b]
        out.append(total - inflow)
    return out


def pick(odd, when_odd, when_even):
    return jnp.where(odd, when_odd, when_even)


def is_odd(axis):
    return lax.axis_index(axis) % 2 == 1


def add_wells_and_pack(
    cells_in,
    index_in,
    accum,
    trans,
    start,
    agg,
    coupling,
    rhs,
    mine,
    agg_float,
    far,
    near,
    cells,
    index,
    accum_in,
    agg_in,
    sems,
):
    sources = (
        (cells_in, cells),
        (index_in, index),
        (agg, agg_in),
        (accum, accum_in),
        (trans, mine.at[0:3]),
        (start, mine.at[3:6]),
        (coupling, mine.at[8:17]),
        (rhs, mine.at[17:20]),
    )
    copies = [pltpu.make_async_copy(source, target, sems.at[i]) for i, (source, target) in enumerate(sources)]
    for copy in copies:
        copy.start()
    for copy in copies[:2]:
        copy.wait()
    where_row = (lax.broadcasted_iota(jnp.int32, (32, 64), 0) == cells[...] // LANES).astype(f32)
    lane_no = lax.broadcasted_iota(jnp.int32, (LANES, 64), 0)
    share = jnp.where(lane_no == cells[...] % LANES, index[...], 0.0)
    added = lax.dot_general(
        where_row, share, (((1,), (1,)), ((), ())), precision=lax.Precision.HIGHEST, preferred_element_type=f32
    )
    for copy in copies[2:]:
        copy.wait()
    for p in range(4):
        mine[7, p] = accum_in[p] + added[8 * p : 8 * p + 8]
        mine[6, p] = agg_in[p].astype(f32)
        agg_float[p] = agg_in[p].astype(f32)
    odd = is_odd("wide")
    for f in range(FULL):
        for p in range(2):
            east, west = mine[f, 2 + p], mine[f, p]
            at = f * 16 + p * 8
            far[at : at + 8] = pick(odd, east, west)
            near[at : at + 8] = pick(odd, west, east)
    for t in range(THIN):
        east, west = mine[FULL + t, 3], mine[FULL + t, 0]
        at = FULL * 16 + t * 8
        far[at : at + 8] = pick(odd, east, west)
        near[at : at + 8] = pick(odd, west, east)


def rim_rows(odd, far, near, mine, channel_no, at, depth, pair):
    if pair < 2:
        at += 8 * pair if depth == 2 else 0
        return pick(odd, near[at : at + 8], far[at : at + 8])
    if pair >= 6:
        at += 8 * (pair - 6) if depth == 2 else 0
        return pick(odd, far[at : at + 8], near[at : at + 8])
    return mine[channel_no, pair - 2]


def pack_narrow(far, near, mine, low, high):
    odd = is_odd("wide")
    narrow_odd = is_odd("narrow")
    for f in range(FULL):
        for a in range(8):
            v = rim_rows(odd, far, near, mine, f, f * 16, 2, a)
            at = (f * 8 + a) * 3
            low[at : at + 3] = pick(narrow_odd, v[5:8], v[0:3])
            high[at : at + 3] = pick(narrow_odd, v[0:3], v[5:8])
    for t in range(THIN):
        for a in range(1, 7):
            v = rim_rows(odd, far, near, mine, FULL + t, FULL * 16 + t * 8, 1, a)
            at = FULL * 24 + (t * 6 + a - 1) * 2
            low[at : at + 2] = pick(narrow_odd, v[6:8], v[0:2])
            high[at : at + 2] = pick(narrow_odd, v[0:2], v[6:8])


def pack_current(current, far, near, received, low, high, part):
    total = received[0:24]
    for i in range(24, received.shape[0], 24):
        total += received[i : i + 24]
    block_of = lax.broadcasted_iota(jnp.int32, (24, LANES), 0) % 3
    part[...] = jnp.zeros((8, LANES), f32)
    for k in range(3):
        part[k : k + 1, :] = jnp.sum(jnp.where(block_of == k, total, 0.0), axis=0, keepdims=True)
    high[72:80] = part[...]
    odd = is_odd("wide")
    narrow_odd = is_odd("narrow")
    for c in range(3):
        for a in range(8):
            v = rim_rows(odd, far, near, current, c, c * 16, 2, a)
            at = (c * 8 + a) * 3
            low[at : at + 3] = pick(narrow_odd, v[5:8], v[0:3])
            high[at : at + 3] = pick(narrow_odd, v[0:3], v[5:8])


def coarse_part(misfit0, agg, coarse, sums, spread, staged):
    for g in range(AGG_LOC):
        picked = jnp.where(agg[0] == float(g), misfit0[0], 0.0)
        for p in range(1, 4):
            picked += jnp.where(agg[p] == float(g), misfit0[p], 0.0)
        sums[g : g + 1, :] = jnp.sum(picked, axis=0, keepdims=True)
    weight = jnp.broadcast_to(jnp.sum(sums[...], axis=1, keepdims=True), (AGG_LOC, LANES))
    count = coarse.shape[1] // LANES
    for w in range(count):
        row = jnp.sum(coarse[:, w * LANES : (w + 1) * LANES] * weight, axis=0, keepdims=True)
        spread[w + 1 : w + 2, :] = row
    spread[0:1, :] = spread[count : count + 1, :]
    spread[count + 1 : count + 2, :] = spread[1:2, :]
    for w in range(count):
        rows = spread[w : w + 3, :]
        for half in range(2):
            at = 3 * (2 * w + half)
            staged[at : at + 3, :] = rows


def solve_box(values, coef, agg, coarse, factors_hbm, payload, current, far, near, scratch, coarse_fetch=None):
    misfit, sums, spread, staged, one, two, factors, tile_sems, sem = scratch
    inside = box_mask()
    rolled = {}
    for c in range(3):
        misfit[c, 0] = jnp.zeros((ROWS, LANES), f32)
        misfit[c, 7] = jnp.zeros((ROWS, LANES), f32)
    for a in range(1, 7):
        applied = operate_pair(values, coef, a, rolled)
        for c in range(3):
            misfit[c, a] = jnp.where(inside, coef[RHS + c, a - 1] - applied[c], 0.0)
    write = pltpu.make_async_copy(staged, payload, sem)

    def coarse_stretch():
        coarse_part([misfit[0, a, 0:8] for a in range(2, 6)], agg, coarse, sums, spread, staged)
        write.start()

    if coarse_fetch is not None:
        coarse_fetch.wait()
    local_solve(misfit, coef, values, factors_hbm, factors, tile_sems, current, one, two, coarse_stretch)
    odd = is_odd("wide")
    for c in range(3):
        for p in range(2):
            at = c * 16 + p * 8
            far[at : at + 8] = pick(odd, current[c, 2 + p], current[c, p])
            near[at : at + 8] = pick(odd, current[c, p], current[c, 2 + p])
    write.wait()


def fetch_tiles(factors_hbm, factors, sems):
    cols = [slice(1, 11) if a in (0, 5) else slice(0, 12) for a in range(6)]
    return [pltpu.make_async_copy(factors_hbm.at[a, cols[a]], factors.at[a, cols[a]], sems.at[a]) for a in range(6)]


def first_sweep(
    far,
    near,
    low,
    high,
    mine,
    agg,
    coarse_hbm,
    factors_hbm,
    coef,
    slots,
    payload,
    current,
    far_out,
    near_out,
    rim,
    coarse,
    coarse_sem,
    values,
    *scratch,
):
    coarse_fetch = pltpu.make_async_copy(coarse_hbm, coarse, coarse_sem)
    coarse_fetch.start()
    for fetch in fetch_tiles(factors_hbm, scratch[-3], scratch[-2]):
        fetch.start()
    odd = is_odd("wide")
    narrow_odd = is_odd("narrow")
    blank = jnp.zeros((ROWS, LANES), f32)

    def place(target, rows, at, width):
        target[...] = blank
        target[0:8] = rows
        a, b = low[at : at + width], high[at : at + width]
        target[8 : 8 + width] = pick(narrow_odd, a, b)
        target[16 - width : 16] = pick(narrow_odd, b, a)

    for f in range(FULL):
        for a in range(8):
            rows = rim_rows(odd, far, near, mine, f, f * 16, 2, a)
            target = values.at[f - 3, a] if 3 <= f < 6 else rim.at[f if f < 3 else 3, a]
            place(target, rows, (f * 8 + a) * 3, 3)
    for t in range(THIN):
        for a in range(1, 7):
            rows = rim_rows(odd, far, near, mine, FULL + t, FULL * 16 + t * 8, 1, a)
            target = coef.at[CENTRE if t == 0 else COUP + t - 1 if t < 10 else RHS + t - 10, a - 1]
            place(target, rows, FULL * 24 + (t * 6 + a - 1) * 2, 2)
    row = lax.broadcasted_iota(jnp.int32, (ROWS, LANES), 0)
    lane = lane_index((ROWS, LANES))
    low = lane < 64
    place_of = lax.axis_index("narrow")
    below, here, above = (32 * ((place_of + i) % 4) for i in (3, 0, 1))
    offset = jnp.where(row < 8, here, jnp.where(row < 12, above, below))
    inside = box_mask()
    for a in range(8):
        slots[a] = rim[3, a].astype(jnp.int32) + offset
    for a in range(1, 7):
        tx, ty = rim[0, a], rim[1, a]
        tz = jnp.where((lane % 64) < 63, rim[2, a], 0.0)
        txw = jnp.where(low, swap_halves(rim[0, a - 1]), swap_halves(tx))
        tys = shifted(ty, -1, 0)
        tzm = shifted(tz, -1, 1)
        centre = coef[CENTRE, a - 1] + (tx + txw + ty + tys + tz + tzm)
        coef[TX, a - 1] = tx
        coef[TXW, a - 1] = txw
        coef[TY, a - 1] = ty
        coef[TYS, a - 1] = tys
        coef[TZ, a - 1] = tz
        coef[TZM, a - 1] = tzm
        coef[CENTRE, a - 1] = centre
        for c in range(3):
            diagonal = jnp.where(inside, centre + coef[COUP + 4 * c, a - 1], 1.0)
            coef[INV + c, a - 1] = jnp.where(inside, 1.0 / diagonal, 0.0)
    solve_box(values, coef, agg, coarse, factors_hbm, payload, current, far_out, near_out, scratch, coarse_fetch)


def gather_values(current, far, near, low, high, part, slots, values):
    odd = is_odd("wide")
    narrow_odd = is_odd("narrow")
    total = part[...] + high[72:80]
    blank = jnp.zeros((2, LANES), f32)
    for a in range(8):
        block = 0 if a < 2 else 2 if a >= 6 else 1
        table = jnp.broadcast_to(total[block : block + 1], (8, LANES))
        for c in range(3):
            at = (c * 8 + a) * 3
            first, second = low[at : at + 3], high[at : at + 3]
            values[c, a, 0:8] = rim_rows(odd, far, near, current, c, c * 16, 2, a)
            values[c, a, 8:11] = pick(narrow_odd, first, second)
            values[c, a, 11:13] = blank
            values[c, a, 13:16] = pick(narrow_odd, second, first)
        for half in range(2):
            where = slots[a, 8 * half : 8 * half + 8]
            lifted = jnp.take_along_axis(table, where, axis=1, mode="promise_in_bounds")
            values[0, a, 8 * half : 8 * half + 8] += lifted


def next_sweep(
    current,
    far,
    near,
    low,
    high,
    part,
    slots,
    coef,
    agg,
    coarse,
    factors_hbm,
    payload,
    moved,
    far_out,
    near_out,
    values,
    *scratch,
):
    for fetch in fetch_tiles(factors_hbm, scratch[-3], scratch[-2]):
        fetch.start()
    gather_values(current, far, near, low, high, part, slots, values)
    solve_box(values, coef, agg, coarse, factors_hbm, payload, moved, far_out, near_out, scratch)


def last_misfit(current, far, near, low, high, part, slots, coef, iterate, residual, values):
    gather_values(current, far, near, low, high, part, slots, values)
    rolled = {}
    for a in range(2, 6):
        applied = operate_pair(values, coef, a, rolled)
        for c in range(3):
            iterate[c, a - 2] = values[c, a, 0:8]
            residual[c, a - 2] = (coef[RHS + c, a - 1] - applied[c])[0:8]


def local_solve(misfit, coef, values, factors_hbm, factors, sems, moved, one, two, beside):
    fetches = fetch_tiles(factors_hbm, factors, sems)
    own_cols = list(range(8))
    row8 = lax.broadcasted_iota(jnp.int32, (24, LANES), 0) % 8

    def tiles(values, pair, cols, half):
        scaled = [coef[INV + c, pair - 1, 8 * half : 8 * half + 8] * values[c] for c in range(3)]
        left = jnp.concatenate(scaled, axis=0).astype(jnp.bfloat16)
        total = jnp.zeros((24, LANES), f32)
        for y in cols:
            product = lax.dot_general(
                left, factors[pair - 1, y + 2], (((1,), (1,)), ((), ())), preferred_element_type=f32
            )
            total = jnp.where(row8 == y % 8, product, total)
        return [total[8 * c : 8 * c + 8] for c in range(3)]

    blank = jnp.zeros((ROWS, LANES), f32)
    for c in range(3):
        for ref in (one, two):
            ref[c, 0] = blank
            ref[c, 7] = blank
    for a in range(1, 7):
        edge = a in (1, 6)
        if a in (1, 4):
            for fetch in fetches[a - 1 : a + 2]:
                fetch.wait()
        for half, cols in ((0, own_cols), (1, [8, -1] if edge else [8, 9, -2, -1])):
            part = tiles([misfit[c, a, 8 * half : 8 * half + 8] for c in range(3)], a, cols, half)
            for c in range(3):
                one[c, a, 8 * half : 8 * half + 8] = part[c]
        if a == 3:
            beside()
    rolled = {}
    for a in range(1, 7):
        edge = a in (1, 6)
        applied = operate_pair(one, coef, a, rolled)
        left = [misfit[c, a] - applied[c] for c in range(3)]
        for half, cols in ((0, own_cols), (1, [] if edge else [8, -1])):
            if not cols:
                for c in range(3):
                    two[c, a, 8:16] = one[c, a, 8:16]
                continue
            part = tiles([v[8 * half : 8 * half + 8] for v in left], a, cols, half)
            for c in range(3):
                two[c, a, 8 * half : 8 * half + 8] = one[c, a, 8 * half : 8 * half + 8] + part[c]
    rolled = {}
    for a in range(2, 6):
        applied = operate_pair(two, coef, a, rolled)
        part = tiles([(misfit[c, a] - applied[c])[0:8] for c in range(3)], a, own_cols, 0)
        for c in range(3):
            moved[c, a - 2] = values[c, a, 0:8] + (two[c, a, 0:8] + part[c])


def call(body, outs, scratch, operands, in_hbm=(), out_hbm=(), flops=1000000):
    vmem = pl.BlockSpec(memory_space=pltpu.VMEM)
    hbm = pl.BlockSpec(memory_space=pltpu.HBM)
    operands = [pltpu.with_memory_space_constraint(x, pltpu.HBM) if i in in_hbm else x for i, x in enumerate(operands)]
    return pl.pallas_call(
        body,
        out_shape=[
            pltpu.HBM(shape, dtype) if i in out_hbm else jax.ShapeDtypeStruct(shape, dtype)
            for i, (shape, dtype) in enumerate(outs)
        ],
        in_specs=[hbm if i in in_hbm else vmem for i in range(len(operands))],
        out_specs=[hbm if i in out_hbm else vmem for i in range(len(outs))],
        scratch_shapes=scratch,
        compiler_params=pltpu.CompilerParams(vmem_limit_bytes=VMEM_LIMIT),
        cost_estimate=pl.CostEstimate(flops=flops, bytes_accessed=0, transcendentals=0),
    )(*operands)


def swaps(axis, far, near):
    count = lax.axis_size(axis)
    far = lax.ppermute(far, axis, [(i, (i + (1 if i % 2 else -1)) % count) for i in range(count)])
    near = lax.ppermute(near, axis, [(i, i ^ 1) for i in range(count)])
    return far, near


def per_device(
    rhs, start, trans, accum, coupling, well_cells, well_index, agg_map, tile_factors, coarse_inverse
):
    devices = lax.axis_size("wide") * lax.axis_size("narrow")
    members = devices // 2
    groups = [[4 * w + n for w in range(devices // 4) for n in (parity, parity + 2)] for parity in range(2)]
    dma = pltpu.SemaphoreType.DMA
    own = ((3, 4, 8, LANES), f32)
    box = (3, PAIRS, ROWS, LANES)
    wide_type = ((48, LANES), f32)
    narrow_type = ((72, LANES), f32)
    payload_type = ((members * 3, LANES), f32)
    scratch = [
        pltpu.VMEM(box, f32),
        pltpu.VMEM(box, f32),
        pltpu.VMEM((AGG_LOC, LANES), f32),
        pltpu.VMEM((devices // 4 + 8, LANES), f32),
        pltpu.VMEM(payload_type[0], f32),
        pltpu.VMEM(box, f32),
        pltpu.VMEM(box, f32),
        pltpu.VMEM(tile_factors.shape, tile_factors.dtype),
        dma((6,)),
        dma,
    ]

    mine, agg, far, near = call(
        add_wells_and_pack,
        [((FULL + THIN, 4, 8, LANES), f32), ((4, 8, LANES), f32)] + [((WIDE_ROWS, LANES), f32)] * 2,
        [
            pltpu.VMEM((1, 64), jnp.int32),
            pltpu.VMEM((1, 64), f32),
            pltpu.VMEM((4, 8, LANES), f32),
            pltpu.VMEM((4, 8, LANES), jnp.int32),
            dma((8,)),
        ],
        [
            well_cells.reshape(1, -1),
            well_index.reshape(1, -1),
            accum,
            trans,
            start,
            agg_map,
            coupling.reshape((9,) + accum.shape),
            rhs,
        ],
        in_hbm=range(8),
    )
    far, near = swaps("wide", far, near)
    low, high = call(pack_narrow, [((NARROW_ROWS, LANES), f32)] * 2, [], [far, near, mine])
    low, high = swaps("narrow", low, high)
    coef, slots, payload, current, far, near = call(
        first_sweep,
        [((N_COEF, 6, ROWS, LANES), f32), ((PAIRS, ROWS, LANES), jnp.int32), payload_type, own, wide_type, wide_type],
        [pltpu.VMEM((4, PAIRS, ROWS, LANES), f32), pltpu.VMEM(coarse_inverse.shape, f32), dma] + scratch,
        [far, near, low, high, mine, agg, coarse_inverse, tile_factors],
        in_hbm=(6, 7),
        out_hbm=(2,),
    )
    for sweep in range(SWEEPS):
        blocks = payload.reshape(members, 1, 3 * LANES)
        received = lax.all_to_all(blocks, ("wide", "narrow"), 0, 0, axis_index_groups=groups).reshape(payload_type[0])
        far, near = swaps("wide", far, near)
        low, high, part = call(
            pack_current, [narrow_type, ((80, LANES), f32), ((8, LANES), f32)], [], [current, far, near, received]
        )
        low, high = swaps("narrow", low, high)
        known = [current, far, near, low, high, part, slots, coef]
        if sweep < SWEEPS - 1:
            payload, current, far, near = call(
                next_sweep,
                [payload_type, own, wide_type, wide_type],
                scratch,
                known + [agg, coarse_inverse, tile_factors],
                in_hbm=(10,),
                out_hbm=(0,),
            )
        else:
            iterate, residual = call(last_misfit, [own, own], [pltpu.VMEM(box, f32)], known)
    return iterate, residual


def solution(mesh):
    return jax.shard_map(
        per_device,
        mesh=mesh,
        in_specs=(
            P(None, "wide", "narrow", None),
            P(None, "wide", "narrow", None),
            P(None, "wide", "narrow", None),
            P("wide", "narrow", None),
            P(None, None, "wide", "narrow", None),
            P("wide", "narrow", None),
            P("wide", "narrow", None),
            P("wide", "narrow", None),
            P("wide", "narrow", None, None),
            P(("wide", "narrow"), None),
        ),
        out_specs=(P(None, "wide", "narrow", None), P(None, "wide", "narrow", None)),
        check_vma=False,
    )
```

```python
import jax
import jax.numpy as jnp
from jax import lax
from jax.experimental import pallas as pl
from jax.experimental.pallas import tpu as pltpu
from jax.sharding import PartitionSpec as P


AGG_LOC = 32
SWEEPS = 3
PAIRS = 8
ROWS = 16
LANES = 128
FULL = 7
THIN = 13
WIDE_ROWS = FULL * 16 + THIN * 8
NARROW_ROWS = FULL * 24 + THIN * 12
TX, TXW, TY, TYS, TZ, TZM, CENTRE, COUP, INV, RHS = 0, 1, 2, 3, 4, 5, 6, 7, 16, 19
N_COEF = 22
VMEM_LIMIT = 24 * 1024 * 1024

f32 = jnp.float32


def swap_halves(v):
    return pltpu.roll(v, 64, axis=1)


def shifted(v, offset, axis):
    return pltpu.roll(v, (-offset) % v.shape[axis], axis=axis)


def lane_index(shape):
    return lax.broadcasted_iota(jnp.int32, shape, 1)


def box_mask():
    row = lax.broadcasted_iota(jnp.int32, (ROWS, LANES), 0)
    return (row < 10) | (row >= 14)


def operate_pair(values, coef, pair, rolled):
    low = lane_index((ROWS, LANES)) < 64
    mids = [values[c, pair] for c in range(3)]

    def halves(c, p):
        if (c, p) not in rolled:
            rolled[c, p] = swap_halves(values[c, p])
        return rolled[c, p]

    out = []
    for c in range(3):
        v = mids[c]
        own = halves(c, pair)
        inflow = coef[TX, pair - 1] * jnp.where(low, own, halves(c, pair + 1))
        inflow += coef[TXW, pair - 1] * jnp.where(low, halves(c, pair - 1), own)
        inflow += coef[TY, pair - 1] * shifted(v, 1, 0)
        inflow += coef[TYS, pair - 1] * shifted(v, -1, 0)
        inflow += coef[TZ, pair - 1] * shifted(v, 1, 1)
        inflow += coef[TZM, pair - 1] * shifted(v, -1, 1)
        total = coef[CENTRE, pair - 1] * v
        for b in range(3):
            total += coef[COUP + 3 * c + b, pair - 1] * mids[b]
        out.append(total - inflow)
    return out


def pick(odd, when_odd, when_even):
    return jnp.where(odd, when_odd, when_even)


def is_odd(axis):
    return lax.axis_index(axis) % 2 == 1


def add_wells_and_pack(
    cells_in,
    index_in,
    accum,
    trans,
    start,
    agg,
    coupling,
    rhs,
    mine,
    agg_float,
    far,
    near,
    cells,
    index,
    accum_in,
    agg_in,
    sems,
):
    sources = (
        (cells_in, cells),
        (index_in, index),
        (agg, agg_in),
        (accum, accum_in),
        (trans, mine.at[0:3]),
        (start, mine.at[3:6]),
        (coupling, mine.at[8:17]),
        (rhs, mine.at[17:20]),
    )
    copies = [pltpu.make_async_copy(source, target, sems.at[i]) for i, (source, target) in enumerate(sources)]
    for copy in copies:
        copy.start()
    for copy in copies[:2]:
        copy.wait()
    where_row = (lax.broadcasted_iota(jnp.int32, (32, 64), 0) == cells[...] // LANES).astype(f32)
    lane_no = lax.broadcasted_iota(jnp.int32, (LANES, 64), 0)
    share = jnp.where(lane_no == cells[...] % LANES, index[...], 0.0)
    added = lax.dot_general(
        where_row, share, (((1,), (1,)), ((), ())), precision=lax.Precision.HIGHEST, preferred_element_type=f32
    )
    for copy in copies[2:]:
        copy.wait()
    for p in range(4):
        mine[7, p] = accum_in[p] + added[8 * p : 8 * p + 8]
        mine[6, p] = agg_in[p].astype(f32)
        agg_float[p] = agg_in[p].astype(f32)
    odd = is_odd("wide")
    for f in range(FULL):
        for p in range(2):
            east, west = mine[f, 2 + p], mine[f, p]
            at = f * 16 + p * 8
            far[at : at + 8] = pick(odd, east, west)
            near[at : at + 8] = pick(odd, west, east)
    for t in range(THIN):
        east, west = mine[FULL + t, 3], mine[FULL + t, 0]
        at = FULL * 16 + t * 8
        far[at : at + 8] = pick(odd, east, west)
        near[at : at + 8] = pick(odd, west, east)


def rim_rows(odd, far, near, mine, channel_no, at, depth, pair):
    if pair < 2:
        at += 8 * pair if depth == 2 else 0
        return pick(odd, near[at : at + 8], far[at : at + 8])
    if pair >= 6:
        at += 8 * (pair - 6) if depth == 2 else 0
        return pick(odd, far[at : at + 8], near[at : at + 8])
    return mine[channel_no, pair - 2]


def pack_narrow(far, near, mine, low, high):
    odd = is_odd("wide")
    narrow_odd = is_odd("narrow")
    for f in range(FULL):
        for a in range(8):
            v = rim_rows(odd, far, near, mine, f, f * 16, 2, a)
            at = (f * 8 + a) * 3
            low[at : at + 3] = pick(narrow_odd, v[5:8], v[0:3])
            high[at : at + 3] = pick(narrow_odd, v[0:3], v[5:8])
    for t in range(THIN):
        for a in range(1, 7):
            v = rim_rows(odd, far, near, mine, FULL + t, FULL * 16 + t * 8, 1, a)
            at = FULL * 24 + (t * 6 + a - 1) * 2
            low[at : at + 2] = pick(narrow_odd, v[6:8], v[0:2])
            high[at : at + 2] = pick(narrow_odd, v[0:2], v[6:8])


def group_sums(received, part):
    total = received[0:24]
    for i in range(24, received.shape[0], 24):
        total += received[i : i + 24]
    block_of = lax.broadcasted_iota(jnp.int32, (24, LANES), 0) % 3
    part[...] = jnp.zeros((8, LANES), f32)
    for k in range(3):
        part[k : k + 1, :] = jnp.sum(jnp.where(block_of == k, total, 0.0), axis=0, keepdims=True)


def pack_current(current, far, near, received, low, high, part):
    group_sums(received, part)
    high[72:80] = part[...]
    odd = is_odd("wide")
    narrow_odd = is_odd("narrow")
    for c in range(3):
        for a in range(8):
            v = rim_rows(odd, far, near, current, c, c * 16, 2, a)
            at = (c * 8 + a) * 3
            low[at : at + 3] = pick(narrow_odd, v[5:8], v[0:3])
            high[at : at + 3] = pick(narrow_odd, v[0:3], v[5:8])


def coarse_part(misfit0, agg, coarse, sums, spread, staged):
    for g in range(AGG_LOC):
        picked = jnp.where(agg[0] == float(g), misfit0[0], 0.0)
        for p in range(1, 4):
            picked += jnp.where(agg[p] == float(g), misfit0[p], 0.0)
        sums[g : g + 1, :] = jnp.sum(picked, axis=0, keepdims=True)
    weight = jnp.broadcast_to(jnp.sum(sums[...], axis=1, keepdims=True), (AGG_LOC, LANES))
    count = coarse.shape[1] // LANES
    for w in range(count):
        row = jnp.sum(coarse[:, w * LANES : (w + 1) * LANES] * weight, axis=0, keepdims=True)
        spread[w + 1 : w + 2, :] = row
    spread[0:1, :] = spread[count : count + 1, :]
    spread[count + 1 : count + 2, :] = spread[1:2, :]
    for w in range(count):
        rows = spread[w : w + 3, :]
        for half in range(2):
            at = 3 * (2 * w + half)
            staged[at : at + 3, :] = rows


def solve_box(values, coef, agg, coarse, factors_hbm, payload, current, far, near, scratch, coarse_fetch=None):
    misfit, sums, spread, staged, one, two, factors, tile_sems, sem = scratch
    inside = box_mask()
    rolled = {}
    for c in range(3):
        misfit[c, 0] = jnp.zeros((ROWS, LANES), f32)
        misfit[c, 7] = jnp.zeros((ROWS, LANES), f32)
    for a in range(1, 7):
        applied = operate_pair(values, coef, a, rolled)
        for c in range(3):
            misfit[c, a] = jnp.where(inside, coef[RHS + c, a - 1] - applied[c], 0.0)
    write = pltpu.make_async_copy(staged, payload, sem)

    def coarse_stretch():
        coarse_part([misfit[0, a, 0:8] for a in range(2, 6)], agg, coarse, sums, spread, staged)
        write.start()

    if coarse_fetch is not None:
        coarse_fetch.wait()
    local_solve(misfit, coef, values, factors_hbm, factors, tile_sems, current, one, two, coarse_stretch)
    odd = is_odd("wide")
    for c in range(3):
        for p in range(2):
            at = c * 16 + p * 8
            far[at : at + 8] = pick(odd, current[c, 2 + p], current[c, p])
            near[at : at + 8] = pick(odd, current[c, p], current[c, 2 + p])
    write.wait()


def fetch_tiles(factors_hbm, factors, sems):
    cols = [slice(1, 11) if a in (0, 5) else slice(0, 12) for a in range(6)]
    return [pltpu.make_async_copy(factors_hbm.at[a, cols[a]], factors.at[a, cols[a]], sems.at[a]) for a in range(6)]


def first_sweep(
    far,
    near,
    low,
    high,
    mine,
    agg,
    coarse_hbm,
    factors_hbm,
    coef,
    slots,
    payload,
    current,
    far_out,
    near_out,
    rim,
    coarse,
    coarse_sem,
    values,
    *scratch,
):
    coarse_fetch = pltpu.make_async_copy(coarse_hbm, coarse, coarse_sem)
    coarse_fetch.start()
    for fetch in fetch_tiles(factors_hbm, scratch[-3], scratch[-2]):
        fetch.start()
    odd = is_odd("wide")
    narrow_odd = is_odd("narrow")
    blank = jnp.zeros((ROWS, LANES), f32)

    def place(target, rows, at, width):
        target[...] = blank
        target[0:8] = rows
        a, b = low[at : at + width], high[at : at + width]
        target[8 : 8 + width] = pick(narrow_odd, a, b)
        target[16 - width : 16] = pick(narrow_odd, b, a)

    for f in range(FULL):
        for a in range(8):
            rows = rim_rows(odd, far, near, mine, f, f * 16, 2, a)
            target = values.at[f - 3, a] if 3 <= f < 6 else rim.at[f if f < 3 else 3, a]
            place(target, rows, (f * 8 + a) * 3, 3)
    for t in range(THIN):
        for a in range(1, 7):
            rows = rim_rows(odd, far, near, mine, FULL + t, FULL * 16 + t * 8, 1, a)
            target = coef.at[CENTRE if t == 0 else COUP + t - 1 if t < 10 else RHS + t - 10, a - 1]
            place(target, rows, FULL * 24 + (t * 6 + a - 1) * 2, 2)
    row = lax.broadcasted_iota(jnp.int32, (ROWS, LANES), 0)
    lane = lane_index((ROWS, LANES))
    low = lane < 64
    place_of = lax.axis_index("narrow")
    below, here, above = (32 * ((place_of + i) % 4) for i in (3, 0, 1))
    offset = jnp.where(row < 8, here, jnp.where(row < 12, above, below))
    inside = box_mask()
    for a in range(8):
        slots[a] = rim[3, a].astype(jnp.int32) + offset
    for a in range(1, 7):
        tx, ty = rim[0, a], rim[1, a]
        tz = jnp.where((lane % 64) < 63, rim[2, a], 0.0)
        txw = jnp.where(low, swap_halves(rim[0, a - 1]), swap_halves(tx))
        tys = shifted(ty, -1, 0)
        tzm = shifted(tz, -1, 1)
        centre = coef[CENTRE, a - 1] + (tx + txw + ty + tys + tz + tzm)
        coef[TX, a - 1] = tx
        coef[TXW, a - 1] = txw
        coef[TY, a - 1] = ty
        coef[TYS, a - 1] = tys
        coef[TZ, a - 1] = tz
        coef[TZM, a - 1] = tzm
        coef[CENTRE, a - 1] = centre
        for c in range(3):
            diagonal = jnp.where(inside, centre + coef[COUP + 4 * c, a - 1], 1.0)
            coef[INV + c, a - 1] = jnp.where(inside, 1.0 / diagonal, 0.0)
    solve_box(values, coef, agg, coarse, factors_hbm, payload, current, far_out, near_out, scratch, coarse_fetch)


def gather_values(current, far, near, low, high, part, slots, values):
    odd = is_odd("wide")
    narrow_odd = is_odd("narrow")
    total = part[...] + high[72:80]
    blank = jnp.zeros((2, LANES), f32)
    for a in range(8):
        block = 0 if a < 2 else 2 if a >= 6 else 1
        table = jnp.broadcast_to(total[block : block + 1], (8, LANES))
        for c in range(3):
            at = (c * 8 + a) * 3
            first, second = low[at : at + 3], high[at : at + 3]
            values[c, a, 0:8] = rim_rows(odd, far, near, current, c, c * 16, 2, a)
            values[c, a, 8:11] = pick(narrow_odd, first, second)
            values[c, a, 11:13] = blank
            values[c, a, 13:16] = pick(narrow_odd, second, first)
        for half in range(2):
            where = slots[a, 8 * half : 8 * half + 8]
            lifted = jnp.take_along_axis(table, where, axis=1, mode="promise_in_bounds")
            values[0, a, 8 * half : 8 * half + 8] += lifted


def next_sweep(
    current,
    far,
    near,
    low,
    high,
    part,
    slots,
    coef,
    agg,
    coarse,
    factors_hbm,
    payload,
    moved,
    far_out,
    near_out,
    values,
    *scratch,
):
    for fetch in fetch_tiles(factors_hbm, scratch[-3], scratch[-2]):
        fetch.start()
    gather_values(current, far, near, low, high, part, slots, values)
    solve_box(values, coef, agg, coarse, factors_hbm, payload, moved, far_out, near_out, scratch)


def pack_last_low(current, low):
    narrow_odd = is_odd("narrow")
    for c in range(3):
        for p in range(4):
            v = current[c, p]
            low[4 * c + p : 4 * c + p + 1] = pick(narrow_odd, v[7:8], v[0:1])
    low[12:16] = jnp.zeros((4, LANES), f32)


def pack_last_high(current, received, _, high, part):
    narrow_odd = is_odd("narrow")
    for c in range(3):
        for p in range(4):
            v = current[c, p]
            high[4 * c + p : 4 * c + p + 1] = pick(narrow_odd, v[0:1], v[7:8])
    high[12:16] = jnp.zeros((4, LANES), f32)
    group_sums(received, part)
    high[16:24] = part[...]


def last_misfit(current, far, near, low, high, part, slots, coef, iterate, residual, values):
    odd = is_odd("wide")
    narrow_odd = is_odd("narrow")
    total = part[...] + high[16:24]
    blank = jnp.zeros((8, LANES), f32)
    for a in range(1, 7):
        block = 0 if a < 2 else 2 if a >= 6 else 1
        table = jnp.broadcast_to(total[block : block + 1], (8, LANES))
        for c in range(3):
            values[c, a, 0:8] = rim_rows(odd, far, near, current, c, c * 16, 2, a)
            values[c, a, 8:16] = blank
            if 2 <= a < 6:
                at = 4 * c + a - 2
                first, second = low[at : at + 1], high[at : at + 1]
                values[c, a, 8:9] = pick(narrow_odd, first, second)
                values[c, a, 15:16] = pick(narrow_odd, second, first)
        for half in range(2):
            where = slots[a, 8 * half : 8 * half + 8]
            lifted = jnp.take_along_axis(table, where, axis=1, mode="promise_in_bounds")
            values[0, a, 8 * half : 8 * half + 8] += lifted
    rolled = {}
    for a in range(2, 6):
        applied = operate_pair(values, coef, a, rolled)
        for c in range(3):
            iterate[c, a - 2] = values[c, a, 0:8]
            residual[c, a - 2] = (coef[RHS + c, a - 1] - applied[c])[0:8]


def local_solve(misfit, coef, values, factors_hbm, factors, sems, moved, one, two, beside):
    fetches = fetch_tiles(factors_hbm, factors, sems)
    own_cols = list(range(8))
    row8 = lax.broadcasted_iota(jnp.int32, (24, LANES), 0) % 8

    def tiles(values, pair, cols, half):
        scaled = [coef[INV + c, pair - 1, 8 * half : 8 * half + 8] * values[c] for c in range(3)]
        left = jnp.concatenate(scaled, axis=0).astype(jnp.bfloat16)
        total = jnp.zeros((24, LANES), f32)
        for y in cols:
            product = lax.dot_general(
                left, factors[pair - 1, y + 2], (((1,), (1,)), ((), ())), preferred_element_type=f32
            )
            total = jnp.where(row8 == y % 8, product, total)
        return [total[8 * c : 8 * c + 8] for c in range(3)]

    blank = jnp.zeros((ROWS, LANES), f32)
    for c in range(3):
        for ref in (one, two):
            ref[c, 0] = blank
            ref[c, 7] = blank
    for a in range(1, 7):
        edge = a in (1, 6)
        if a in (1, 4):
            for fetch in fetches[a - 1 : a + 2]:
                fetch.wait()
        for half, cols in ((0, own_cols), (1, [8, -1] if edge else [8, 9, -2, -1])):
            part = tiles([misfit[c, a, 8 * half : 8 * half + 8] for c in range(3)], a, cols, half)
            for c in range(3):
                one[c, a, 8 * half : 8 * half + 8] = part[c]
        if a == 3:
            beside()
    rolled = {}
    for a in range(1, 7):
        edge = a in (1, 6)
        applied = operate_pair(one, coef, a, rolled)
        left = [misfit[c, a] - applied[c] for c in range(3)]
        for half, cols in ((0, own_cols), (1, [] if edge else [8, -1])):
            if not cols:
                for c in range(3):
                    two[c, a, 8:16] = one[c, a, 8:16]
                continue
            part = tiles([v[8 * half : 8 * half + 8] for v in left], a, cols, half)
            for c in range(3):
                two[c, a, 8 * half : 8 * half + 8] = one[c, a, 8 * half : 8 * half + 8] + part[c]
    rolled = {}
    for a in range(2, 6):
        applied = operate_pair(two, coef, a, rolled)
        part = tiles([(misfit[c, a] - applied[c])[0:8] for c in range(3)], a, own_cols, 0)
        for c in range(3):
            moved[c, a - 2] = values[c, a, 0:8] + (two[c, a, 0:8] + part[c])


def call(body, outs, scratch, operands, in_hbm=(), out_hbm=(), flops=1000000):
    vmem = pl.BlockSpec(memory_space=pltpu.VMEM)
    hbm = pl.BlockSpec(memory_space=pltpu.HBM)
    operands = [pltpu.with_memory_space_constraint(x, pltpu.HBM) if i in in_hbm else x for i, x in enumerate(operands)]
    return pl.pallas_call(
        body,
        out_shape=[
            pltpu.HBM(shape, dtype) if i in out_hbm else jax.ShapeDtypeStruct(shape, dtype)
            for i, (shape, dtype) in enumerate(outs)
        ],
        in_specs=[hbm if i in in_hbm else vmem for i in range(len(operands))],
        out_specs=[hbm if i in out_hbm else vmem for i in range(len(outs))],
        scratch_shapes=scratch,
        compiler_params=pltpu.CompilerParams(vmem_limit_bytes=VMEM_LIMIT),
        cost_estimate=pl.CostEstimate(flops=flops, bytes_accessed=0, transcendentals=0),
    )(*operands)


def swap_far(axis, values):
    count = lax.axis_size(axis)
    return lax.ppermute(values, axis, [(i, (i + (1 if i % 2 else -1)) % count) for i in range(count)])


def swap_near(axis, values):
    return lax.ppermute(values, axis, [(i, i ^ 1) for i in range(lax.axis_size(axis))])


def swaps(axis, far, near):
    return swap_far(axis, far), swap_near(axis, near)


def per_device(
    rhs, start, trans, accum, coupling, well_cells, well_index, agg_map, tile_factors, coarse_inverse
):
    devices = lax.axis_size("wide") * lax.axis_size("narrow")
    members = devices // 2
    groups = [[4 * w + n for w in range(devices // 4) for n in (parity, parity + 2)] for parity in range(2)]
    dma = pltpu.SemaphoreType.DMA
    own = ((3, 4, 8, LANES), f32)
    box = (3, PAIRS, ROWS, LANES)
    wide_type = ((48, LANES), f32)
    narrow_type = ((72, LANES), f32)
    payload_type = ((members * 3, LANES), f32)
    scratch = [
        pltpu.VMEM(box, f32),
        pltpu.VMEM(box, f32),
        pltpu.VMEM((AGG_LOC, LANES), f32),
        pltpu.VMEM((devices // 4 + 8, LANES), f32),
        pltpu.VMEM(payload_type[0], f32),
        pltpu.VMEM(box, f32),
        pltpu.VMEM(box, f32),
        pltpu.VMEM(tile_factors.shape, tile_factors.dtype),
        dma((6,)),
        dma,
    ]

    mine, agg, far, near = call(
        add_wells_and_pack,
        [((FULL + THIN, 4, 8, LANES), f32), ((4, 8, LANES), f32)] + [((WIDE_ROWS, LANES), f32)] * 2,
        [
            pltpu.VMEM((1, 64), jnp.int32),
            pltpu.VMEM((1, 64), f32),
            pltpu.VMEM((4, 8, LANES), f32),
            pltpu.VMEM((4, 8, LANES), jnp.int32),
            dma((8,)),
        ],
        [
            well_cells.reshape(1, -1),
            well_index.reshape(1, -1),
            accum,
            trans,
            start,
            agg_map,
            coupling.reshape((9,) + accum.shape),
            rhs,
        ],
        in_hbm=range(8),
    )
    far, near = swaps("wide", far, near)
    low, high = call(pack_narrow, [((NARROW_ROWS, LANES), f32)] * 2, [], [far, near, mine])
    low, high = swaps("narrow", low, high)
    coef, slots, payload, current, far, near = call(
        first_sweep,
        [((N_COEF, 6, ROWS, LANES), f32), ((PAIRS, ROWS, LANES), jnp.int32), payload_type, own, wide_type, wide_type],
        [pltpu.VMEM((4, PAIRS, ROWS, LANES), f32), pltpu.VMEM(coarse_inverse.shape, f32), dma] + scratch,
        [far, near, low, high, mine, agg, coarse_inverse, tile_factors],
        in_hbm=(6, 7),
        out_hbm=(2,),
    )
    for sweep in range(SWEEPS):
        blocks = payload.reshape(members, 1, 3 * LANES)
        received = lax.all_to_all(blocks, ("wide", "narrow"), 0, 0, axis_index_groups=groups).reshape(payload_type[0])
        far, near = swaps("wide", far, near)
        if sweep < SWEEPS - 1:
            low, high, part = call(
                pack_current, [narrow_type, ((80, LANES), f32), ((8, LANES), f32)], [], [current, far, near, received]
            )
            low, high = swaps("narrow", low, high)
        else:
            (low,) = call(pack_last_low, [((16, LANES), f32)], [], [current])
            low = swap_far("narrow", low)
            high, part = call(pack_last_high, [((24, LANES), f32), ((8, LANES), f32)], [], [current, received, low])
            high = swap_near("narrow", high)
        known = [current, far, near, low, high, part, slots, coef]
        if sweep < SWEEPS - 1:
            payload, current, far, near = call(
                next_sweep,
                [payload_type, own, wide_type, wide_type],
                scratch,
                known + [agg, coarse_inverse, tile_factors],
                in_hbm=(10,),
                out_hbm=(0,),
            )
        else:
            iterate, residual = call(last_misfit, [own, own], [pltpu.VMEM(box, f32)], known)
    return iterate, residual


def solution(mesh):
    return jax.shard_map(
        per_device,
        mesh=mesh,
        in_specs=(
            P(None, "wide", "narrow", None),
            P(None, "wide", "narrow", None),
            P(None, "wide", "narrow", None),
            P("wide", "narrow", None),
            P(None, None, "wide", "narrow", None),
            P("wide", "narrow", None),
            P("wide", "narrow", None),
            P("wide", "narrow", None),
            P("wide", "narrow", None, None),
            P(("wide", "narrow"), None),
        ),
        out_specs=(P(None, "wide", "narrow", None), P(None, "wide", "narrow", None)),
        check_vma=False,
    )
```
